128 devices in a mesh: teach: 2 (over core), dp: 64 (over x, z, y).
Axes of the slice: x: 4, y: 4, z: 4, core: 2. Of those that a mesh axis runs over, the one named last changes fastest.
Arguments:
- teacher_logits: bfloat16 [2, 16384, 5000], P('teach', 'dp'), may hold values from -18 to 400
- routes: int32 [16384, 1], P('dp'), may hold values from 0 to 127; in each aligned block of 256 rows (0 to 255, 256 to 511, ...) at most 4 rows name the same one
- agreement: int32 [16384], P('dp'), may hold values 0 or 1
- targets: int32 [16384], P('dp'), may hold values from 0 to 4999
- lengths: int32 [64], P('dp'), may hold values from 64 to 256
- student_hidden: bfloat16 [32768, 1024], P(('teach', 'dp')), may hold values from -6 to 6
- out_weight: bfloat16 [1024, 5000], replicated, may hold values from -2 to 2
- out_bias: float32 [5000], replicated, may hold values from -6 to 6
- gain: float32 [1024], replicated, may hold values from 0.5 to 1.5
Outputs:
- weight_grad: float32 [1024, 5000], P(('teach', 'dp'))
- gain_grad: float32 [1024], replicated
- bias_grad: float32 [5000], replicated
- loss: float32 [], replicated
The draws below stay inside these ranges and needn't reach their ends.
Inputs may be any that keep to these rules, and one draw needn't show every extreme that they name: `routes`: within the 256 rows of one index of dp, each student device is named at most 4 times, and some device exactly 4 times.
All inputs are finite; a program needn't handle non-finite values. No bound on the sum of `agreement` on one device may be relied on, other than what follows from the above.
Results may differ from the reference program's by a relative error of at most 0.0031.
Values may be sent and summed in bfloat16 or wider, within the bound.
A program may use at most 128 MiB of HBM per device.

```python
import math
import jax
import jax.numpy as jnp
import numpy as np
from jax import lax

D = 1024
V = 5000
LMAX = 256
UT = 1
RDEV = 256
NUTT = 64
TROWS = 16384
SROWS = 32768
MOST = 4
N_TEACH = 2
N_DP = 64
DEVICES = 128


def drawn_pair(key):
    states = jnp.clip(jax.random.normal(jax.random.fold_in(key, 11), (SROWS, D), jnp.float32), -6.0, 6.0)
    weights = jnp.clip(jax.random.normal(jax.random.fold_in(key, 12), (D, V), jnp.float32), -6.0, 6.0) / math.sqrt(D)
    return (states, jnp.clip(weights, -2.0, 2.0))


def draw_student_hidden(key, part):
    states, weights = drawn_pair(key)
    return states.astype(jnp.bfloat16)


def draw_out_weight(key, part):
    states, weights = drawn_pair(key)
    return weights.astype(jnp.bfloat16)


def draw_teacher_logits(key, part):
    shape = (2, TROWS, V)
    values = jnp.clip(3.0 * jax.random.normal(jax.random.fold_in(key, 22), shape, jnp.float32), -18.0, 18.0)
    return values.astype(jnp.bfloat16)


def draw_lengths(key, part):
    utterance = jnp.arange(NUTT, dtype=jnp.int32)
    device_pos = utterance // UT
    lowest = LMAX // 4 + LMAX // 2 * device_pos // max(N_DP - 1, 1)
    values = lowest + jax.random.randint(jax.random.fold_in(key, 31), (NUTT,), 0, LMAX // 4 + 1)
    values = jnp.minimum(values, LMAX)
    values = values.at[0].set(LMAX // 4).at[NUTT - 1].set(LMAX)
    return values.astype(jnp.int32)


def plant(values, key, smallest, largest):
    place = [jax.random.randint(jax.random.fold_in(key, axis), (), 0, length) for axis, length in enumerate(values.shape)]
    widest = values.shape.index(max(values.shape))
    next_to = place[:widest] + [(place[widest] + 1) % values.shape[widest]] + place[widest + 1:]
    return values.at[tuple(place)].set(smallest).at[tuple(next_to)].set(largest)


def routed_block(stream_key, own, number, rows, number_of, top, reach, skew):
    sequence = jax.random.permutation(stream_key, number_of)
    heavy_load, ordinary = portions_of(number_of, rows * top, reach, skew, True), portions_of(number_of, rows * top, reach, skew, False)
    places = jnp.arange(number_of)

    def named(tallies, turn):
        used = int((tallies > 0).sum())
        fixed = max(1, used // 4)
        passed = fixed + (places - fixed + turn * (used - fixed)) % max(1, number_of - fixed)
        return jnp.zeros((number_of,), jnp.int32).at[sequence[jnp.where(places < fixed, places, passed)]].set(jnp.asarray(tallies, jnp.int32))

    tallies = jnp.where(number % 4 == 0, named(heavy_load, number // 4), named(ordinary, number - number // 4 - 1))
    mixed = jax.random.permutation(jax.random.fold_in(own, 3), number_of)
    giver, taker = mixed[0:number_of // 2 * 2:2], mixed[1:number_of // 2 * 2:2]
    room = jnp.minimum(tallies[giver] - 1, reach - tallies[taker]) // 2
    room = jnp.where((giver == sequence[0]) | (taker == sequence[0]) | (tallies[taker] == 0), 0, jnp.maximum(room, 0))
    passed = jax.random.randint(jax.random.fold_in(own, 4), (number_of // 2,), 0, 1 << 20) % (room + 1)
    tallies = tallies.at[giver].add(-passed).at[taker].add(passed)
    items = jnp.searchsorted(jnp.cumsum(tallies), jnp.arange(rows * top), side="right").astype(jnp.int32)
    listing = items.reshape(top, rows).T
    listing = listing[jax.random.permutation(jax.random.fold_in(own, 1), rows)]
    turn = jax.random.randint(jax.random.fold_in(own, 2), (rows, 1), 0, top)
    return jnp.take_along_axis(listing, (jnp.arange(top)[None, :] + turn) % top, axis=1)


def portions_of(amount, total, reach, lean, full):
    portions = [(1 << 20) // math.isqrt(grade ** lean) + 1 for grade in range(1, amount + 1)]
    largest = reach if full else min(reach, max(-(-total // amount), total * portions[0] // sum(portions)))
    least = 1 if total - largest >= amount - 1 else 0
    counts, surplus = [largest] + [least] * (amount - 1), total - largest - least * (amount - 1)
    while surplus > 0:
        candidates = [i for i in range(1, amount) if counts[i] < largest] or [i for i in range(1, amount) if counts[i] < reach]
        mass, remaining = sum([portions[i] for i in candidates]), surplus
        for i in candidates:
            more = min(reach - counts[i], max(1, remaining * portions[i] // mass), surplus)
            counts[i] = counts[i] + more
            surplus = surplus - more
    return np.array(counts)


def bell_draw(key, shape, scale, bound, kind=jnp.bfloat16):
    return jnp.clip(scale * jax.random.normal(key, shape, jnp.float32), -bound, bound).astype(kind)


def setup_inputs(seed: int = 0) -> dict:
    keys = jax.random.split(jax.random.key(seed), 10)
    teacher_logits = draw_teacher_logits(jax.random.fold_in(keys[9], 71), 0)
    routes_keys = jax.random.split(jax.random.fold_in(keys[1], 1), TROWS // RDEV)
    routes_turns = jax.random.permutation(jax.random.fold_in(keys[1], 3), TROWS // RDEV)
    routes = jax.vmap(lambda own, number: routed_block(jax.random.fold_in(keys[1], 2), own, number, RDEV, DEVICES, 1, MOST, 2))(routes_keys, routes_turns).reshape((TROWS, 1))
    agreement = plant((jax.random.randint(keys[2], (TROWS,), 0, 4) < 3).astype(jnp.int32), jax.random.fold_in(keys[2], 1), 0, 1)
    targets = plant(jax.random.randint(keys[3], (TROWS,), 0, V), jax.random.fold_in(keys[3], 1), 0, V - 1).astype(jnp.int32)
    lengths = draw_lengths(jax.random.fold_in(keys[9], 71), 0)
    student_hidden = draw_student_hidden(jax.random.fold_in(keys[9], 71), 0)
    out_weight = draw_out_weight(jax.random.fold_in(keys[9], 71), 0)
    out_bias = bell_draw(keys[7], (V,), 1.0, 6.0, jnp.float32)
    gain = jnp.clip(1.0 + 0.1 * jax.random.normal(keys[8], (D,), jnp.float32), 0.5, 1.5)
    return {"teacher_logits": teacher_logits, "routes": routes, "agreement": agreement, "targets": targets, "lengths": lengths, "student_hidden": student_hidden, "out_weight": out_weight, "out_bias": out_bias, "gain": gain}


EPSILON = 1e-05

def route_slots(dest_device, devices):
    onehot = (dest_device[:, None] == jnp.arange(devices, dtype=jnp.int32)[None, :]).astype(jnp.float32)
    row_ids = jnp.arange(dest_device.shape[0], dtype=jnp.int32)
    earlier = (row_ids[None, :] < row_ids[:, None]).astype(jnp.float32)
    before = jnp.dot(earlier, onehot, preferred_element_type=jnp.float32, precision=lax.Precision.HIGHEST)
    return lax.optimization_barrier(jnp.sum(before * onehot, axis=1)).astype(jnp.int32)

def live_mask(lengths_block, row_total):
    row_ids = jnp.arange(row_total, dtype=jnp.int32)
    utterance = row_ids // LMAX
    frame_pos = row_ids % LMAX
    picks = utterance[:, None] == jnp.arange(lengths_block.shape[0], dtype=jnp.int32)[None, :]
    row_length = lax.optimization_barrier(jnp.sum(jnp.where(picks, lengths_block[None, :], 0), axis=1))
    return (frame_pos < row_length).astype(jnp.float32)

def soft_targets(teacher_rows, agree_rows, target_rows, live_rows):
    probs_teacher = jax.nn.softmax(teacher_rows.astype(jnp.float32), axis=-1)
    onehot = (target_rows[:, None] == jnp.arange(probs_teacher.shape[1], dtype=jnp.int32)[None, :]).astype(jnp.float32)
    weight = (0.5 * agree_rows.astype(jnp.float32))[:, None]
    return (live_rows[:, None] * (weight * probs_teacher + 0.5 * onehot)).astype(jnp.bfloat16)

def student_forward(hidden_rows, gain, out_weight, out_bias):
    states = hidden_rows.astype(jnp.float32)
    centre = lax.optimization_barrier(jnp.mean(states, axis=1, keepdims=True))
    spread = lax.optimization_barrier(jnp.mean(jnp.square(states - centre), axis=1, keepdims=True))
    normed = (states - centre) * lax.rsqrt(spread + EPSILON)
    scaled = (normed * gain[None, :]).astype(jnp.bfloat16)
    logits = jnp.dot(scaled, out_weight, preferred_element_type=jnp.float32) + out_bias[None, :]
    return (normed, scaled, jax.nn.log_softmax(logits, axis=-1))

def combined_grads(first_soft, second_soft, log_probs):
    first_float = first_soft.astype(jnp.float32)
    second_float = second_soft.astype(jnp.float32)
    row_mass = lax.optimization_barrier(jnp.sum(first_float + second_float, axis=1, keepdims=True))
    return (row_mass * jnp.exp(log_probs) - first_float - second_float).astype(jnp.bfloat16)

def reference(teacher_logits, routes, agreement, targets, lengths, student_hidden, out_weight, out_bias, gain):
    devices = N_TEACH * N_DP
    most_slots = 2 * RDEV // devices

    def one_block(totals, block_id):
        first_row = block_id * RDEV
        dest_device = lax.dynamic_slice_in_dim(routes[:, 0], first_row, RDEV, 0)
        slot_index = route_slots(dest_device, devices)
        lengths_block = lax.dynamic_slice_in_dim(lengths, block_id * UT, UT, 0)
        live_rows = live_mask(lengths_block, RDEV)
        agree_rows = lax.dynamic_slice_in_dim(agreement, first_row, RDEV, 0)
        target_rows = lax.dynamic_slice_in_dim(targets, first_row, RDEV, 0)
        student_index = (dest_device * RDEV + block_id * most_slots + slot_index).astype(jnp.int32)
        hidden_rows = jnp.take(student_hidden, student_index, axis=0)
        normed, scaled, log_probs = student_forward(hidden_rows, gain, out_weight, out_bias)
        weight_sum, gain_sum, bias_sum, loss_sum, frame_sum = totals
        first_soft = soft_targets(lax.dynamic_slice_in_dim(teacher_logits[0], first_row, RDEV, 0), agree_rows, target_rows, live_rows)
        second_soft = soft_targets(lax.dynamic_slice_in_dim(teacher_logits[1], first_row, RDEV, 0), agree_rows, target_rows, live_rows)
        grad_rows = combined_grads(first_soft, second_soft, log_probs)
        weight_sum = weight_sum + jnp.dot(scaled.T, grad_rows, preferred_element_type=jnp.float32)
        back_rows = lax.dot_general(grad_rows, out_weight, (((1,), (1,)), ((), ())), preferred_element_type=jnp.float32)
        gain_sum = gain_sum + lax.optimization_barrier(jnp.sum(back_rows * normed, axis=0))
        bias_sum = bias_sum + lax.optimization_barrier(jnp.sum(grad_rows.astype(jnp.float32), axis=0))
        loss_sum = loss_sum - jnp.sum((first_soft.astype(jnp.float32) + second_soft.astype(jnp.float32)) * log_probs)
        frame_sum = frame_sum + jnp.sum(live_rows)
        return ((weight_sum, gain_sum, bias_sum, loss_sum, frame_sum), None)
    initial = (jnp.zeros((D, V), jnp.float32), jnp.zeros((D,), jnp.float32), jnp.zeros((V,), jnp.float32), jnp.zeros((), jnp.float32), jnp.zeros((), jnp.float32))
    totals, _ = lax.scan(one_block, initial, jnp.arange(N_DP, dtype=jnp.int32))
    weight_sum, gain_sum, bias_sum, loss_sum, frame_sum = totals
    inverse = 1.0 / frame_sum
    return (weight_sum * inverse, gain_sum * inverse, bias_sum * inverse, loss_sum * inverse)
```

```python
import jax
import jax.numpy as jnp
from jax import lax
from jax.experimental import pallas as pl
from jax.experimental.pallas import tpu as pltpu
from jax.sharding import Mesh
from jax.sharding import PartitionSpec as P

LMAX = 256
DP = ("dp_0", "dp_1", "dp_2")
TEACH_DP = ("teach", "dp_0", "dp_1", "dp_2")
MESH = pl.DeviceIdType.MESH

EPSILON = 1e-05

HALF_V = 2560
THIRDS = ((0, 896), (896, 896), (1792, 768))
WIDEST = 896
STAGE_ROWS = (256, 128, 64, 32, 16, 8)
STAGE_AT = (0, 256, 384, 448, 480, 496)
PARTS = 6
STAGES = 6


def route_slots(dest_device, devices):
    onehot = (dest_device[:, None] == jnp.arange(devices, dtype=jnp.int32)[None, :]).astype(
        jnp.float32
    )
    row_ids = jnp.arange(dest_device.shape[0], dtype=jnp.int32)
    earlier = (row_ids[None, :] < row_ids[:, None]).astype(jnp.float32)
    before = jnp.dot(
        earlier, onehot, preferred_element_type=jnp.float32, precision=lax.Precision.HIGHEST
    )
    return jnp.sum(before * onehot, axis=1).astype(jnp.int32)


def live_mask(lengths_block, row_total):
    row_ids = jnp.arange(row_total, dtype=jnp.int32)
    utterance = row_ids // LMAX
    frame_pos = row_ids % LMAX
    picks = utterance[:, None] == jnp.arange(lengths_block.shape[0], dtype=jnp.int32)[None, :]
    row_length = jnp.sum(jnp.where(picks, lengths_block[None, :], 0), axis=1)
    return (frame_pos < row_length).astype(jnp.float32)


def soft_targets(teacher_rows, agree_rows, target_rows, live_rows):
    probs_teacher = jax.nn.softmax(teacher_rows.astype(jnp.float32), axis=-1)
    onehot = (
        target_rows[:, None] == jnp.arange(probs_teacher.shape[1], dtype=jnp.int32)[None, :]
    ).astype(jnp.float32)
    weight = (0.5 * agree_rows.astype(jnp.float32))[:, None]
    return (live_rows[:, None] * (weight * probs_teacher + 0.5 * onehot)).astype(jnp.bfloat16)


def student_forward(hidden_rows, gain, out_weight, out_bias):
    states = hidden_rows.astype(jnp.float32)
    centre = jnp.mean(states, axis=1, keepdims=True)
    spread = jnp.mean(jnp.square(states - centre), axis=1, keepdims=True)
    normed = (states - centre) * lax.rsqrt(spread + EPSILON)
    scaled = (normed * gain[None, :]).astype(jnp.bfloat16)
    logits = jnp.dot(scaled, out_weight, preferred_element_type=jnp.float32) + out_bias[None, :]
    return (normed, scaled, jax.nn.log_softmax(logits, axis=-1))


def combined_grads(first_soft, second_soft, log_probs):
    first_float = first_soft.astype(jnp.float32)
    second_float = second_soft.astype(jnp.float32)
    row_mass = jnp.sum(first_float + second_float, axis=1, keepdims=True)
    return (row_mass * jnp.exp(log_probs) - first_float - second_float).astype(jnp.bfloat16)


def chunk_of(part, row):
    bits = [0] * 6
    for k in range(6):
        bits[(part + k) % 6] = (row >> (5 - k)) & 1
    chip = 0
    for dim in range(3):
        low, high = bits[dim], bits[3 + dim]
        chip = chip * 4 + high * 2 + (high ^ low)
    return chip


def reduce_kernel(
    scaled_ref, grad_ref, vec_ref, out_ref, vec_out_ref,
    lhs, acc, sent, got, sent_last, got_last, final, final_in, vec, vec_in,
    send_sem, recv_sem, vec_send_sem, vec_recv_sem, final_send_sem, final_recv_sem,
):
    t = lax.axis_index("teach")
    place = [lax.axis_index(axis) for axis in DP]

    def partner(bit):
        ids = list(place)
        v = place[bit % 3]
        ids[bit % 3] = (3 - v) if bit >= 3 else (v + 1 - 2 * (v % 2))
        return (t, ids[0], ids[1], ids[2])

    def my_bit(bit):
        v = place[bit % 3]
        return v // 2 if bit >= 3 else (v // 2 + v % 2) % 2

    partners = [partner(bit) for bit in range(6)]
    mine = [my_bit(bit) for bit in range(6)]
    other_core = (1 - t, place[0], place[1], place[2])

    barrier = pltpu.get_barrier_semaphore()
    for device in partners + [other_core]:
        pl.semaphore_signal(barrier, inc=1, device_id=device, device_id_type=MESH)

    for part in range(PARTS):
        half = part // 3
        for row in range(0, 64, 2):
            pair = jnp.concatenate(
                [scaled_ref[half * 64 + chunk_of(part, row)], scaled_ref[half * 64 + chunk_of(part, row + 1)]],
                axis=0,
            )
            lhs[part, row * 8:row * 8 + 16, :] = pair.astype(jnp.bfloat16)

    pl.semaphore_wait(barrier, 7)

    def copy_of(part, stage):
        width = THIRDS[part % 3][1]
        if stage == STAGES - 1:
            source = sent_last.at[part, :, 0:width]
            target = got_last.at[part, :, 0:width]
        else:
            rows = slice(STAGE_AT[stage], STAGE_AT[stage] + STAGE_ROWS[stage])
            source = sent.at[part, rows, 0:width]
            target = got.at[part, rows, 0:width]
        return pltpu.make_async_remote_copy(
            src_ref=source,
            dst_ref=target,
            send_sem=send_sem.at[part * STAGES + stage],
            recv_sem=recv_sem.at[part * STAGES + stage],
            device_id=partners[(part + stage) % 6],
            device_id_type=MESH,
        )

    def vec_copy(stage):
        return pltpu.make_async_remote_copy(
            src_ref=vec.at[stage],
            dst_ref=vec_in.at[stage],
            send_sem=vec_send_sem.at[stage],
            recv_sem=vec_recv_sem.at[stage],
            device_id=partners[stage] if stage < STAGES else other_core,
            device_id_type=MESH,
        )

    vec[0] = vec_ref[...]
    vec_copy(0).start()

    for part in range(PARTS):
        first, width = THIRDS[part % 3]
        away = pl.multiple_of((1 - mine[part]) * 256, 256)
        block = jnp.dot(
            lhs[part, pl.ds(away, 256), :], grad_ref[:, first:first + width],
            preferred_element_type=jnp.float32,
        )
        sent[part, 0:256, 0:width] = block.astype(jnp.bfloat16)
        copy_of(part, 0).start()
    for part in range(PARTS):
        first, width = THIRDS[part % 3]
        stay = pl.multiple_of(mine[part] * 256, 256)
        acc[part, :, 0:width] = jnp.dot(
            lhs[part, pl.ds(stay, 256), :], grad_ref[:, first:first + width],
            preferred_element_type=jnp.float32,
        )

    base = [0] * PARTS
    for stage in range(1, STAGES):
        rows = STAGE_ROWS[stage]
        before = STAGE_AT[stage - 1]
        for part in range(PARTS):
            width = THIRDS[part % 3][1]
            bit = mine[(part + stage) % 6]
            away, stay = (1 - bit) * rows, bit * rows
            copy_of(part, stage - 1).wait_recv()
            if stage < STAGES - 1:
                at = pl.multiple_of(base[part] + away, 16)
                block = acc[part, pl.ds(at, rows), 0:width] + got[
                    part, pl.ds(pl.multiple_of(before + away, 16), rows), 0:width
                ].astype(jnp.float32)
                sent[part, STAGE_AT[stage]:STAGE_AT[stage] + rows, 0:width] = block.astype(jnp.bfloat16)
                copy_of(part, stage).start()
                at = pl.multiple_of(base[part] + stay, 16)
                acc[part, pl.ds(at, rows), 0:width] += got[
                    part, pl.ds(pl.multiple_of(before + stay, 16), rows), 0:width
                ].astype(jnp.float32)
            else:
                at = pl.multiple_of(base[part] + 0, 16)
                acc[part, pl.ds(at, 2 * rows), 0:width] += got[
                    part, before:before + 2 * rows, 0:width
                ].astype(jnp.float32)
                at = pl.multiple_of(base[part] + away, 8)
                sent_last[part, :, 0:width] = acc[part, pl.ds(at, rows), 0:width]
                copy_of(part, stage).start()
            base[part] = base[part] + stay
        vec_copy(stage - 1).wait_recv()
        vec[stage] = vec[stage - 1] + vec_in[stage - 1]
        vec_copy(stage).start()

    vec_copy(STAGES - 1).wait_recv()
    vec[STAGES] = vec[STAGES - 1] + vec_in[STAGES - 1]
    vec_copy(STAGES).start()
    for part in range(PARTS):
        first, width = THIRDS[part % 3]
        copy_of(part, STAGES - 1).wait_recv()
        at = pl.multiple_of(base[part], 8)
        final[part // 3, :, first:first + width] = (
            acc[part, pl.ds(at, 8), 0:width] + got_last[part, :, 0:width]
        )

    swap = pltpu.make_async_remote_copy(
        src_ref=final.at[1 - t],
        dst_ref=final_in,
        send_sem=final_send_sem,
        recv_sem=final_recv_sem,
        device_id=other_core,
        device_id_type=MESH,
    )
    swap.start()
    out_ref[t] = final[t]
    vec_out_ref[t] = vec[STAGES]
    vec_copy(STAGES).wait_recv()
    vec_out_ref[1 - t] = vec_in[STAGES]
    swap.wait_recv()
    out_ref[1 - t] = final_in[...]

    for part in range(PARTS):
        for stage in range(STAGES):
            copy_of(part, stage).wait_send()
    for stage in range(STAGES + 1):
        vec_copy(stage).wait_send()
    swap.wait_send()


def reduce_grads(scaled_t, grad, vec):
    rows = scaled_t.shape[-1]
    vmem = pl.BlockSpec(memory_space=pltpu.VMEM)
    buffer_rows = STAGE_AT[-1]
    dma = pltpu.SemaphoreType.DMA
    return pl.pallas_call(
        reduce_kernel,
        out_shape=(
            jax.ShapeDtypeStruct((2, 8, HALF_V), jnp.float32),
            jax.ShapeDtypeStruct((2,) + vec.shape, jnp.float32),
        ),
        in_specs=[vmem] * 3,
        out_specs=(vmem, vmem),
        scratch_shapes=[
            pltpu.VMEM((PARTS, 512, rows), jnp.bfloat16),
            pltpu.VMEM((PARTS, 256, WIDEST), jnp.float32),
            pltpu.VMEM((PARTS, buffer_rows, WIDEST), jnp.bfloat16),
            pltpu.VMEM((PARTS, buffer_rows, WIDEST), jnp.bfloat16),
            pltpu.VMEM((PARTS, 8, WIDEST), jnp.float32),
            pltpu.VMEM((PARTS, 8, WIDEST), jnp.float32),
            pltpu.VMEM((2, 8, HALF_V), jnp.float32),
            pltpu.VMEM((8, HALF_V), jnp.float32),
            pltpu.VMEM((STAGES + 1,) + vec.shape, jnp.float32),
            pltpu.VMEM((STAGES + 1,) + vec.shape, jnp.float32),
            dma((PARTS * STAGES,)),
            dma((PARTS * STAGES,)),
            dma((STAGES + 1,)),
            dma((STAGES + 1,)),
            dma,
            dma,
        ],
        compiler_params=pltpu.CompilerParams(
            collective_id=0, has_side_effects=True, vmem_limit_bytes=48 * 1024 * 1024
        ),
    )(scaled_t, grad, vec)


def body(
    teacher_logits, routes, agreement, targets, lengths, student_hidden, out_weight, out_bias, gain
):
    teach_count = lax.axis_size("teach")
    data_count = lax.axis_size(DP)
    devices = teach_count * data_count
    rows_here = teacher_logits.shape[1]
    most_slots = 2 * rows_here // devices
    vocab = teacher_logits.shape[2]
    width = student_hidden.shape[1]
    dest_device = routes[:, 0]
    slot_index = route_slots(dest_device, devices)
    live_rows = live_mask(lengths, rows_here)
    soft_rows = soft_targets(teacher_logits[0], agreement, targets, live_rows)
    half = rows_here // 2
    first_here = lax.axis_index("teach") * half
    count_term = jnp.sum(lax.dynamic_slice_in_dim(live_rows, first_here, half, 0))
    stacked = soft_rows.reshape(2, half, vocab)
    both_soft = lax.all_to_all(stacked, "teach", split_axis=0, concat_axis=0, tiled=True)
    dest_half = lax.dynamic_slice_in_dim(dest_device, first_here, half, 0)
    slot_half = lax.dynamic_slice_in_dim(slot_index, first_here, half, 0)
    replicated = jnp.broadcast_to(
        student_hidden.reshape(1, data_count, most_slots, width),
        (teach_count, data_count, most_slots, width),
    ).reshape(devices, most_slots, width)
    arrived = lax.all_to_all(replicated, TEACH_DP, split_axis=0, concat_axis=0, tiled=True)
    hidden_rows = arrived[dest_half, slot_half]
    norm_rows, state_rows, log_probs = student_forward(hidden_rows, gain, out_weight, out_bias)
    grad_rows = combined_grads(both_soft[0], both_soft[1], log_probs)
    loss_term = -jnp.sum(
        (both_soft[0].astype(jnp.float32) + both_soft[1].astype(jnp.float32)) * log_probs
    )
    back_rows = lax.dot_general(
        grad_rows, out_weight, (((1,), (1,)), ((), ())), preferred_element_type=jnp.float32
    )
    gain_grad = jnp.sum(back_rows * norm_rows, axis=0)

    padded = jnp.pad(grad_rows, ((0, 0), (0, 2 * HALF_V - vocab)))
    halves = jnp.swapaxes(padded.reshape(half, 2, HALF_V), 0, 1)
    grad_half = lax.all_to_all(halves, "teach", split_axis=0, concat_axis=0, tiled=True)
    grad_half = grad_half.reshape(rows_here, HALF_V)
    state_all = lax.all_gather(state_rows, "teach", axis=0, tiled=True)
    bias_grad = jnp.sum(grad_half.astype(jnp.float32), axis=0)
    scaled_t = state_all.astype(jnp.float32).T.reshape(width // 8, 8, rows_here)
    vec = jnp.concatenate(
        [gain_grad, bias_grad, loss_term[None], count_term[None], jnp.zeros((510,), jnp.float32)]
    ).reshape(8, 512)
    weight_grad, sums = reduce_grads(scaled_t, grad_half, vec)
    sums = sums.reshape(2, 4096)
    both = sums[0] + sums[1]
    inverse = 1.0 / both[width + HALF_V + 1]
    weight_grad = jnp.concatenate([weight_grad[0], weight_grad[1]], axis=1)[:, :vocab]
    bias_sum = jnp.concatenate(
        [sums[0, width:width + HALF_V], sums[1, width:width + vocab - HALF_V]]
    )
    return (
        weight_grad * inverse,
        both[:width] * inverse,
        bias_sum * inverse,
        both[width + HALF_V] * inverse,
    )


def solution(mesh):
    finer = Mesh(
        mesh.devices.reshape(mesh.shape["teach"], 4, 4, 4), ("teach", "dp_0", "dp_1", "dp_2")
    )
    in_specs = (
        P("teach", DP, None),
        P(DP, None),
        P(DP),
        P(DP),
        P(DP),
        P(TEACH_DP, None),
        P(),
        P(),
        P(),
    )
    out_specs = (P(TEACH_DP, None), P(), P(), P())
    return jax.shard_map(body, mesh=finer, in_specs=in_specs, out_specs=out_specs, check_vma=False)
```

```python
import jax
import jax.numpy as jnp
from jax import lax
from jax.experimental import pallas as pl
from jax.experimental.pallas import tpu as pltpu
from jax.sharding import Mesh
from jax.sharding import PartitionSpec as P

DP = ("dp_0", "dp_1", "dp_2")
TEACH_DP = ("teach", "dp_0", "dp_1", "dp_2")
MESH = pl.DeviceIdType.MESH
F32 = jnp.float32
BF16 = jnp.bfloat16

EPSILON = 1e-05
VOCAB = 5000
WIDTH = 1024
ROWS = 256
STUDENTS = 128

HALF_V = 2560
BLOCK_V = 512
BLOCKS = 5
LAST_WHOLE = 384
TAIL = 4992
THIRDS = ((0, 896), (896, 896), (1792, 768))
WIDEST = 896
STAGE_ROWS = (256, 128, 64, 32, 16, 8)
STAGE_AT = (0, 256, 384, 0, 32, 48)
NARROW = 3
NARROW_ROWS = 448
WIDE_ROWS = 56
PARTS = 6
STAGES = 6
VEC = WIDTH + HALF_V + 128
LOSS_AT = WIDTH + HALF_V
STEP = 16
QUARTERS = 4


def chunk_of(part, row):
    bits = [0] * 6
    for k in range(6):
        bits[(part + k) % 6] = (row >> (5 - k)) & 1
    chip = 0
    for dim in range(3):
        low, high = bits[dim], bits[3 + dim]
        chip = chip * 4 + high * 2 + (high ^ low)
    return chip


def rows_at(k, size=STEP):
    return pl.ds(pl.multiple_of(k * size, size), size)


def lane_ids(rows, width):
    return lax.broadcasted_iota(jnp.int32, (rows, width), 1)


def step_kernel(
    teacher_hbm, weight_hbm, tail_ref, meta_ref, arrived_ref, bias_ref, gain_ref,
    weight_out, gain_out, bias_out, loss_out,
    teacher, soft, soft_in, weight, cols, stats, stats_in, mine_h, their_h,
    normed, scaled, scaled_t, logits, grad,
    lhs, acc, sent, got, sent_wide, got_wide, final, final_in, vec, vec_in,
    teacher_sem, weight_sem, soft_send, soft_recv, pair_send, pair_recv,
    send_sem, recv_sem, vec_send_sem, vec_recv_sem,
):
    t = lax.axis_index("teach")
    place = [lax.axis_index(axis) for axis in DP]

    def partner(bit):
        ids = list(place)
        v = place[bit % 3]
        ids[bit % 3] = (3 - v) if bit >= 3 else (v + 1 - 2 * (v % 2))
        return (t, ids[0], ids[1], ids[2])

    def my_bit(bit):
        v = place[bit % 3]
        return v // 2 if bit >= 3 else (v // 2 + v % 2) % 2

    partners = [partner(bit) for bit in range(6)]
    mine = [my_bit(bit) for bit in range(6)]
    other_core = (1 - t, place[0], place[1], place[2])

    barrier = pltpu.get_barrier_semaphore()
    for device in partners + [other_core]:
        pl.semaphore_signal(barrier, inc=1, device_id=device, device_id_type=MESH)

    size = ROWS // QUARTERS
    teacher_copies = [
        pltpu.make_async_copy(
            teacher_hbm.at[0, q * size:(q + 1) * size, :],
            teacher.at[q * size:(q + 1) * size, :],
            teacher_sem.at[q],
        )
        for q in range(QUARTERS)
    ]
    for copy in teacher_copies:
        copy.start()
    first_column = t * HALF_V
    weight_copies = [
        pltpu.make_async_copy(
            weight_hbm.at[:, pl.ds(pl.multiple_of(first_column + i * BLOCK_V, 128), BLOCK_V)],
            weight.at[:, i * BLOCK_V:(i + 1) * BLOCK_V],
            weight_sem.at[i],
        )
        for i in range(BLOCKS - 1)
    ]
    last_at = (BLOCKS - 1) * BLOCK_V
    last_first = pltpu.make_async_copy(
        weight_hbm.at[:, last_at:HALF_V],
        weight.at[:, last_at:HALF_V],
        weight_sem.at[BLOCKS - 1],
    )
    last_second = pltpu.make_async_copy(
        weight_hbm.at[:, HALF_V + last_at:TAIL],
        weight.at[:, last_at:last_at + LAST_WHOLE],
        weight_sem.at[BLOCKS - 1],
    )
    for copy in weight_copies:
        copy.start()

    @pl.when(t == 0)
    def _():
        last_first.start()

    @pl.when(t == 1)
    def _():
        last_second.start()
        weight[:, last_at + LAST_WHOLE:HALF_V] = tail_ref[...]

    cols[:, 0:8] = jnp.transpose(meta_ref[...])
    routes_col = cols[:, 0:1]
    live = (
        lax.broadcasted_iota(jnp.int32, (ROWS, 1), 0).astype(F32) < cols[:, 3:4]
    ).astype(F32)
    cols[:, 4:5] = live * 0.5
    cols[:, 5:6] = live * 0.5 * cols[:, 1:2]
    frames_here = jnp.sum(live, axis=0, keepdims=True)

    named = (routes_col == lane_ids(ROWS, STUDENTS).astype(F32)).astype(F32)
    earlier = (lane_ids(ROWS, ROWS) < lax.broadcasted_iota(jnp.int32, (ROWS, ROWS), 0)).astype(F32)
    before = jnp.dot(earlier.astype(BF16), named.astype(BF16), preferred_element_type=F32)
    slot = jnp.sum(before * named, axis=1, keepdims=True)
    wanted = routes_col * 4.0 + slot - (t * ROWS).astype(F32)
    pick = (wanted == lane_ids(ROWS, ROWS).astype(F32)).astype(F32).astype(BF16)
    mine_h[...] = jnp.dot(pick, arrived_ref[...], preferred_element_type=F32).astype(BF16)

    def to_pair(source, target, index):
        return pltpu.make_async_remote_copy(
            src_ref=source,
            dst_ref=target,
            send_sem=pair_send.at[index],
            recv_sem=pair_recv.at[index],
            device_id=other_core,
            device_id_type=MESH,
        )

    pl.semaphore_wait(barrier, 7)
    hidden_swap = to_pair(mine_h, their_h, 0)
    hidden_swap.start()

    soft[:, TAIL:2 * HALF_V] = jnp.zeros((ROWS, 2 * HALF_V - TAIL), BF16)
    stat_lane = lane_ids(STEP, 128)

    def soft_step(k, carry):
        rows = rows_at(k)
        x = teacher[rows, :].astype(F32)
        e = jnp.exp(x - jnp.max(x, axis=1, keepdims=True))
        facts = cols[rows, :]
        scale = facts[:, 5:6] / jnp.sum(e, axis=1, keepdims=True)
        hit = lane_ids(STEP, VOCAB) == facts[:, 2:3].astype(jnp.int32)
        s = (e * scale + jnp.where(hit, facts[:, 4:5], 0.0)).astype(BF16)
        soft[rows, 0:VOCAB] = s
        mass = jnp.sum(s.astype(F32), axis=1, keepdims=True)
        stats[rows, :] = jnp.where(stat_lane == 1, mass, 0.0)
        return carry

    away_column = pl.multiple_of((1 - t) * HALF_V, 128)
    own_column = pl.multiple_of(t * HALF_V, 128)
    soft_copies = [
        pltpu.make_async_remote_copy(
            src_ref=soft.at[q * size:(q + 1) * size, pl.ds(away_column, HALF_V)],
            dst_ref=soft_in.at[q * size:(q + 1) * size, :],
            send_sem=soft_send.at[q],
            recv_sem=soft_recv.at[q],
            device_id=other_core,
            device_id_type=MESH,
        )
        for q in range(QUARTERS)
    ]
    for q in range(QUARTERS):
        teacher_copies[q].wait()
        lax.fori_loop(q * size // STEP, (q + 1) * size // STEP, soft_step, 0)
        soft_copies[q].start()

    hidden_swap.wait_recv()
    states = mine_h[...].astype(F32) + their_h[...].astype(F32)
    states = states - jnp.mean(states, axis=1, keepdims=True)
    spread = jnp.mean(jnp.square(states), axis=1, keepdims=True)
    states = states * lax.rsqrt(spread + EPSILON)
    normed[...] = states
    rounded = (states * gain_ref[...]).astype(BF16)
    scaled[...] = rounded
    scaled_t[...] = jnp.transpose(rounded.astype(F32)).reshape(WIDTH // 8, 8, ROWS)

    for i in range(BLOCKS):
        if i < BLOCKS - 1:
            weight_copies[i].wait()
        else:
            @pl.when(t == 0)
            def _():
                last_first.wait()

            @pl.when(t == 1)
            def _():
                last_second.wait()
        at = slice(i * BLOCK_V, (i + 1) * BLOCK_V)
        block = jnp.dot(scaled[...], weight[:, at], preferred_element_type=F32) + bias_ref[t, :, at]
        if i == BLOCKS - 1:
            inside = lane_ids(ROWS, BLOCK_V) < VOCAB - i * BLOCK_V - t * HALF_V
            block = jnp.where(inside, block, -1e30)
        logits[:, at] = block

    for part in range(PARTS):
        half = part // 3
        for row in range(0, 64, 2):
            pair = jnp.concatenate(
                [scaled_t[half * 64 + chunk_of(part, row)], scaled_t[half * 64 + chunk_of(part, row + 1)]],
                axis=0,
            )
            lhs[part, row * 8:row * 8 + 16, :] = pair.astype(BF16)

    def lse_step(k, carry):
        rows = rows_at(k)
        x = logits[rows, :]
        top = jnp.max(x, axis=1, keepdims=True)
        lse = top + jnp.log(jnp.sum(jnp.exp(x - top), axis=1, keepdims=True))
        stats[rows, :] = jnp.where(stat_lane == 0, lse, stats[rows, :])
        return carry

    lax.fori_loop(0, ROWS // STEP, lse_step, 0)
    stats_swap = to_pair(stats, stats_in, 1)
    stats_swap.start()
    for copy in soft_copies:
        copy.wait_recv()
    stats_swap.wait_recv()

    def grad_step(k, loss):
        rows = rows_at(k)
        here, there = stats[rows, :], stats_in[rows, :]
        one, two = here[:, 0:1], there[:, 0:1]
        top = jnp.maximum(one, two)
        lse = top + jnp.log(jnp.exp(one - top) + jnp.exp(two - top))
        mass = here[:, 1:2] + there[:, 1:2]
        log_probs = logits[rows, :] - lse
        both = soft[rows, pl.ds(own_column, HALF_V)].astype(F32) + soft_in[rows, :].astype(F32)
        grad[rows, :] = (mass * jnp.exp(log_probs) - both).astype(BF16)
        return loss - jnp.sum(both * log_probs, axis=1, keepdims=True)

    loss = lax.fori_loop(0, ROWS // STEP, grad_step, jnp.zeros((STEP, 1), F32))

    def copy_of(part, stage):
        width = THIRDS[part % 3][1]
        rows = slice(STAGE_AT[stage], STAGE_AT[stage] + STAGE_ROWS[stage])
        source, target = (sent, got) if stage < NARROW else (sent_wide, got_wide)
        return pltpu.make_async_remote_copy(
            src_ref=source.at[part, rows, 0:width],
            dst_ref=target.at[part, rows, 0:width],
            send_sem=send_sem.at[part * STAGES + stage],
            recv_sem=recv_sem.at[part * STAGES + stage],
            device_id=partners[(part + stage) % 6],
            device_id_type=MESH,
        )

    def vec_copy(stage):
        return pltpu.make_async_remote_copy(
            src_ref=vec.at[stage],
            dst_ref=vec_in.at[stage],
            send_sem=vec_send_sem.at[stage],
            recv_sem=vec_recv_sem.at[stage],
            device_id=partners[stage] if stage < STAGES else other_core,
            device_id_type=MESH,
        )

    for part in (0, 3, 1, 4, 2, 5):
        first, width = THIRDS[part % 3]
        away = pl.multiple_of((1 - mine[part]) * 256, 256)
        block = jnp.dot(
            lhs[part, pl.ds(away, 256), :], grad[:, first:first + width],
            preferred_element_type=F32,
        )
        sent[part, 0:256, 0:width] = block.astype(BF16)
        copy_of(part, 0).start()

    for i in range(4):
        at = slice(i * 256, (i + 1) * 256)
        back = lax.dot_general(
            grad[...], weight[at, :], (((1,), (1,)), ((), ())), preferred_element_type=F32
        )
        vec[0, :, at] = jnp.sum(back * normed[:, at], axis=0, keepdims=True)
    ones = jnp.ones((16, ROWS), BF16)
    vec[0, :, WIDTH:LOSS_AT] = jnp.dot(ones, grad[...], preferred_element_type=F32)[0:1, :]
    lane = lane_ids(1, 128)
    loss_here = jnp.sum(loss, axis=0, keepdims=True)
    vec[0, :, LOSS_AT:VEC] = jnp.where(lane == 0, loss_here, jnp.where(lane == 1, frames_here, 0.0))
    vec_copy(0).start()
    for part in range(PARTS):
        first, width = THIRDS[part % 3]
        stay = pl.multiple_of(mine[part] * 256, 256)
        acc[part, :, 0:width] = jnp.dot(
            lhs[part, pl.ds(stay, 256), :], grad[:, first:first + width],
            preferred_element_type=F32,
        )

    base = [0] * PARTS
    for stage in range(1, STAGES):
        rows = STAGE_ROWS[stage]
        before_at = STAGE_AT[stage - 1]
        arrived = got if stage - 1 < NARROW else got_wide
        for part in (0, 3, 1, 4, 2, 5):
            width = THIRDS[part % 3][1]
            bit = mine[(part + stage) % 6]
            away, stay = (1 - bit) * rows, bit * rows
            unit = min(rows, 16)

            def joined(offset):
                at = pl.multiple_of(base[part] + offset, unit)
                return acc[part, pl.ds(at, rows), 0:width] + arrived[
                    part, pl.ds(pl.multiple_of(before_at + offset, unit), rows), 0:width
                ].astype(F32)

            copy_of(part, stage - 1).wait_recv()
            block = joined(away)
            place_at = slice(STAGE_AT[stage], STAGE_AT[stage] + rows)
            if stage < NARROW:
                sent[part, place_at, 0:width] = block.astype(BF16)
            else:
                sent_wide[part, place_at, 0:width] = block
            copy_of(part, stage).start()
            acc[part, pl.ds(pl.multiple_of(base[part] + stay, unit), rows), 0:width] = joined(stay)
            base[part] = base[part] + stay
        vec_copy(stage - 1).wait_recv()
        vec[stage] = vec[stage - 1] + vec_in[stage - 1]
        vec_copy(stage).start()

    vec_copy(STAGES - 1).wait_recv()
    vec[STAGES] = vec[STAGES - 1] + vec_in[STAGES - 1]
    vec_copy(STAGES).start()
    inverse = 1.0 / vec[STAGES, :, LOSS_AT + 1:LOSS_AT + 2]
    for part in range(PARTS):
        first, width = THIRDS[part % 3]
        copy_of(part, STAGES - 1).wait_recv()
        at = pl.multiple_of(base[part], 8)
        final[part // 3, :, first:first + width] = (
            acc[part, pl.ds(at, 8), 0:width]
            + got_wide[part, STAGE_AT[-1]:STAGE_AT[-1] + 8, 0:width]
        ) * inverse

    swap = to_pair(final.at[1 - t], final_in, 2)
    swap.start()
    vec_copy(STAGES).wait_recv()
    total, beside = vec[STAGES], vec_in[STAGES]
    gain_out[...] = (total[:, 0:WIDTH] + beside[:, 0:WIDTH]) * inverse
    loss_out[...] = (total[:, LOSS_AT:VEC] + beside[:, LOSS_AT:VEC]) * inverse
    rest = VOCAB - HALF_V

    @pl.when(t == 0)
    def _():
        bias_out[:, 0:HALF_V] = total[:, WIDTH:LOSS_AT] * inverse
        bias_out[:, HALF_V:VOCAB] = beside[:, WIDTH:WIDTH + rest] * inverse
        weight_out[:, 0:HALF_V] = final[0]

    @pl.when(t == 1)
    def _():
        bias_out[:, 0:HALF_V] = beside[:, WIDTH:LOSS_AT] * inverse
        bias_out[:, HALF_V:VOCAB] = total[:, WIDTH:WIDTH + rest] * inverse
        weight_out[:, HALF_V:VOCAB] = final[1, :, 0:rest]

    swap.wait_recv()

    @pl.when(t == 0)
    def _():
        weight_out[:, HALF_V:VOCAB] = final_in[:, 0:rest]

    @pl.when(t == 1)
    def _():
        weight_out[:, 0:HALF_V] = final_in[...]

    hidden_swap.wait_send()
    stats_swap.wait_send()
    swap.wait_send()
    for copy in soft_copies:
        copy.wait_send()
    for part in range(PARTS):
        for stage in range(STAGES):
            copy_of(part, stage).wait_send()
    for stage in range(STAGES + 1):
        vec_copy(stage).wait_send()


def distill(teacher_logits, weight, tail, meta, arrived, bias, gain):
    vmem = pl.BlockSpec(memory_space=pltpu.VMEM)
    hbm = pl.BlockSpec(memory_space=pl.ANY)
    dma = pltpu.SemaphoreType.DMA
    return pl.pallas_call(
        step_kernel,
        out_shape=(
            jax.ShapeDtypeStruct((8, VOCAB), F32),
            jax.ShapeDtypeStruct((1, WIDTH), F32),
            jax.ShapeDtypeStruct((1, VOCAB), F32),
            jax.ShapeDtypeStruct((1, 128), F32),
        ),
        in_specs=[hbm, hbm] + [vmem] * 5,
        out_specs=(vmem,) * 4,
        scratch_shapes=[
            pltpu.VMEM((ROWS, VOCAB), BF16),
            pltpu.VMEM((ROWS, 2 * HALF_V), BF16),
            pltpu.VMEM((ROWS, HALF_V), BF16),
            pltpu.VMEM((WIDTH, HALF_V), BF16),
            pltpu.VMEM((ROWS, 128), F32),
            pltpu.VMEM((ROWS, 128), F32),
            pltpu.VMEM((ROWS, 128), F32),
            pltpu.VMEM((ROWS, WIDTH), BF16),
            pltpu.VMEM((ROWS, WIDTH), BF16),
            pltpu.VMEM((ROWS, WIDTH), F32),
            pltpu.VMEM((ROWS, WIDTH), BF16),
            pltpu.VMEM((WIDTH // 8, 8, ROWS), F32),
            pltpu.VMEM((ROWS, HALF_V), F32),
            pltpu.VMEM((ROWS, HALF_V), BF16),
            pltpu.VMEM((PARTS, 512, ROWS), BF16),
            pltpu.VMEM((PARTS, 256, WIDEST), F32),
            pltpu.VMEM((PARTS, NARROW_ROWS, WIDEST), BF16),
            pltpu.VMEM((PARTS, NARROW_ROWS, WIDEST), BF16),
            pltpu.VMEM((PARTS, WIDE_ROWS, WIDEST), F32),
            pltpu.VMEM((PARTS, WIDE_ROWS, WIDEST), F32),
            pltpu.VMEM((2, 8, HALF_V), F32),
            pltpu.VMEM((8, HALF_V), F32),
            pltpu.VMEM((STAGES + 1, 1, VEC), F32),
            pltpu.VMEM((STAGES + 1, 1, VEC), F32),
            dma((QUARTERS,)),
            dma((BLOCKS,)),
            dma((QUARTERS,)),
            dma((QUARTERS,)),
            dma((3,)),
            dma((3,)),
            dma((PARTS * STAGES,)),
            dma((PARTS * STAGES,)),
            dma((STAGES + 1,)),
            dma((STAGES + 1,)),
        ],
        compiler_params=pltpu.CompilerParams(
            collective_id=0, has_side_effects=True, vmem_limit_bytes=60 * 1024 * 1024
        ),
    )(teacher_logits, weight, tail, meta, arrived, bias, gain)


def body(
    teacher_logits, routes, agreement, targets, lengths, student_hidden, out_weight, out_bias, gain
):
    arrived = lax.all_to_all(student_hidden, DP, split_axis=0, concat_axis=0, tiled=True)
    meta = jnp.concatenate(
        [
            routes.reshape(1, ROWS),
            agreement[None],
            targets[None],
            jnp.broadcast_to(lengths[:, None], (1, ROWS)),
            jnp.zeros((4, ROWS), jnp.int32),
        ]
    ).astype(F32)
    tail = jnp.pad(out_weight[:, TAIL:], ((0, 0), (0, 2 * HALF_V - VOCAB)))
    bias = jnp.pad(out_bias, (0, 2 * HALF_V - VOCAB)).reshape(2, 1, HALF_V)
    weight_grad, gain_grad, bias_grad, loss = distill(
        teacher_logits, out_weight, tail, meta, arrived, bias, gain[None]
    )
    return (weight_grad, gain_grad[0], bias_grad[0], loss[0, 0])


def solution(mesh):
    finer = Mesh(
        mesh.devices.reshape(mesh.shape["teach"], 4, 4, 4), ("teach", "dp_0", "dp_1", "dp_2")
    )
    in_specs = (
        P("teach", DP, None),
        P(DP, None),
        P(DP),
        P(DP),
        P(DP),
        P(TEACH_DP, None),
        P(),
        P(),
        P(),
    )
    out_specs = (P(TEACH_DP, None), P(), P(), P())
    return jax.shard_map(body, mesh=finer, in_specs=in_specs, out_specs=out_specs, check_vma=False)
```

```python
import jax
import jax.numpy as jnp
from jax import lax
from jax.experimental import pallas as pl
from jax.experimental.pallas import tpu as pltpu
from jax.sharding import Mesh
from jax.sharding import PartitionSpec as P

DP = ("dp_0", "dp_1", "dp_2")
TEACH_DP = ("teach", "dp_0", "dp_1", "dp_2")
MESH = pl.DeviceIdType.MESH
F32 = jnp.float32
BF16 = jnp.bfloat16

EPSILON = 1e-05
VOCAB = 5000
WIDTH = 1024
ROWS = 256
STUDENTS = 128

HALF_V = 2560
BLOCK_V = 512
BLOCKS = 5
THIRDS = ((0, 896), (896, 896), (1792, 768))
WIDEST = 896
STAGE_ROWS = (256, 128, 64, 32, 16, 8)
STAGE_AT = (0, 256, 384, 0, 32, 48)
NARROW = 3
NARROW_ROWS = 448
WIDE_ROWS = 56
PARTS = 6
STAGES = 6
VEC = WIDTH + HALF_V + 128
LOSS_AT = WIDTH + HALF_V
STEP = 64
PIECES = 4
CHIPS = 64


def chunk_of(part, row):
    bits = [0] * 6
    for k in range(6):
        bits[(part + k) % 6] = (row >> (5 - k)) & 1
    chip = 0
    for dim in range(3):
        low, high = bits[dim], bits[3 + dim]
        chip = chip * 4 + high * 2 + (high ^ low)
    return chip


def rows_at(k, size=STEP):
    return pl.ds(pl.multiple_of(k * size, size), size)


def lane_ids(rows, width):
    return lax.broadcasted_iota(jnp.int32, (rows, width), 1)


def sublane_ids(rows, width):
    return lax.broadcasted_iota(jnp.int32, (rows, width), 0)


def folded(x, rows, op):
    groups = x.reshape(x.shape[0] // rows, rows, x.shape[1])
    total = groups[0]
    for k in range(1, groups.shape[0]):
        total = op(total, groups[k])
    return total


def step_kernel(
    teacher_hbm, weight_hbm, hidden_ref, routes_ref, agree_ref, target_ref, length_ref, bias_ref, gain_ref,
    weight_out, gain_out, bias_out, loss_out,
    teacher, soft, soft_in, weight, message, arrived, stats, stats_in, mine_h, their_h,
    bias_row, bias_t, normed, scaled, scaled_t, logits, grad, grad_n,
    lhs, acc, sent, got, sent_wide, got_wide, final, final_in, vec, vec_in,
    teacher_sem, weight_sem, hidden_send, hidden_recv, soft_send, soft_recv, pair_send, pair_recv,
    send_sem, recv_sem, vec_send_sem, vec_recv_sem,
):
    t = lax.axis_index("teach")
    place = [lax.axis_index(axis) for axis in DP]
    me = place[0] * 16 + place[1] * 4 + place[2]

    def partner(bit):
        ids = list(place)
        v = place[bit % 3]
        ids[bit % 3] = (3 - v) if bit >= 3 else (v + 1 - 2 * (v % 2))
        return (t, ids[0], ids[1], ids[2])

    def my_bit(bit):
        v = place[bit % 3]
        return v // 2 if bit >= 3 else (v // 2 + v % 2) % 2

    partners = [partner(bit) for bit in range(6)]
    mine = [my_bit(bit) for bit in range(6)]
    other_core = (1 - t, place[0], place[1], place[2])

    def moved(k, sign):
        step = (k * 21) % CHIPS
        steps = (step // 16, (step // 4) % 4, step % 4)
        return [(v + 4 + sign * s) % 4 for v, s in zip(place, steps)]

    def index_of(ids):
        return ids[0] * 16 + ids[1] * 4 + ids[2]

    barrier = pltpu.get_barrier_semaphore()
    pl.semaphore_signal(barrier, inc=1, device_id=other_core, device_id_type=MESH)

    def greet(k, carry):
        ids = moved(k, 1)
        pl.semaphore_signal(
            barrier, inc=1, device_id=(t, ids[0], ids[1], ids[2]), device_id_type=MESH
        )
        return carry

    lax.fori_loop(1, CHIPS, greet, 0)

    cuts = (0, 1280, 2560, 3840, VOCAB)
    teacher_copies = [
        pltpu.make_async_copy(
            teacher_hbm.at[cuts[q]:cuts[q + 1], :],
            teacher.at[cuts[q]:cuts[q + 1], :],
            teacher_sem.at[q],
        )
        for q in range(PIECES)
    ]
    for copy in teacher_copies:
        copy.start()
    weight_copies = [
        pltpu.make_async_copy(
            weight_hbm.at[pl.ds(pl.multiple_of(t * HALF_V + i * BLOCK_V, BLOCK_V), BLOCK_V), :],
            weight.at[i * BLOCK_V:(i + 1) * BLOCK_V, :],
            weight_sem.at[i],
        )
        for i in range(BLOCKS - 1)
    ]
    last_at = (BLOCKS - 1) * BLOCK_V
    rest = VOCAB - HALF_V
    last_first = pltpu.make_async_copy(
        weight_hbm.at[last_at:HALF_V, :],
        weight.at[last_at:HALF_V, :],
        weight_sem.at[BLOCKS - 1],
    )
    last_second = pltpu.make_async_copy(
        weight_hbm.at[HALF_V + last_at:VOCAB, :],
        weight.at[last_at:rest, :],
        weight_sem.at[BLOCKS - 1],
    )
    for copy in weight_copies:
        copy.start()

    @pl.when(t == 0)
    def _():
        last_first.start()

    @pl.when(t == 1)
    def _():
        last_second.start()
        weight[rest:HALF_V, :] = jnp.zeros((HALF_V - rest, WIDTH), BF16)

    low = sublane_ids(8, 512) < 4

    def pack(k, carry):
        x = hidden_ref[pl.ds(pl.multiple_of(k * 16, 16), 16), :].astype(F32)
        for i in range(2):
            left, right = x[8 * i:8 * i + 8, 0:512], x[8 * i:8 * i + 8, 512:1024]
            message[4 * k + 2 * i] = jnp.where(low, left, pltpu.roll(right, 4, 0)).astype(BF16)
            message[4 * k + 2 * i + 1] = jnp.where(low, pltpu.roll(left, 4, 0), right).astype(BF16)
        return carry

    lax.fori_loop(0, ROWS // 16, pack, 0)
    arrived[me] = message[me]

    routes_row = routes_ref[...].astype(F32)
    live = (lane_ids(1, ROWS) < length_ref[...]).astype(F32)
    half_live = live * 0.5
    weight_row = half_live * agree_ref[...].astype(F32)
    frames_here = jnp.sum(live, axis=1, keepdims=True)
    named = (routes_row == sublane_ids(STUDENTS, ROWS).astype(F32)).astype(F32)
    earlier = (sublane_ids(ROWS, ROWS) < lane_ids(ROWS, ROWS)).astype(F32)
    before = jnp.dot(named.astype(BF16), earlier.astype(BF16), preferred_element_type=F32)
    slot = jnp.sum(before * named, axis=0, keepdims=True)
    wanted = (routes_row - (t * CHIPS).astype(F32)) * 8.0 + slot
    wanted = jnp.transpose(jnp.broadcast_to(wanted, (8, ROWS)))[:, 0:1]

    teacher[VOCAB:2 * HALF_V, :] = jnp.full((2 * HALF_V - VOCAB, ROWS), -1e30, BF16)

    def max_step(k, top):
        return jnp.maximum(top, folded(teacher[rows_at(k), :], 16, jnp.maximum))

    top = jnp.full((16, ROWS), -1e30, BF16)
    for q in range(PIECES):
        teacher_copies[q].wait()
        last = cuts[q + 1] // STEP if q < PIECES - 1 else 2 * HALF_V // STEP
        top = lax.fori_loop(cuts[q] // STEP, last, max_step, top, unroll=2)
    top = jnp.max(top.astype(F32), axis=0, keepdims=True)

    def sum_step(k, total):
        return total + folded(jnp.exp(teacher[rows_at(k), :].astype(F32) - top), 8, jnp.add)

    total = lax.fori_loop(0, 2 * HALF_V // STEP, sum_step, jnp.zeros((8, ROWS), F32), unroll=2)
    scale_row = weight_row / jnp.sum(total, axis=0, keepdims=True)

    pl.semaphore_wait(barrier, CHIPS)

    def hidden_copy(k, receiving):
        ids = moved(k, 1)
        source = index_of(moved(k, -1)) if receiving else me
        return pltpu.make_async_remote_copy(
            src_ref=message.at[index_of(ids)],
            dst_ref=arrived.at[source],
            send_sem=hidden_send.at[k],
            recv_sem=hidden_recv.at[k],
            device_id=(t, ids[0], ids[1], ids[2]),
            device_id_type=MESH,
        )

    def send_hidden(k, carry):
        hidden_copy(k, False).start()
        return carry

    lax.fori_loop(1, CHIPS, send_hidden, 0)

    target_row = target_ref[...]
    step_rows = sublane_ids(STEP, ROWS)

    def soft_step(k, mass):
        rows = rows_at(k)
        e = jnp.exp(teacher[rows, :].astype(F32) - top)
        hit = step_rows == target_row - k * STEP
        s = (e * scale_row + jnp.where(hit, half_live, 0.0)).astype(BF16)
        soft[rows, :] = s
        return mass + folded(s.astype(F32), 8, jnp.add)

    piece = HALF_V // PIECES
    soft_copies = [
        pltpu.make_async_remote_copy(
            src_ref=soft.at[pl.ds(pl.multiple_of((1 - t) * HALF_V + q * piece, 64), piece), :],
            dst_ref=soft_in.at[q * piece:(q + 1) * piece, :],
            send_sem=soft_send.at[q],
            recv_sem=soft_recv.at[q],
            device_id=other_core,
            device_id_type=MESH,
        )
        for q in range(PIECES)
    ]
    mass = jnp.zeros((8, ROWS), F32)
    for q in range(PIECES):
        first = (1 - t) * (HALF_V // STEP) + q * (piece // STEP)
        mass = lax.fori_loop(first, first + piece // STEP, soft_step, mass)
        soft_copies[q].start()
    first = t * (HALF_V // STEP)
    mass = lax.fori_loop(first, first + HALF_V // STEP, soft_step, mass)
    mass = jnp.sum(mass, axis=0, keepdims=True)

    bias_row[:, 0:VOCAB] = bias_ref[...]
    bias_row[:, VOCAB:2 * HALF_V] = jnp.zeros((1, 2 * HALF_V - VOCAB), F32)

    def bias_step(k, carry):
        strip = bias_row[:, pl.ds(pl.multiple_of(t * HALF_V + k * 128, 128), 128)]
        bias_t[rows_at(k, 128), :] = jnp.transpose(jnp.broadcast_to(strip, (128, 128)))
        return carry

    lax.fori_loop(0, HALF_V // 128, bias_step, 0)

    def wait_hidden(k, carry):
        hidden_copy(k, True).wait_recv()
        return carry

    lax.fori_loop(1, CHIPS, wait_hidden, 0)
    rows_in = arrived[...].reshape(CHIPS * 8, 512)
    for i in range(2):
        pick = (wanted + 4.0 * i == lane_ids(ROWS, CHIPS * 8).astype(F32)).astype(F32).astype(BF16)
        mine_h[:, 512 * i:512 * i + 512] = jnp.dot(
            pick, rows_in, preferred_element_type=F32
        ).astype(BF16)

    def to_pair(source, target, index):
        return pltpu.make_async_remote_copy(
            src_ref=source,
            dst_ref=target,
            send_sem=pair_send.at[index],
            recv_sem=pair_recv.at[index],
            device_id=other_core,
            device_id_type=MESH,
        )

    hidden_swap = to_pair(mine_h, their_h, 0)
    hidden_swap.start()

    hidden_swap.wait_recv()
    states = mine_h[...].astype(F32) + their_h[...].astype(F32)
    states = states - jnp.mean(states, axis=1, keepdims=True)
    spread = jnp.mean(jnp.square(states), axis=1, keepdims=True)
    states = states * lax.rsqrt(spread + EPSILON)
    normed[...] = states
    turned = jnp.transpose((states * gain_ref[...]).astype(BF16).astype(F32))
    scaled_t[...] = turned.reshape(WIDTH // 8, 8, ROWS)
    scaled[...] = turned.astype(BF16)

    peak = jnp.full((8, ROWS), -1e30, F32)
    for i in range(BLOCKS):
        if i < BLOCKS - 1:
            weight_copies[i].wait()
        else:
            @pl.when(t == 0)
            def _():
                last_first.wait()

            @pl.when(t == 1)
            def _():
                last_second.wait()
        at = slice(i * BLOCK_V, (i + 1) * BLOCK_V)
        slope = bias_t[at, :]
        block = jnp.dot(weight[at, :], scaled[...], preferred_element_type=F32)
        block = block + jnp.concatenate([slope, slope], axis=1)
        if i == BLOCKS - 1:
            inside = sublane_ids(BLOCK_V, ROWS) < VOCAB - i * BLOCK_V - t * HALF_V
            block = jnp.where(inside, block, -1e30)
        logits[at, :] = block
        peak = jnp.maximum(peak, folded(block, 8, jnp.maximum))
    peak = jnp.max(peak, axis=0, keepdims=True)

    def lse_step(k, total):
        return total + folded(jnp.exp(logits[rows_at(k), :] - peak), 8, jnp.add)

    total = lax.fori_loop(0, HALF_V // STEP, lse_step, jnp.zeros((8, ROWS), F32), unroll=2)
    lse = peak + jnp.log(jnp.sum(total, axis=0, keepdims=True))
    stats[...] = jnp.concatenate([lse, mass, jnp.zeros((6, ROWS), F32)], axis=0)
    stats_swap = to_pair(stats, stats_in, 1)
    stats_swap.start()

    for part in range(PARTS):
        half = part // 3
        for row in range(0, 64, 2):
            pair = jnp.concatenate(
                [scaled_t[half * 64 + chunk_of(part, row)], scaled_t[half * 64 + chunk_of(part, row + 1)]],
                axis=0,
            )
            lhs[part, row * 8:row * 8 + 16, :] = pair.astype(BF16)

    for copy in soft_copies:
        copy.wait_recv()
    stats_swap.wait_recv()
    there = stats_in[...]
    other_lse = there[0:1, :]
    highest = jnp.maximum(lse, other_lse)
    lse = highest + jnp.log(jnp.exp(lse - highest) + jnp.exp(other_lse - highest))
    mass = mass + there[1:2, :]

    def grad_step(k, loss):
        rows = rows_at(k)
        log_probs = logits[rows, :] - lse
        own = pl.ds(pl.multiple_of(t * HALF_V + k * STEP, STEP), STEP)
        both = soft[own, :].astype(F32) + soft_in[rows, :].astype(F32)
        grad[rows, :] = (mass * jnp.exp(log_probs) - both).astype(BF16)
        return loss - folded(both * log_probs, 8, jnp.add)

    def copy_of(part, stage):
        width = THIRDS[part % 3][1]
        rows = slice(STAGE_AT[stage], STAGE_AT[stage] + STAGE_ROWS[stage])
        source, target = (sent, got) if stage < NARROW else (sent_wide, got_wide)
        return pltpu.make_async_remote_copy(
            src_ref=source.at[part, rows, 0:width],
            dst_ref=target.at[part, rows, 0:width],
            send_sem=send_sem.at[part * STAGES + stage],
            recv_sem=recv_sem.at[part * STAGES + stage],
            device_id=partners[(part + stage) % 6],
            device_id_type=MESH,
        )

    def vec_copy(stage):
        return pltpu.make_async_remote_copy(
            src_ref=vec.at[stage],
            dst_ref=vec_in.at[stage],
            send_sem=vec_send_sem.at[stage],
            recv_sem=vec_recv_sem.at[stage],
            device_id=partners[stage] if stage < STAGES else other_core,
            device_id_type=MESH,
        )

    def product(part, at):
        first, width = THIRDS[part % 3]
        return lax.dot_general(
            lhs[part, pl.ds(pl.multiple_of(at, 256), 256), :], grad[first:first + width, :],
            (((1,), (1,)), ((), ())), preferred_element_type=F32,
        )

    loss = jnp.zeros((8, ROWS), F32)
    for third in range(3):
        first, width = THIRDS[third]
        loss = lax.fori_loop(first // STEP, (first + width) // STEP, grad_step, loss)
        for part in (third, third + 3):
            sent[part, 0:256, 0:width] = product(part, (1 - mine[part]) * 256).astype(BF16)
            copy_of(part, 0).start()

    for part in range(PARTS):
        acc[part, :, 0:THIRDS[part % 3][1]] = product(part, mine[part] * 256)
    for i in range(BLOCKS):
        at = slice(i * BLOCK_V, (i + 1) * BLOCK_V)
        grad_n[:, at] = jnp.transpose(grad[at, :].astype(F32)).astype(BF16)
    for i in range(4):
        at = slice(i * 256, (i + 1) * 256)
        back = jnp.dot(grad_n[...], weight[:, at], preferred_element_type=F32)
        vec[0, :, at] = jnp.sum(back * normed[:, at], axis=0, keepdims=True)
    ones = jnp.ones((16, ROWS), BF16)
    vec[0, :, WIDTH:LOSS_AT] = jnp.dot(ones, grad_n[...], preferred_element_type=F32)[0:1, :]
    lane = lane_ids(1, 128)
    loss_here = jnp.sum(jnp.sum(loss, axis=0, keepdims=True), axis=1, keepdims=True)
    vec[0, :, LOSS_AT:VEC] = jnp.where(lane == 0, loss_here, jnp.where(lane == 1, frames_here, 0.0))
    vec_copy(0).start()

    base = [0] * PARTS
    for stage in range(1, STAGES):
        rows = STAGE_ROWS[stage]
        before_at = STAGE_AT[stage - 1]
        incoming = got if stage - 1 < NARROW else got_wide
        for part in (0, 3, 1, 4, 2, 5):
            width = THIRDS[part % 3][1]
            bit = mine[(part + stage) % 6]
            away, stay = (1 - bit) * rows, bit * rows
            unit = min(rows, 16)

            def joined(offset):
                at = pl.multiple_of(base[part] + offset, unit)
                return acc[part, pl.ds(at, rows), 0:width] + incoming[
                    part, pl.ds(pl.multiple_of(before_at + offset, unit), rows), 0:width
                ].astype(F32)

            copy_of(part, stage - 1).wait_recv()
            block = joined(away)
            place_at = slice(STAGE_AT[stage], STAGE_AT[stage] + rows)
            if stage < NARROW:
                sent[part, place_at, 0:width] = block.astype(BF16)
            else:
                sent_wide[part, place_at, 0:width] = block
            copy_of(part, stage).start()
            acc[part, pl.ds(pl.multiple_of(base[part] + stay, unit), rows), 0:width] = joined(stay)
            base[part] = base[part] + stay
        vec_copy(stage - 1).wait_recv()
        vec[stage] = vec[stage - 1] + vec_in[stage - 1]
        vec_copy(stage).start()

    vec_copy(STAGES - 1).wait_recv()
    vec[STAGES] = vec[STAGES - 1] + vec_in[STAGES - 1]
    vec_copy(STAGES).start()
    inverse = 1.0 / vec[STAGES, :, LOSS_AT + 1:LOSS_AT + 2]
    for part in range(PARTS):
        first, width = THIRDS[part % 3]
        copy_of(part, STAGES - 1).wait_recv()
        at = pl.multiple_of(base[part], 8)
        final[part // 3, :, first:first + width] = (
            acc[part, pl.ds(at, 8), 0:width]
            + got_wide[part, STAGE_AT[-1]:STAGE_AT[-1] + 8, 0:width]
        ) * inverse

    swap = to_pair(final.at[1 - t], final_in, 2)
    swap.start()
    vec_copy(STAGES).wait_recv()
    total, beside = vec[STAGES], vec_in[STAGES]
    gain_out[...] = (total[:, 0:WIDTH] + beside[:, 0:WIDTH]) * inverse
    loss_out[...] = (total[:, LOSS_AT:VEC] + beside[:, LOSS_AT:VEC]) * inverse

    @pl.when(t == 0)
    def _():
        bias_out[:, 0:HALF_V] = total[:, WIDTH:LOSS_AT] * inverse
        bias_out[:, HALF_V:VOCAB] = beside[:, WIDTH:WIDTH + rest] * inverse
        weight_out[:, 0:HALF_V] = final[0]

    @pl.when(t == 1)
    def _():
        bias_out[:, 0:HALF_V] = beside[:, WIDTH:LOSS_AT] * inverse
        bias_out[:, HALF_V:VOCAB] = total[:, WIDTH:WIDTH + rest] * inverse
        weight_out[:, HALF_V:VOCAB] = final[1, :, 0:rest]

    swap.wait_recv()

    @pl.when(t == 0)
    def _():
        weight_out[:, HALF_V:VOCAB] = final_in[:, 0:rest]

    @pl.when(t == 1)
    def _():
        weight_out[:, 0:HALF_V] = final_in[...]

    def sent_hidden(k, carry):
        hidden_copy(k, False).wait_send()
        return carry

    lax.fori_loop(1, CHIPS, sent_hidden, 0)
    hidden_swap.wait_send()
    stats_swap.wait_send()
    swap.wait_send()
    for copy in soft_copies:
        copy.wait_send()
    for part in range(PARTS):
        for stage in range(STAGES):
            copy_of(part, stage).wait_send()
    for stage in range(STAGES + 1):
        vec_copy(stage).wait_send()


def distill(teacher, weight, *small):
    vmem = pl.BlockSpec(memory_space=pltpu.VMEM)
    hbm = pl.BlockSpec(memory_space=pl.ANY)
    dma = pltpu.SemaphoreType.DMA
    return pl.pallas_call(
        step_kernel,
        out_shape=(
            jax.ShapeDtypeStruct((8, VOCAB), F32),
            jax.ShapeDtypeStruct((1, WIDTH), F32),
            jax.ShapeDtypeStruct((1, VOCAB), F32),
            jax.ShapeDtypeStruct((1, 128), F32),
        ),
        in_specs=[hbm, hbm] + [vmem] * len(small),
        out_specs=(vmem,) * 4,
        scratch_shapes=[
            pltpu.VMEM((2 * HALF_V, ROWS), BF16),
            pltpu.VMEM((2 * HALF_V, ROWS), BF16),
            pltpu.VMEM((HALF_V, ROWS), BF16),
            pltpu.VMEM((HALF_V, WIDTH), BF16),
            pltpu.VMEM((CHIPS, 8, 512), BF16),
            pltpu.VMEM((CHIPS, 8, 512), BF16),
            pltpu.VMEM((8, ROWS), F32),
            pltpu.VMEM((8, ROWS), F32),
            pltpu.VMEM((ROWS, WIDTH), BF16),
            pltpu.VMEM((ROWS, WIDTH), BF16),
            pltpu.VMEM((1, 2 * HALF_V), F32),
            pltpu.VMEM((HALF_V, 128), F32),
            pltpu.VMEM((ROWS, WIDTH), F32),
            pltpu.VMEM((WIDTH, ROWS), BF16),
            pltpu.VMEM((WIDTH // 8, 8, ROWS), F32),
            pltpu.VMEM((HALF_V, ROWS), F32),
            pltpu.VMEM((HALF_V, ROWS), BF16),
            pltpu.VMEM((ROWS, HALF_V), BF16),
            pltpu.VMEM((PARTS, 512, ROWS), BF16),
            pltpu.VMEM((PARTS, 256, WIDEST), F32),
            pltpu.VMEM((PARTS, NARROW_ROWS, WIDEST), BF16),
            pltpu.VMEM((PARTS, NARROW_ROWS, WIDEST), BF16),
            pltpu.VMEM((PARTS, WIDE_ROWS, WIDEST), F32),
            pltpu.VMEM((PARTS, WIDE_ROWS, WIDEST), F32),
            pltpu.VMEM((2, 8, HALF_V), F32),
            pltpu.VMEM((8, HALF_V), F32),
            pltpu.VMEM((STAGES + 1, 1, VEC), F32),
            pltpu.VMEM((STAGES + 1, 1, VEC), F32),
            dma((PIECES,)),
            dma((BLOCKS,)),
            dma((CHIPS,)),
            dma((CHIPS,)),
            dma((PIECES,)),
            dma((PIECES,)),
            dma((3,)),
            dma((3,)),
            dma((PARTS * STAGES,)),
            dma((PARTS * STAGES,)),
            dma((STAGES + 1,)),
            dma((STAGES + 1,)),
        ],
        compiler_params=pltpu.CompilerParams(
            collective_id=0, has_side_effects=True, vmem_limit_bytes=60 * 1024 * 1024
        ),
    )(teacher, weight, *small)


def body(
    teacher_logits, routes, agreement, targets, lengths, student_hidden, out_weight, out_bias, gain
):
    weight_grad, gain_grad, bias_grad, loss = distill(
        teacher_logits[0].T,
        out_weight.T,
        student_hidden,
        routes.reshape(1, ROWS),
        agreement[None],
        targets[None],
        lengths[None],
        out_bias[None],
        gain[None],
    )
    return (weight_grad, gain_grad[0], bias_grad[0], loss[0, 0])


def solution(mesh):
    finer = Mesh(
        mesh.devices.reshape(mesh.shape["teach"], 4, 4, 4), ("teach", "dp_0", "dp_1", "dp_2")
    )
    in_specs = (
        P("teach", DP, None),
        P(DP, None),
        P(DP),
        P(DP),
        P(DP),
        P(TEACH_DP, None),
        P(),
        P(),
        P(),
    )
    out_specs = (P(TEACH_DP, None), P(), P(), P())
    return jax.shard_map(body, mesh=finer, in_specs=in_specs, out_specs=out_specs, check_vma=False)
```

```python
import jax
import jax.numpy as jnp
from jax import lax
from jax.experimental import pallas as pl
from jax.experimental.pallas import tpu as pltpu
from jax.sharding import Mesh
from jax.sharding import PartitionSpec as P

DP = ("dp_0", "dp_1", "dp_2")
TEACH_DP = ("teach", "dp_0", "dp_1", "dp_2")
MESH = pl.DeviceIdType.MESH
F32 = jnp.float32
BF16 = jnp.bfloat16

EPSILON = 1e-05
VOCAB = 5000
WIDTH = 1024
ROWS = 256
STUDENTS = 128

HALF_V = 2560
BLOCK_V = 512
BLOCKS = 5
THIRDS = ((0, 896), (896, 896), (1792, 768))
WIDEST = 896
CHUNKS = (((0, 512), (512, 384)), ((0, 512), (512, 384)), ((0, 384), (384, 384)))
STAGE_ROWS = (256, 128, 64, 32)
STAGE_AT = (0, 256, 384, 0)
NARROW = 3
NARROW_ROWS = 448
WIDE_ROWS = 56
LAST_AT = 32
FLIPS = ((1, 0), (0, 1), (1, 1))
PARTS = 6
STAGES = 4
COPIES = 7
ORDER = (0, 3, 1, 4, 2, 5)
BITS = 6
VEC = WIDTH + HALF_V + 128
LOSS_AT = WIDTH + HALF_V
STEP = 64
PIECES = 4
CHIPS = 64


def chunk_of(part, row):
    bits = [0] * 6
    for k in range(6):
        bits[(part + k) % 6] = (row >> (5 - k)) & 1
    chip = 0
    for dim in range(3):
        low, high = bits[dim], bits[3 + dim]
        chip = chip * 4 + high * 2 + (high ^ low)
    return chip


def rows_at(k, size=STEP):
    return pl.ds(pl.multiple_of(k * size, size), size)


def lane_ids(rows, width):
    return lax.broadcasted_iota(jnp.int32, (rows, width), 1)


def sublane_ids(rows, width):
    return lax.broadcasted_iota(jnp.int32, (rows, width), 0)


def folded(x, rows, op):
    groups = x.reshape(x.shape[0] // rows, rows, x.shape[1])
    total = groups[0]
    for k in range(1, groups.shape[0]):
        total = op(total, groups[k])
    return total


def step_kernel(
    teacher_hbm, weight_hbm, hidden_ref, routes_ref, agree_ref, target_ref, length_ref, bias_ref, gain_ref,
    weight_out, gain_out, bias_out, loss_out,
    teacher, soft, soft_in, weight, message, arrived, stats, stats_in, mine_h, their_h,
    bias_row, bias_t, normed, scaled, scaled_t, logits, grad, grad_n,
    lhs, acc, sent, got, sent_wide, got_wide, final, final_in, vec, vec_in,
    teacher_sem, weight_sem, hidden_send, hidden_recv, soft_send, soft_recv, pair_send, pair_recv,
    send_sem, recv_sem, vec_send_sem, vec_recv_sem,
):
    t = lax.axis_index("teach")
    place = [lax.axis_index(axis) for axis in DP]
    me = place[0] * 16 + place[1] * 4 + place[2]

    def partner(*bits):
        ids = list(place)
        for bit in bits:
            v = place[bit % 3]
            ids[bit % 3] = (3 - v) if bit >= 3 else (v + 1 - 2 * (v % 2))
        return (t, ids[0], ids[1], ids[2])

    def my_bit(bit):
        v = place[bit % 3]
        return v // 2 if bit >= 3 else (v // 2 + v % 2) % 2

    partners = [partner(bit) for bit in range(6)]
    mine = [my_bit(bit) for bit in range(6)]
    other_core = (1 - t, place[0], place[1], place[2])

    turned_by = [[(v + d) % 4 for d in range(4)] for v in place]

    def moved(k, sign):
        step = (k * 21) % CHIPS
        steps = (step // 16, (step // 4) % 4, step % 4)
        return [turned_by[axis][(sign * d) % 4] for axis, d in enumerate(steps)]

    def index_of(ids):
        return ids[0] * 16 + ids[1] * 4 + ids[2]

    barrier = pltpu.get_barrier_semaphore()
    for k in range(1, CHIPS):
        ids = moved(k, 1)
        pl.semaphore_signal(
            barrier, inc=1, device_id=(t, ids[0], ids[1], ids[2]), device_id_type=MESH
        )
    pl.semaphore_signal(barrier, inc=1, device_id=other_core, device_id_type=MESH)

    cuts = (0, 1280, 2560, 3840, VOCAB)
    teacher_copies = [
        pltpu.make_async_copy(
            teacher_hbm.at[cuts[q]:cuts[q + 1], :],
            teacher.at[cuts[q]:cuts[q + 1], :],
            teacher_sem.at[q],
        )
        for q in range(PIECES)
    ]
    for copy in teacher_copies:
        copy.start()
    weight_copies = [
        pltpu.make_async_copy(
            weight_hbm.at[pl.ds(pl.multiple_of(t * HALF_V + i * BLOCK_V, BLOCK_V), BLOCK_V), :],
            weight.at[i * BLOCK_V:(i + 1) * BLOCK_V, :],
            weight_sem.at[i],
        )
        for i in range(BLOCKS - 1)
    ]
    last_at = (BLOCKS - 1) * BLOCK_V
    rest = VOCAB - HALF_V
    last_first = pltpu.make_async_copy(
        weight_hbm.at[last_at:HALF_V, :],
        weight.at[last_at:HALF_V, :],
        weight_sem.at[BLOCKS - 1],
    )
    last_second = pltpu.make_async_copy(
        weight_hbm.at[HALF_V + last_at:VOCAB, :],
        weight.at[last_at:rest, :],
        weight_sem.at[BLOCKS - 1],
    )
    for copy in weight_copies:
        copy.start()

    @pl.when(t == 0)
    def _():
        last_first.start()

    @pl.when(t == 1)
    def _():
        last_second.start()
        weight[rest:HALF_V, :] = jnp.zeros((HALF_V - rest, WIDTH), BF16)

    low = sublane_ids(8, 512) < 4

    def pack(k, carry):
        x = hidden_ref[pl.ds(pl.multiple_of(k * 16, 16), 16), :].astype(F32)
        for i in range(2):
            left, right = x[8 * i:8 * i + 8, 0:512], x[8 * i:8 * i + 8, 512:1024]
            message[4 * k + 2 * i] = jnp.where(low, left, pltpu.roll(right, 4, 0)).astype(BF16)
            message[4 * k + 2 * i + 1] = jnp.where(low, pltpu.roll(left, 4, 0), right).astype(BF16)
        return carry

    lax.fori_loop(0, ROWS // 16, pack, 0)
    arrived[me] = message[me]

    pl.semaphore_wait(barrier, CHIPS)

    def hidden_copy(k, receiving):
        ids = moved(k, 1)
        source = index_of(moved(k, -1)) if receiving else me
        return pltpu.make_async_remote_copy(
            src_ref=message.at[index_of(ids)],
            dst_ref=arrived.at[source],
            send_sem=hidden_send.at[k],
            recv_sem=hidden_recv.at[k],
            device_id=(t, ids[0], ids[1], ids[2]),
            device_id_type=MESH,
        )

    for k in range(1, CHIPS):
        hidden_copy(k, False).start()

    routes_row = routes_ref[...].astype(F32)
    live = (lane_ids(1, ROWS) < length_ref[...]).astype(F32)
    half_live = live * 0.5
    weight_row = half_live * agree_ref[...].astype(F32)
    frames_here = jnp.sum(live, axis=1, keepdims=True)
    named = (routes_row == sublane_ids(STUDENTS, ROWS).astype(F32)).astype(F32)
    earlier = (sublane_ids(ROWS, ROWS) < lane_ids(ROWS, ROWS)).astype(F32)
    before = jnp.dot(named.astype(BF16), earlier.astype(BF16), preferred_element_type=F32)
    slot = jnp.sum(before * named, axis=0, keepdims=True)
    wanted = (routes_row - (t * CHIPS).astype(F32)) * 8.0 + slot
    wanted = jnp.transpose(jnp.broadcast_to(wanted, (8, ROWS)))[:, 0:1]

    teacher[VOCAB:2 * HALF_V, :] = jnp.full((2 * HALF_V - VOCAB, ROWS), -1e30, BF16)

    def max_step(k, top):
        return jnp.maximum(top, folded(teacher[rows_at(k), :], 16, jnp.maximum))

    top = jnp.full((16, ROWS), -1e30, BF16)
    for q in range(PIECES):
        teacher_copies[q].wait()
        last = cuts[q + 1] // STEP if q < PIECES - 1 else 2 * HALF_V // STEP
        top = lax.fori_loop(cuts[q] // STEP, last, max_step, top, unroll=2)
    top = jnp.max(top.astype(F32), axis=0, keepdims=True)

    def sum_step(k, total):
        return total + folded(jnp.exp(teacher[rows_at(k), :].astype(F32) - top), 8, jnp.add)

    total = lax.fori_loop(0, 2 * HALF_V // STEP, sum_step, jnp.zeros((8, ROWS), F32), unroll=2)
    scale_row = weight_row / jnp.sum(total, axis=0, keepdims=True)

    target_row = target_ref[...]
    step_rows = sublane_ids(STEP, ROWS)

    def soft_step(k, mass):
        rows = rows_at(k)
        e = jnp.exp(teacher[rows, :].astype(F32) - top)
        hit = step_rows == target_row - k * STEP
        s = (e * scale_row + jnp.where(hit, half_live, 0.0)).astype(BF16)
        soft[rows, :] = s
        return mass + folded(s.astype(F32), 8, jnp.add)

    piece = HALF_V // PIECES
    soft_copies = [
        pltpu.make_async_remote_copy(
            src_ref=soft.at[pl.ds(pl.multiple_of((1 - t) * HALF_V + q * piece, 64), piece), :],
            dst_ref=soft_in.at[q * piece:(q + 1) * piece, :],
            send_sem=soft_send.at[q],
            recv_sem=soft_recv.at[q],
            device_id=other_core,
            device_id_type=MESH,
        )
        for q in range(PIECES)
    ]
    mass = jnp.zeros((8, ROWS), F32)
    for q in range(PIECES):
        first = (1 - t) * (HALF_V // STEP) + q * (piece // STEP)
        mass = lax.fori_loop(first, first + piece // STEP, soft_step, mass)
        soft_copies[q].start()
    first = t * (HALF_V // STEP)
    mass = lax.fori_loop(first, first + HALF_V // STEP, soft_step, mass)
    mass = jnp.sum(mass, axis=0, keepdims=True)

    bias_row[:, 0:VOCAB] = bias_ref[...]
    bias_row[:, VOCAB:2 * HALF_V] = jnp.zeros((1, 2 * HALF_V - VOCAB), F32)

    def bias_step(k, carry):
        strip = bias_row[:, pl.ds(pl.multiple_of(t * HALF_V + k * 128, 128), 128)]
        bias_t[rows_at(k, 128), :] = jnp.transpose(jnp.broadcast_to(strip, (128, 128)))
        return carry

    lax.fori_loop(0, HALF_V // 128, bias_step, 0)

    for k in range(1, CHIPS):
        hidden_copy(k, True).wait_recv()
    rows_in = arrived[...].reshape(CHIPS * 8, 512)
    for i in range(2):
        pick = (wanted + 4.0 * i == lane_ids(ROWS, CHIPS * 8).astype(F32)).astype(F32).astype(BF16)
        mine_h[:, 512 * i:512 * i + 512] = jnp.dot(
            pick, rows_in, preferred_element_type=F32
        ).astype(BF16)

    def to_pair(source, target, index):
        return pltpu.make_async_remote_copy(
            src_ref=source,
            dst_ref=target,
            send_sem=pair_send.at[index],
            recv_sem=pair_recv.at[index],
            device_id=other_core,
            device_id_type=MESH,
        )

    hidden_swap = to_pair(mine_h, their_h, 0)
    hidden_swap.start()

    hidden_swap.wait_recv()
    states = mine_h[...].astype(F32) + their_h[...].astype(F32)
    states = states - jnp.mean(states, axis=1, keepdims=True)
    spread = jnp.mean(jnp.square(states), axis=1, keepdims=True)
    states = states * lax.rsqrt(spread + EPSILON)
    normed[...] = states
    turned = jnp.transpose((states * gain_ref[...]).astype(BF16).astype(F32))
    scaled_t[...] = turned.reshape(WIDTH // 8, 8, ROWS)
    scaled[...] = turned.astype(BF16)

    peak = jnp.full((8, ROWS), -1e30, F32)
    for i in range(BLOCKS):
        if i < BLOCKS - 1:
            weight_copies[i].wait()
        else:
            @pl.when(t == 0)
            def _():
                last_first.wait()

            @pl.when(t == 1)
            def _():
                last_second.wait()
        at = slice(i * BLOCK_V, (i + 1) * BLOCK_V)
        slope = bias_t[at, :]
        block = jnp.dot(weight[at, :], scaled[...], preferred_element_type=F32)
        block = block + jnp.concatenate([slope, slope], axis=1)
        if i == BLOCKS - 1:
            inside = sublane_ids(BLOCK_V, ROWS) < VOCAB - i * BLOCK_V - t * HALF_V
            block = jnp.where(inside, block, -1e30)
        logits[at, :] = block
        peak = jnp.maximum(peak, folded(block, 8, jnp.maximum))
    peak = jnp.max(peak, axis=0, keepdims=True)

    def lse_step(k, total):
        return total + folded(jnp.exp(logits[rows_at(k), :] - peak), 8, jnp.add)

    total = lax.fori_loop(0, HALF_V // STEP, lse_step, jnp.zeros((8, ROWS), F32), unroll=2)
    lse = peak + jnp.log(jnp.sum(total, axis=0, keepdims=True))
    stats[...] = jnp.concatenate([lse, mass, jnp.zeros((6, ROWS), F32)], axis=0)
    stats_swap = to_pair(stats, stats_in, 1)
    stats_swap.start()

    for part in range(PARTS):
        half = part // 3
        for row in range(0, 64, 2):
            pair = jnp.concatenate(
                [scaled_t[half * 64 + chunk_of(part, row)], scaled_t[half * 64 + chunk_of(part, row + 1)]],
                axis=0,
            )
            lhs[part, row * 8:row * 8 + 16, :] = pair.astype(BF16)

    for copy in soft_copies:
        copy.wait_recv()
    stats_swap.wait_recv()
    there = stats_in[...]
    other_lse = there[0:1, :]
    highest = jnp.maximum(lse, other_lse)
    lse = highest + jnp.log(jnp.exp(lse - highest) + jnp.exp(other_lse - highest))
    mass = mass + there[1:2, :]

    def grad_step(k, loss):
        rows = rows_at(k)
        log_probs = logits[rows, :] - lse
        own = pl.ds(pl.multiple_of(t * HALF_V + k * STEP, STEP), STEP)
        both = soft[own, :].astype(F32) + soft_in[rows, :].astype(F32)
        grad[rows, :] = (mass * jnp.exp(log_probs) - both).astype(BF16)
        return loss - folded(both * log_probs, 8, jnp.add)

    def columns(part, chunk):
        first, width = CHUNKS[part % 3][chunk]
        return slice(first, first + width)

    def grad_columns(part, chunk):
        first = THIRDS[part % 3][0]
        at = columns(part, chunk)
        return slice(first + at.start, first + at.stop)

    def remote(part, chunk, source, target, rows, index, device):
        at = columns(part, chunk)
        number = (part * 2 + chunk) * COPIES + index
        return pltpu.make_async_remote_copy(
            src_ref=source.at[part, rows, at],
            dst_ref=target.at[part, rows, at],
            send_sem=send_sem.at[number],
            recv_sem=recv_sem.at[number],
            device_id=device,
            device_id_type=MESH,
        )

    def copy_of(part, chunk, stage):
        rows = slice(STAGE_AT[stage], STAGE_AT[stage] + STAGE_ROWS[stage])
        source, target = (sent, got) if stage < NARROW else (sent_wide, got_wide)
        return remote(part, chunk, source, target, rows, stage, partners[(part + stage) % 6])

    def last_copy(part, chunk, flip):
        rows = slice(LAST_AT + 8 * flip, LAST_AT + 8 * flip + 8)
        bits = [(part + STAGES + k) % 6 for k in range(2) if FLIPS[flip][k]]
        return remote(part, chunk, sent_wide, got_wide, rows, STAGES + flip, partner(*bits))

    def vec_copy(step):
        return pltpu.make_async_remote_copy(
            src_ref=vec.at[step],
            dst_ref=vec_in.at[step],
            send_sem=vec_send_sem.at[step],
            recv_sem=vec_recv_sem.at[step],
            device_id=partners[step] if step < BITS else other_core,
            device_id_type=MESH,
        )

    def vec_step(step):
        vec_copy(step - 1).wait_recv()
        vec[step] = vec[step - 1] + vec_in[step - 1]
        vec_copy(step).start()

    def product(part, chunk, at):
        return lax.dot_general(
            lhs[part, pl.ds(pl.multiple_of(at, 256), 256), :], grad[grad_columns(part, chunk), :],
            (((1,), (1,)), ((), ())), preferred_element_type=F32,
        )

    loss = jnp.zeros((8, ROWS), F32)
    for chunk in range(2):
        for third in range(3):
            at = grad_columns(third, chunk)
            loss = lax.fori_loop(at.start // STEP, at.stop // STEP, grad_step, loss)
            for part in (third, third + 3):
                block = product(part, chunk, (1 - mine[part]) * 256)
                sent[part, 0:256, columns(part, chunk)] = block.astype(BF16)
                copy_of(part, chunk, 0).start()

    for i in range(BLOCKS):
        at = slice(i * BLOCK_V, (i + 1) * BLOCK_V)
        grad_n[:, at] = jnp.transpose(grad[at, :].astype(F32)).astype(BF16)
    for i in range(4):
        at = slice(i * 256, (i + 1) * 256)
        back = jnp.dot(grad_n[...], weight[:, at], preferred_element_type=F32)
        vec[0, :, at] = jnp.sum(back * normed[:, at], axis=0, keepdims=True)
    ones = jnp.ones((16, ROWS), BF16)
    vec[0, :, WIDTH:LOSS_AT] = jnp.dot(ones, grad_n[...], preferred_element_type=F32)[0:1, :]
    lane = lane_ids(1, 128)
    loss_here = jnp.sum(jnp.sum(loss, axis=0, keepdims=True), axis=1, keepdims=True)
    vec[0, :, LOSS_AT:VEC] = jnp.where(lane == 0, loss_here, jnp.where(lane == 1, frames_here, 0.0))
    vec_copy(0).start()
    for chunk in range(2):
        for part in ORDER:
            acc[part, :, columns(part, chunk)] = product(part, chunk, mine[part] * 256)
    for k in range(1, CHIPS):
        hidden_copy(k, False).wait_send()
    hidden_swap.wait_send()
    stats_swap.wait_send()
    for copy in soft_copies:
        copy.wait_send()

    base = [0] * PARTS
    for stage in range(1, STAGES):
        rows = STAGE_ROWS[stage]
        before_at = STAGE_AT[stage - 1]
        incoming = got if stage - 1 < NARROW else got_wide
        for chunk in range(2):
            if 2 * stage + chunk - 1 < BITS:
                vec_step(2 * stage + chunk - 1)
            for part in ORDER:
                bit = mine[(part + stage) % 6]
                away, stay = (1 - bit) * rows, bit * rows
                at = columns(part, chunk)

                def joined(offset):
                    first = pl.multiple_of(base[part] + offset, 16)
                    return acc[part, pl.ds(first, rows), at] + incoming[
                        part, pl.ds(pl.multiple_of(before_at + offset, 16), rows), at
                    ].astype(F32)

                copy_of(part, chunk, stage - 1).wait_recv()
                block = joined(away)
                place_at = slice(STAGE_AT[stage], STAGE_AT[stage] + rows)
                if stage < NARROW:
                    sent[part, place_at, at] = block.astype(BF16)
                else:
                    sent_wide[part, place_at, at] = block
                copy_of(part, chunk, stage).start()
                acc[part, pl.ds(pl.multiple_of(base[part] + stay, 16), rows), at] = joined(stay)
        for part in range(PARTS):
            base[part] = base[part] + mine[(part + stage) % 6] * rows

    for chunk in range(2):
        for part in ORDER:
            at = columns(part, chunk)
            rows = pl.ds(pl.multiple_of(base[part], 32), 32)
            high, low_bit = mine[(part + STAGES) % 6], mine[(part + STAGES + 1) % 6]
            copy_of(part, chunk, STAGES - 1).wait_recv()
            acc[part, rows, at] += got_wide[part, 0:32, at]
            for flip in (2, 0, 1):
                to_high = 1 - high if FLIPS[flip][0] else high
                to_low = 1 - low_bit if FLIPS[flip][1] else low_bit
                first = pl.multiple_of(base[part] + to_high * 16 + to_low * 8, 8)
                sent_wide[part, LAST_AT + 8 * flip:LAST_AT + 8 * flip + 8, at] = acc[
                    part, pl.ds(first, 8), at
                ]
                last_copy(part, chunk, flip).start()
        if chunk == 0:
            vec_step(BITS)
    inverse = 1.0 / vec[BITS, :, LOSS_AT + 1:LOSS_AT + 2]
    for chunk in range(2):
        for part in ORDER:
            at = columns(part, chunk)
            high, low_bit = mine[(part + STAGES) % 6], mine[(part + STAGES + 1) % 6]
            first = pl.multiple_of(base[part] + high * 16 + low_bit * 8, 8)
            total = acc[part, pl.ds(first, 8), at]
            for flip in range(3):
                last_copy(part, chunk, flip).wait_recv()
                total = total + got_wide[part, LAST_AT + 8 * flip:LAST_AT + 8 * flip + 8, at]
            final[part // 3, :, grad_columns(part, chunk)] = total * inverse

    swap = to_pair(final.at[1 - t], final_in, 2)
    swap.start()
    vec_copy(BITS).wait_recv()
    total, beside = vec[BITS], vec_in[BITS]
    gain_out[...] = (total[:, 0:WIDTH] + beside[:, 0:WIDTH]) * inverse
    loss_out[...] = (total[:, LOSS_AT:VEC] + beside[:, LOSS_AT:VEC]) * inverse

    @pl.when(t == 0)
    def _():
        bias_out[:, 0:HALF_V] = total[:, WIDTH:LOSS_AT] * inverse
        bias_out[:, HALF_V:VOCAB] = beside[:, WIDTH:WIDTH + rest] * inverse
        weight_out[:, 0:HALF_V] = final[0]

    @pl.when(t == 1)
    def _():
        bias_out[:, 0:HALF_V] = beside[:, WIDTH:LOSS_AT] * inverse
        bias_out[:, HALF_V:VOCAB] = total[:, WIDTH:WIDTH + rest] * inverse
        weight_out[:, HALF_V:VOCAB] = final[1, :, 0:rest]

    for part in range(PARTS):
        for chunk in range(2):
            for stage in range(STAGES):
                copy_of(part, chunk, stage).wait_send()
            for flip in range(3):
                last_copy(part, chunk, flip).wait_send()
    for step in range(BITS + 1):
        vec_copy(step).wait_send()
    swap.wait_recv()

    @pl.when(t == 0)
    def _():
        weight_out[:, HALF_V:VOCAB] = final_in[:, 0:rest]

    @pl.when(t == 1)
    def _():
        weight_out[:, 0:HALF_V] = final_in[...]

    swap.wait_send()


def finish_kernel(weight_in, gain_in, bias_in, loss_in, weight_out, gain_out, bias_out, loss_out):
    weight_out[...] = weight_in[...]
    gain_out[...] = gain_in[...]
    bias_out[...] = bias_in[...]
    loss_out[...] = loss_in[...]


def distill(teacher, weight, *small):
    vmem = pl.BlockSpec(memory_space=pltpu.VMEM)
    hbm = pl.BlockSpec(memory_space=pl.ANY)
    dma = pltpu.SemaphoreType.DMA
    return pl.pallas_call(
        step_kernel,
        out_shape=(
            jax.ShapeDtypeStruct((8, VOCAB), F32),
            jax.ShapeDtypeStruct((1, WIDTH), F32),
            jax.ShapeDtypeStruct((1, VOCAB), F32),
            jax.ShapeDtypeStruct((1, 128), F32),
        ),
        in_specs=[hbm, hbm] + [vmem] * len(small),
        out_specs=(vmem,) * 4,
        scratch_shapes=[
            pltpu.VMEM((2 * HALF_V, ROWS), BF16),
            pltpu.VMEM((2 * HALF_V, ROWS), BF16),
            pltpu.VMEM((HALF_V, ROWS), BF16),
            pltpu.VMEM((HALF_V, WIDTH), BF16),
            pltpu.VMEM((CHIPS, 8, 512), BF16),
            pltpu.VMEM((CHIPS, 8, 512), BF16),
            pltpu.VMEM((8, ROWS), F32),
            pltpu.VMEM((8, ROWS), F32),
            pltpu.VMEM((ROWS, WIDTH), BF16),
            pltpu.VMEM((ROWS, WIDTH), BF16),
            pltpu.VMEM((1, 2 * HALF_V), F32),
            pltpu.VMEM((HALF_V, 128), F32),
            pltpu.VMEM((ROWS, WIDTH), F32),
            pltpu.VMEM((WIDTH, ROWS), BF16),
            pltpu.VMEM((WIDTH // 8, 8, ROWS), F32),
            pltpu.VMEM((HALF_V, ROWS), F32),
            pltpu.VMEM((HALF_V, ROWS), BF16),
            pltpu.VMEM((ROWS, HALF_V), BF16),
            pltpu.VMEM((PARTS, 512, ROWS), BF16),
            pltpu.VMEM((PARTS, 256, WIDEST), F32),
            pltpu.VMEM((PARTS, NARROW_ROWS, WIDEST), BF16),
            pltpu.VMEM((PARTS, NARROW_ROWS, WIDEST), BF16),
            pltpu.VMEM((PARTS, WIDE_ROWS, WIDEST), F32),
            pltpu.VMEM((PARTS, WIDE_ROWS, WIDEST), F32),
            pltpu.VMEM((2, 8, HALF_V), F32),
            pltpu.VMEM((8, HALF_V), F32),
            pltpu.VMEM((BITS + 1, 1, VEC), F32),
            pltpu.VMEM((BITS + 1, 1, VEC), F32),
            dma((PIECES,)),
            dma((BLOCKS,)),
            dma((CHIPS,)),
            dma((CHIPS,)),
            dma((PIECES,)),
            dma((PIECES,)),
            dma((3,)),
            dma((3,)),
            dma((PARTS * 2 * COPIES,)),
            dma((PARTS * 2 * COPIES,)),
            dma((BITS + 1,)),
            dma((BITS + 1,)),
        ],
        compiler_params=pltpu.CompilerParams(
            collective_id=0, has_side_effects=True, vmem_limit_bytes=60 * 1024 * 1024
        ),
    )(teacher, weight, *small)


def body(
    teacher_logits, routes, agreement, targets, lengths, student_hidden, out_weight, out_bias, gain
):
    weight_grad, gain_grad, bias_grad, loss = distill(
        teacher_logits[0].T,
        out_weight.T,
        student_hidden,
        routes.reshape(1, ROWS),
        agreement[None],
        targets[None],
        lengths[None],
        out_bias[None],
        gain[None],
    )
    vmem = pl.BlockSpec(memory_space=pltpu.VMEM)
    parts = (weight_grad, gain_grad, bias_grad, loss)
    weight_grad, gain_grad, bias_grad, loss = pl.pallas_call(
        finish_kernel,
        out_shape=tuple(jax.ShapeDtypeStruct(x.shape, x.dtype) for x in parts),
        in_specs=[vmem] * 4,
        out_specs=(vmem,) * 4,
    )(*parts)
    return (weight_grad, gain_grad[0], bias_grad[0], loss[0, 0])


def solution(mesh):
    finer = Mesh(
        mesh.devices.reshape(mesh.shape["teach"], 4, 4, 4), ("teach", "dp_0", "dp_1", "dp_2")
    )
    in_specs = (
        P("teach", DP, None),
        P(DP, None),
        P(DP),
        P(DP),
        P(DP),
        P(TEACH_DP, None),
        P(),
        P(),
        P(),
    )
    out_specs = (P(TEACH_DP, None), P(), P(), P())
    return jax.shard_map(body, mesh=finer, in_specs=in_specs, out_specs=out_specs, check_vma=False)
```

```python
import jax
import jax.numpy as jnp
from jax import lax
from jax.experimental import pallas as pl
from jax.experimental.pallas import tpu as pltpu
from jax.sharding import Mesh
from jax.sharding import PartitionSpec as P

DP = ("dp_0", "dp_1", "dp_2")
TEACH_DP = ("teach", "dp_0", "dp_1", "dp_2")
MESH = pl.DeviceIdType.MESH
F32 = jnp.float32
BF16 = jnp.bfloat16

EPSILON = 1e-05
VOCAB = 5000
WIDTH = 1024
ROWS = 256
STUDENTS = 128

HALF_V = 2560
BLOCK_V = 512
BLOCKS = 5
THIRDS = ((0, 896), (896, 896), (1792, 768))
WIDEST = 896
CHUNKS = (((0, 512), (512, 384)), ((0, 512), (512, 384)), ((0, 384), (384, 384)))
STAGE_ROWS = (256, 128, 64, 32)
STAGE_AT = (0, 256, 384, 0)
NARROW = 3
NARROW_ROWS = 448
WIDE_ROWS = 56
LAST_AT = 32
FLIPS = ((1, 0), (0, 1), (1, 1))
PARTS = 6
STAGES = 4
COPIES = 7
ORDER = (0, 3, 1, 4, 2, 5)
BITS = 6
VEC = WIDTH + HALF_V + 128
LOSS_AT = WIDTH + HALF_V
STEP = 64
PIECES = 4
CHIPS = 64


def chunk_of(part, row):
    bits = [0] * 6
    for k in range(6):
        bits[(part + k) % 6] = (row >> (5 - k)) & 1
    chip = 0
    for dim in range(3):
        low, high = bits[dim], bits[3 + dim]
        chip = chip * 4 + high * 2 + (high ^ low)
    return chip


def rows_at(k, size=STEP):
    return pl.ds(pl.multiple_of(k * size, size), size)


def lane_ids(rows, width):
    return lax.broadcasted_iota(jnp.int32, (rows, width), 1)


def sublane_ids(rows, width):
    return lax.broadcasted_iota(jnp.int32, (rows, width), 0)


def folded(x, rows, op):
    groups = x.reshape(x.shape[0] // rows, rows, x.shape[1])
    total = groups[0]
    for k in range(1, groups.shape[0]):
        total = op(total, groups[k])
    return total


def step_kernel(
    teacher_hbm, weight_hbm, hidden_hbm, routes_hbm, agree_hbm, target_hbm, bias_hbm, gain_hbm, length_ref,
    weight_out, gain_out, bias_out, loss_out,
    hidden_ref, routes_ref, agree_ref, target_ref, gain_ref, bias_ref,
    teacher, soft, soft_in, weight, message, arrived, stats, stats_in, mine_h, their_h,
    bias_row, bias_t, normed, scaled, scaled_t, logits, grad, grad_n,
    lhs, acc, sent, got, sent_wide, got_wide, final, final_in, vec, vec_in,
    small_sem, teacher_sem, weight_sem, hidden_send, hidden_recv, soft_send, soft_recv, pair_send, pair_recv,
    send_sem, recv_sem, vec_send_sem, vec_recv_sem,
):
    t = lax.axis_index("teach")
    place = [lax.axis_index(axis) for axis in DP]
    me = place[0] * 16 + place[1] * 4 + place[2]

    def partner(*bits):
        ids = list(place)
        for bit in bits:
            v = place[bit % 3]
            ids[bit % 3] = (3 - v) if bit >= 3 else (v + 1 - 2 * (v % 2))
        return (t, ids[0], ids[1], ids[2])

    def my_bit(bit):
        v = place[bit % 3]
        return v // 2 if bit >= 3 else (v // 2 + v % 2) % 2

    partners = [partner(bit) for bit in range(6)]
    mine = [my_bit(bit) for bit in range(6)]
    other_core = (1 - t, place[0], place[1], place[2])

    turned_by = [[(v + d) % 4 for d in range(4)] for v in place]

    def moved(k, sign):
        step = (k * 21) % CHIPS
        steps = (step // 16, (step // 4) % 4, step % 4)
        return [turned_by[axis][(sign * d) % 4] for axis, d in enumerate(steps)]

    def index_of(ids):
        return ids[0] * 16 + ids[1] * 4 + ids[2]

    small_copies = [
        pltpu.make_async_copy(source, target, small_sem.at[i])
        for i, (source, target) in enumerate(
            (
                (hidden_hbm, hidden_ref),
                (routes_hbm, routes_ref),
                (agree_hbm, agree_ref),
                (target_hbm, target_ref),
                (gain_hbm, gain_ref),
                (bias_hbm, bias_ref),
            )
        )
    ]
    for copy in small_copies:
        copy.start()
    barrier = pltpu.get_barrier_semaphore()
    for k in range(1, CHIPS):
        ids = moved(k, 1)
        pl.semaphore_signal(
            barrier, inc=1, device_id=(t, ids[0], ids[1], ids[2]), device_id_type=MESH
        )
    pl.semaphore_signal(barrier, inc=1, device_id=other_core, device_id_type=MESH)

    cuts = (0, 1280, 2560, 3840, VOCAB)
    teacher_copies = [
        pltpu.make_async_copy(
            teacher_hbm.at[cuts[q]:cuts[q + 1], :],
            teacher.at[cuts[q]:cuts[q + 1], :],
            teacher_sem.at[q],
        )
        for q in range(PIECES)
    ]
    for copy in teacher_copies:
        copy.start()
    weight_copies = [
        pltpu.make_async_copy(
            weight_hbm.at[pl.ds(pl.multiple_of(t * HALF_V + i * BLOCK_V, BLOCK_V), BLOCK_V), :],
            weight.at[i * BLOCK_V:(i + 1) * BLOCK_V, :],
            weight_sem.at[i],
        )
        for i in range(BLOCKS - 1)
    ]
    last_at = (BLOCKS - 1) * BLOCK_V
    rest = VOCAB - HALF_V
    last_first = pltpu.make_async_copy(
        weight_hbm.at[last_at:HALF_V, :],
        weight.at[last_at:HALF_V, :],
        weight_sem.at[BLOCKS - 1],
    )
    last_second = pltpu.make_async_copy(
        weight_hbm.at[HALF_V + last_at:VOCAB, :],
        weight.at[last_at:rest, :],
        weight_sem.at[BLOCKS - 1],
    )
    for copy in weight_copies:
        copy.start()

    @pl.when(t == 0)
    def _():
        last_first.start()

    @pl.when(t == 1)
    def _():
        last_second.start()
        weight[rest:HALF_V, :] = jnp.zeros((HALF_V - rest, WIDTH), BF16)

    low = sublane_ids(8, 512) < 4
    for copy in small_copies:
        copy.wait()

    def pack(k, carry):
        x = hidden_ref[pl.ds(pl.multiple_of(k * 16, 16), 16), :].astype(F32)
        for i in range(2):
            left, right = x[8 * i:8 * i + 8, 0:512], x[8 * i:8 * i + 8, 512:1024]
            message[4 * k + 2 * i] = jnp.where(low, left, pltpu.roll(right, 4, 0)).astype(BF16)
            message[4 * k + 2 * i + 1] = jnp.where(low, pltpu.roll(left, 4, 0), right).astype(BF16)
        return carry

    lax.fori_loop(0, ROWS // 16, pack, 0)
    arrived[me] = message[me]

    routes_row = routes_ref[...].astype(F32)
    live = (lane_ids(1, ROWS) < length_ref[0]).astype(F32)
    half_live = live * 0.5
    weight_row = half_live * agree_ref[...].astype(F32)
    frames_here = jnp.sum(live, axis=1, keepdims=True)
    named = (routes_row == sublane_ids(STUDENTS, ROWS).astype(F32)).astype(F32)
    earlier = (sublane_ids(ROWS, ROWS) < lane_ids(ROWS, ROWS)).astype(F32)
    before = jnp.dot(named.astype(BF16), earlier.astype(BF16), preferred_element_type=F32)
    slot = jnp.sum(before * named, axis=0, keepdims=True)
    wanted = (routes_row - (t * CHIPS).astype(F32)) * 8.0 + slot
    wanted = jnp.transpose(jnp.broadcast_to(wanted, (8, ROWS)))[:, 0:1]

    bias_row[:, 0:VOCAB] = bias_ref[...]
    bias_row[:, VOCAB:2 * HALF_V] = jnp.zeros((1, 2 * HALF_V - VOCAB), F32)

    def bias_step(k, carry):
        strip = bias_row[:, pl.ds(pl.multiple_of(t * HALF_V + k * 128, 128), 128)]
        bias_t[rows_at(k, 128), :] = jnp.transpose(jnp.broadcast_to(strip, (128, 128)))
        return carry

    lax.fori_loop(0, HALF_V // 128, bias_step, 0)

    teacher[VOCAB:2 * HALF_V, :] = jnp.full((2 * HALF_V - VOCAB, ROWS), -1e30, BF16)

    def max_step(k, top):
        return jnp.maximum(top, folded(teacher[rows_at(k), :], 16, jnp.maximum))

    top = jnp.full((16, ROWS), -1e30, BF16)
    for q in range(PIECES):
        teacher_copies[q].wait()
        last = cuts[q + 1] // STEP if q < PIECES - 1 else 2 * HALF_V // STEP
        top = lax.fori_loop(cuts[q] // STEP, last, max_step, top, unroll=2)
    top = jnp.max(top.astype(F32), axis=0, keepdims=True)

    pl.semaphore_wait(barrier, CHIPS)

    def hidden_copy(k, receiving):
        ids = moved(k, 1)
        source = index_of(moved(k, -1)) if receiving else me
        return pltpu.make_async_remote_copy(
            src_ref=message.at[index_of(ids)],
            dst_ref=arrived.at[source],
            send_sem=hidden_send.at[k],
            recv_sem=hidden_recv.at[k],
            device_id=(t, ids[0], ids[1], ids[2]),
            device_id_type=MESH,
        )

    for k in range(1, CHIPS):
        hidden_copy(k, False).start()

    def sum_step(k, total):
        return total + folded(jnp.exp(teacher[rows_at(k), :].astype(F32) - top), 8, jnp.add)

    total = lax.fori_loop(0, 2 * HALF_V // STEP, sum_step, jnp.zeros((8, ROWS), F32), unroll=2)
    scale_row = weight_row / jnp.sum(total, axis=0, keepdims=True)

    target_row = target_ref[...]
    step_rows = sublane_ids(STEP, ROWS)

    def soft_step(k, mass):
        rows = rows_at(k)
        e = jnp.exp(teacher[rows, :].astype(F32) - top)
        hit = step_rows == target_row - k * STEP
        s = (e * scale_row + jnp.where(hit, half_live, 0.0)).astype(BF16)
        soft[rows, :] = s
        return mass + folded(s.astype(F32), 8, jnp.add)

    piece = HALF_V // PIECES
    soft_copies = [
        pltpu.make_async_remote_copy(
            src_ref=soft.at[pl.ds(pl.multiple_of((1 - t) * HALF_V + q * piece, 64), piece), :],
            dst_ref=soft_in.at[q * piece:(q + 1) * piece, :],
            send_sem=soft_send.at[q],
            recv_sem=soft_recv.at[q],
            device_id=other_core,
            device_id_type=MESH,
        )
        for q in range(PIECES)
    ]
    mass = jnp.zeros((8, ROWS), F32)
    for q in range(PIECES):
        first = (1 - t) * (HALF_V // STEP) + q * (piece // STEP)
        mass = lax.fori_loop(first, first + piece // STEP, soft_step, mass)
        soft_copies[q].start()
    first = t * (HALF_V // STEP)
    mass = lax.fori_loop(first, first + HALF_V // STEP, soft_step, mass)
    mass = jnp.sum(mass, axis=0, keepdims=True)

    for k in range(1, CHIPS):
        hidden_copy(k, True).wait_recv()
    rows_in = arrived[...].reshape(CHIPS * 8, 512)
    for i in range(2):
        pick = (wanted + 4.0 * i == lane_ids(ROWS, CHIPS * 8).astype(F32)).astype(F32).astype(BF16)
        mine_h[:, 512 * i:512 * i + 512] = jnp.dot(
            pick, rows_in, preferred_element_type=F32
        ).astype(BF16)

    def to_pair(source, target, index):
        return pltpu.make_async_remote_copy(
            src_ref=source,
            dst_ref=target,
            send_sem=pair_send.at[index],
            recv_sem=pair_recv.at[index],
            device_id=other_core,
            device_id_type=MESH,
        )

    hidden_swap = to_pair(mine_h, their_h, 0)
    hidden_swap.start()

    hidden_swap.wait_recv()
    states = mine_h[...].astype(F32) + their_h[...].astype(F32)
    states = states - jnp.mean(states, axis=1, keepdims=True)
    spread = jnp.mean(jnp.square(states), axis=1, keepdims=True)
    states = states * lax.rsqrt(spread + EPSILON)
    normed[...] = states
    turned = jnp.transpose((states * gain_ref[...]).astype(BF16).astype(F32))
    scaled_t[...] = turned.reshape(WIDTH // 8, 8, ROWS)
    scaled[...] = turned.astype(BF16)

    for copy in weight_copies:
        copy.wait()

    @pl.when(t == 0)
    def _():
        last_first.wait()

    @pl.when(t == 1)
    def _():
        last_second.wait()

    peaks, sums = [], []
    for i in range(BLOCKS):
        at = slice(i * BLOCK_V, (i + 1) * BLOCK_V)
        slope = bias_t[at, :]
        block = jnp.dot(weight[at, :], scaled[...], preferred_element_type=F32)
        block = block + jnp.concatenate([slope, slope], axis=1)
        if i == BLOCKS - 1:
            inside = sublane_ids(BLOCK_V, ROWS) < VOCAB - i * BLOCK_V - t * HALF_V
            block = jnp.where(inside, block, -1e30)
        logits[at, :] = block
        peak = jnp.max(folded(block, 8, jnp.maximum), axis=0, keepdims=True)
        total = jnp.zeros((8, ROWS), F32)
        for k in range(BLOCK_V // STEP):
            part_at = slice(i * BLOCK_V + k * STEP, i * BLOCK_V + (k + 1) * STEP)
            total = total + folded(jnp.exp(logits[part_at, :] - peak), 8, jnp.add)
        peaks.append(peak)
        sums.append(total)
    peak = peaks[0]
    for other in peaks[1:]:
        peak = jnp.maximum(peak, other)
    total = jnp.zeros((8, ROWS), F32)
    for other, terms in zip(peaks, sums):
        total = total + terms * jnp.exp(other - peak)
    lse = peak + jnp.log(jnp.sum(total, axis=0, keepdims=True))
    stats[...] = jnp.concatenate([lse, mass, jnp.zeros((6, ROWS), F32)], axis=0)
    stats_swap = to_pair(stats, stats_in, 1)
    stats_swap.start()

    for part in range(PARTS):
        half = part // 3
        for row in range(0, 64, 2):
            pair = jnp.concatenate(
                [scaled_t[half * 64 + chunk_of(part, row)], scaled_t[half * 64 + chunk_of(part, row + 1)]],
                axis=0,
            )
            lhs[part, row * 8:row * 8 + 16, :] = pair.astype(BF16)

    for copy in soft_copies:
        copy.wait_recv()
    stats_swap.wait_recv()
    there = stats_in[...]
    other_lse = there[0:1, :]
    highest = jnp.maximum(lse, other_lse)
    lse = highest + jnp.log(jnp.exp(lse - highest) + jnp.exp(other_lse - highest))
    mass = mass + there[1:2, :]

    def grad_step(k, loss):
        rows = slice(k * STEP, (k + 1) * STEP)
        log_probs = logits[rows, :] - lse
        own = pl.ds(pl.multiple_of(t * HALF_V + k * STEP, STEP), STEP)
        both = soft[own, :].astype(F32) + soft_in[rows, :].astype(F32)
        grad[rows, :] = (mass * jnp.exp(log_probs) - both).astype(BF16)
        return loss - folded(both * log_probs, 8, jnp.add)

    def columns(part, chunk):
        first, width = CHUNKS[part % 3][chunk]
        return slice(first, first + width)

    def grad_columns(part, chunk):
        first = THIRDS[part % 3][0]
        at = columns(part, chunk)
        return slice(first + at.start, first + at.stop)

    def remote(part, chunk, source, target, rows, index, device):
        at = columns(part, chunk)
        number = (part * 2 + chunk) * COPIES + index
        return pltpu.make_async_remote_copy(
            src_ref=source.at[part, rows, at],
            dst_ref=target.at[part, rows, at],
            send_sem=send_sem.at[number],
            recv_sem=recv_sem.at[number],
            device_id=device,
            device_id_type=MESH,
        )

    def copy_of(part, chunk, stage):
        rows = slice(STAGE_AT[stage], STAGE_AT[stage] + STAGE_ROWS[stage])
        source, target = (sent, got) if stage < NARROW else (sent_wide, got_wide)
        return remote(part, chunk, source, target, rows, stage, partners[(part + stage) % 6])

    def last_copy(part, chunk, flip):
        rows = slice(LAST_AT + 8 * flip, LAST_AT + 8 * flip + 8)
        bits = [(part + STAGES + k) % 6 for k in range(2) if FLIPS[flip][k]]
        return remote(part, chunk, sent_wide, got_wide, rows, STAGES + flip, partner(*bits))

    def vec_copy(step):
        return pltpu.make_async_remote_copy(
            src_ref=vec.at[step],
            dst_ref=vec_in.at[step],
            send_sem=vec_send_sem.at[step],
            recv_sem=vec_recv_sem.at[step],
            device_id=partners[step] if step < BITS else other_core,
            device_id_type=MESH,
        )

    def vec_step(step):
        vec_copy(step - 1).wait_recv()
        vec[step] = vec[step - 1] + vec_in[step - 1]
        vec_copy(step).start()

    def product(part, chunk, at):
        return lax.dot_general(
            lhs[part, pl.ds(pl.multiple_of(at, 256), 256), :], grad[grad_columns(part, chunk), :],
            (((1,), (1,)), ((), ())), preferred_element_type=F32,
        )

    loss = jnp.zeros((8, ROWS), F32)
    for chunk in range(2):
        for third in range(3):
            at = grad_columns(third, chunk)
            for k in range(at.start // STEP, at.stop // STEP):
                loss = grad_step(k, loss)
            for part in (third, third + 3):
                block = product(part, chunk, (1 - mine[part]) * 256)
                sent[part, 0:256, columns(part, chunk)] = block.astype(BF16)
                copy_of(part, chunk, 0).start()

    for i in range(BLOCKS):
        at = slice(i * BLOCK_V, (i + 1) * BLOCK_V)
        grad_n[:, at] = jnp.transpose(grad[at, :].astype(F32)).astype(BF16)
    for i in range(4):
        at = slice(i * 256, (i + 1) * 256)
        back = jnp.dot(grad_n[...], weight[:, at], preferred_element_type=F32)
        vec[0, :, at] = jnp.sum(back * normed[:, at], axis=0, keepdims=True)
    ones = jnp.ones((16, ROWS), BF16)
    vec[0, :, WIDTH:LOSS_AT] = jnp.dot(ones, grad_n[...], preferred_element_type=F32)[0:1, :]
    lane = lane_ids(1, 128)
    loss_here = jnp.sum(jnp.sum(loss, axis=0, keepdims=True), axis=1, keepdims=True)
    vec[0, :, LOSS_AT:VEC] = jnp.where(lane == 0, loss_here, jnp.where(lane == 1, frames_here, 0.0))
    vec_copy(0).start()
    for chunk in range(2):
        for part in ORDER:
            acc[part, :, columns(part, chunk)] = product(part, chunk, mine[part] * 256)
    for k in range(1, CHIPS):
        hidden_copy(k, False).wait_send()
    hidden_swap.wait_send()
    stats_swap.wait_send()
    for copy in soft_copies:
        copy.wait_send()

    base = [0] * PARTS
    for stage in range(1, STAGES):
        rows = STAGE_ROWS[stage]
        before_at = STAGE_AT[stage - 1]
        incoming = got if stage - 1 < NARROW else got_wide
        for chunk in range(2):
            if 2 * stage + chunk - 1 < BITS:
                vec_step(2 * stage + chunk - 1)
            for part in ORDER:
                bit = mine[(part + stage) % 6]
                away, stay = (1 - bit) * rows, bit * rows
                at = columns(part, chunk)

                def joined(offset):
                    first = pl.multiple_of(base[part] + offset, 16)
                    return acc[part, pl.ds(first, rows), at] + incoming[
                        part, pl.ds(pl.multiple_of(before_at + offset, 16), rows), at
                    ].astype(F32)

                copy_of(part, chunk, stage - 1).wait_recv()
                block = joined(away)
                place_at = slice(STAGE_AT[stage], STAGE_AT[stage] + rows)
                if stage < NARROW:
                    sent[part, place_at, at] = block.astype(BF16)
                else:
                    sent_wide[part, place_at, at] = block
                copy_of(part, chunk, stage).start()
                acc[part, pl.ds(pl.multiple_of(base[part] + stay, 16), rows), at] = joined(stay)
        for part in range(PARTS):
            base[part] = base[part] + mine[(part + stage) % 6] * rows

    for chunk in range(2):
        for part in ORDER:
            at = columns(part, chunk)
            rows = pl.ds(pl.multiple_of(base[part], 32), 32)
            high, low_bit = mine[(part + STAGES) % 6], mine[(part + STAGES + 1) % 6]
            copy_of(part, chunk, STAGES - 1).wait_recv()
            acc[part, rows, at] += got_wide[part, 0:32, at]
            for flip in (2, 0, 1):
                to_high = 1 - high if FLIPS[flip][0] else high
                to_low = 1 - low_bit if FLIPS[flip][1] else low_bit
                first = pl.multiple_of(base[part] + to_high * 16 + to_low * 8, 8)
                sent_wide[part, LAST_AT + 8 * flip:LAST_AT + 8 * flip + 8, at] = acc[
                    part, pl.ds(first, 8), at
                ]
                last_copy(part, chunk, flip).start()
        if chunk == 0:
            vec_step(BITS)
    inverse = 1.0 / vec[BITS, :, LOSS_AT + 1:LOSS_AT + 2]
    for chunk in range(2):
        for part in ORDER:
            at = columns(part, chunk)
            high, low_bit = mine[(part + STAGES) % 6], mine[(part + STAGES + 1) % 6]
            first = pl.multiple_of(base[part] + high * 16 + low_bit * 8, 8)
            total = acc[part, pl.ds(first, 8), at]
            for flip in range(3):
                last_copy(part, chunk, flip).wait_recv()
                total = total + got_wide[part, LAST_AT + 8 * flip:LAST_AT + 8 * flip + 8, at]
            final[part // 3, :, grad_columns(part, chunk)] = total * inverse

    swap = to_pair(final.at[1 - t], final_in, 2)
    swap.start()
    vec_copy(BITS).wait_recv()
    total, beside = vec[BITS], vec_in[BITS]
    gain_out[...] = (total[:, 0:WIDTH] + beside[:, 0:WIDTH]) * inverse
    loss_out[...] = (total[:, LOSS_AT:VEC] + beside[:, LOSS_AT:VEC]) * inverse

    @pl.when(t == 0)
    def _():
        bias_out[:, 0:HALF_V] = total[:, WIDTH:LOSS_AT] * inverse
        bias_out[:, HALF_V:VOCAB] = beside[:, WIDTH:WIDTH + rest] * inverse
        weight_out[:, 0:HALF_V] = final[0]

    @pl.when(t == 1)
    def _():
        bias_out[:, 0:HALF_V] = beside[:, WIDTH:LOSS_AT] * inverse
        bias_out[:, HALF_V:VOCAB] = total[:, WIDTH:WIDTH + rest] * inverse
        weight_out[:, HALF_V:VOCAB] = final[1, :, 0:rest]

    for part in range(PARTS):
        for chunk in range(2):
            for stage in range(STAGES):
                copy_of(part, chunk, stage).wait_send()
            for flip in range(3):
                last_copy(part, chunk, flip).wait_send()
    for step in range(BITS + 1):
        vec_copy(step).wait_send()
    swap.wait_recv()

    @pl.when(t == 0)
    def _():
        weight_out[:, HALF_V:VOCAB] = final_in[:, 0:rest]

    @pl.when(t == 1)
    def _():
        weight_out[:, 0:HALF_V] = final_in[...]

    swap.wait_send()


def finish_kernel(weight_in, gain_in, bias_in, loss_in, weight_out, gain_out, bias_out, loss_out):
    weight_out[...] = weight_in[...]
    gain_out[...] = gain_in[...]
    bias_out[...] = bias_in[...]
    loss_out[...] = loss_in[...]


def distill(*arrays):
    vmem = pl.BlockSpec(memory_space=pltpu.VMEM)
    hbm = pl.BlockSpec(memory_space=pl.ANY)
    dma = pltpu.SemaphoreType.DMA
    return pl.pallas_call(
        step_kernel,
        out_shape=(
            jax.ShapeDtypeStruct((8, VOCAB), F32),
            jax.ShapeDtypeStruct((1, WIDTH), F32),
            jax.ShapeDtypeStruct((1, VOCAB), F32),
            jax.ShapeDtypeStruct((1, 128), F32),
        ),
        in_specs=[hbm] * 8 + [pl.BlockSpec(memory_space=pltpu.SMEM)],
        out_specs=(vmem,) * 4,
        scratch_shapes=[
            pltpu.VMEM((ROWS, WIDTH), BF16),
            pltpu.VMEM((1, ROWS), jnp.int32),
            pltpu.VMEM((1, ROWS), jnp.int32),
            pltpu.VMEM((1, ROWS), jnp.int32),
            pltpu.VMEM((1, WIDTH), F32),
            pltpu.VMEM((1, VOCAB), F32),
            pltpu.VMEM((2 * HALF_V, ROWS), BF16),
            pltpu.VMEM((2 * HALF_V, ROWS), BF16),
            pltpu.VMEM((HALF_V, ROWS), BF16),
            pltpu.VMEM((HALF_V, WIDTH), BF16),
            pltpu.VMEM((CHIPS, 8, 512), BF16),
            pltpu.VMEM((CHIPS, 8, 512), BF16),
            pltpu.VMEM((8, ROWS), F32),
            pltpu.VMEM((8, ROWS), F32),
            pltpu.VMEM((ROWS, WIDTH), BF16),
            pltpu.VMEM((ROWS, WIDTH), BF16),
            pltpu.VMEM((1, 2 * HALF_V), F32),
            pltpu.VMEM((HALF_V, 128), F32),
            pltpu.VMEM((ROWS, WIDTH), F32),
            pltpu.VMEM((WIDTH, ROWS), BF16),
            pltpu.VMEM((WIDTH // 8, 8, ROWS), F32),
            pltpu.VMEM((HALF_V, ROWS), F32),
            pltpu.VMEM((HALF_V, ROWS), BF16),
            pltpu.VMEM((ROWS, HALF_V), BF16),
            pltpu.VMEM((PARTS, 512, ROWS), BF16),
            pltpu.VMEM((PARTS, 256, WIDEST), F32),
            pltpu.VMEM((PARTS, NARROW_ROWS, WIDEST), BF16),
            pltpu.VMEM((PARTS, NARROW_ROWS, WIDEST), BF16),
            pltpu.VMEM((PARTS, WIDE_ROWS, WIDEST), F32),
            pltpu.VMEM((PARTS, WIDE_ROWS, WIDEST), F32),
            pltpu.VMEM((2, 8, HALF_V), F32),
            pltpu.VMEM((8, HALF_V), F32),
            pltpu.VMEM((BITS + 1, 1, VEC), F32),
            pltpu.VMEM((BITS + 1, 1, VEC), F32),
            dma((6,)),
            dma((PIECES,)),
            dma((BLOCKS,)),
            dma((CHIPS,)),
            dma((CHIPS,)),
            dma((PIECES,)),
            dma((PIECES,)),
            dma((3,)),
            dma((3,)),
            dma((PARTS * 2 * COPIES,)),
            dma((PARTS * 2 * COPIES,)),
            dma((BITS + 1,)),
            dma((BITS + 1,)),
        ],
        compiler_params=pltpu.CompilerParams(
            collective_id=0, has_side_effects=True, vmem_limit_bytes=60 * 1024 * 1024
        ),
    )(*arrays)


def body(
    teacher_logits, routes, agreement, targets, lengths, student_hidden, out_weight, out_bias, gain
):
    weight_grad, gain_grad, bias_grad, loss = distill(
        teacher_logits[0].T,
        out_weight.T,
        student_hidden,
        routes.reshape(1, ROWS),
        agreement[None],
        targets[None],
        out_bias[None],
        gain[None],
        lengths,
    )
    vmem = pl.BlockSpec(memory_space=pltpu.VMEM)
    parts = (weight_grad, gain_grad, bias_grad, loss)
    weight_grad, gain_grad, bias_grad, loss = pl.pallas_call(
        finish_kernel,
        out_shape=tuple(jax.ShapeDtypeStruct(x.shape, x.dtype) for x in parts),
        in_specs=[vmem] * 4,
        out_specs=(vmem,) * 4,
    )(*parts)
    return (weight_grad, gain_grad[0], bias_grad[0], loss[0, 0])


def solution(mesh):
    finer = Mesh(
        mesh.devices.reshape(mesh.shape["teach"], 4, 4, 4), ("teach", "dp_0", "dp_1", "dp_2")
    )
    in_specs = (
        P("teach", DP, None),
        P(DP, None),
        P(DP),
        P(DP),
        P(DP),
        P(TEACH_DP, None),
        P(),
        P(),
        P(),
    )
    out_specs = (P(TEACH_DP, None), P(), P(), P())
    return jax.shard_map(body, mesh=finer, in_specs=in_specs, out_specs=out_specs, check_vma=False)
```

```python
import jax
import jax.numpy as jnp
from jax import lax
from jax.experimental import pallas as pl
from jax.experimental.pallas import tpu as pltpu
from jax.sharding import Mesh
from jax.sharding import PartitionSpec as P

DP = ("dp_0", "dp_1", "dp_2")
TEACH_DP = ("teach", "dp_0", "dp_1", "dp_2")
MESH = pl.DeviceIdType.MESH
F32 = jnp.float32
BF16 = jnp.bfloat16

EPSILON = 1e-05
VOCAB = 5000
WIDTH = 1024
ROWS = 256
STUDENTS = 128

HALF_V = 2560
BLOCK_V = 512
BLOCKS = 5
THIRDS = ((0, 896), (896, 896), (1792, 768))
WIDEST = 896
CHUNKS = (((0, 512), (512, 384)), ((0, 512), (512, 384)), ((0, 384), (384, 384)))
STAGE_ROWS = (256, 128, 64, 32)
STAGE_AT = (0, 256, 384, 0)
NARROW = 3
NARROW_ROWS = 448
WIDE_ROWS = 56
LAST_AT = 32
FLIPS = ((1, 0), (0, 1), (1, 1))
PARTS = 6
STAGES = 4
COPIES = 7
ORDER = (0, 3, 1, 4, 2, 5)
ROUNDS = 3
VEC = WIDTH + HALF_V + 128
LOSS_AT = WIDTH + HALF_V
STEP = 64
PIECES = 4
CHIPS = 64


def chunk_of(part, row):
    bits = [0] * 6
    for k in range(6):
        bits[(part + k) % 6] = (row >> (5 - k)) & 1
    chip = 0
    for dim in range(3):
        low, high = bits[dim], bits[3 + dim]
        chip = chip * 4 + high * 2 + (high ^ low)
    return chip


def hops(k):
    return sum(min(d, 4 - d) for d in (k // 16, (k // 4) % 4, k % 4))


OFFSETS = tuple(sorted(((k * 21) % CHIPS for k in range(1, CHIPS)), key=lambda k: -hops(k)))


def rows_at(k, size=STEP):
    return pl.ds(pl.multiple_of(k * size, size), size)


def lane_ids(rows, width):
    return lax.broadcasted_iota(jnp.int32, (rows, width), 1)


def sublane_ids(rows, width):
    return lax.broadcasted_iota(jnp.int32, (rows, width), 0)


def folded(x, rows, op):
    groups = x.reshape(x.shape[0] // rows, rows, x.shape[1])
    total = groups[0]
    for k in range(1, groups.shape[0]):
        total = op(total, groups[k])
    return total


def step_kernel(
    teacher_hbm, weight_hbm, hidden_hbm, routes_hbm, agree_hbm, target_hbm, bias_hbm, gain_hbm, length_ref,
    weight_out, gain_out, bias_out, loss_out,
    hidden_ref, routes_ref, agree_ref, target_ref, gain_ref, bias_ref,
    teacher, soft, soft_in, weight, message, arrived, stats, stats_in, mine_h, their_h,
    bias_row, bias_t, normed, scaled, scaled_t, logits, grad, grad_n,
    lhs, acc, sent, got, sent_wide, got_wide, final, final_in, vec, vec_in,
    small_sem, teacher_sem, weight_sem, hidden_send, hidden_recv, soft_send, soft_recv, pair_send, pair_recv,
    send_sem, recv_sem, vec_send_sem, vec_recv_sem,
):
    t = lax.axis_index("teach")
    place = [lax.axis_index(axis) for axis in DP]
    me = place[0] * 16 + place[1] * 4 + place[2]

    def partner(*bits):
        ids = list(place)
        for bit in bits:
            v = place[bit % 3]
            ids[bit % 3] = (3 - v) if bit >= 3 else (v + 1 - 2 * (v % 2))
        return (t, ids[0], ids[1], ids[2])

    def my_bit(bit):
        v = place[bit % 3]
        return v // 2 if bit >= 3 else (v // 2 + v % 2) % 2

    partners = [partner(bit) for bit in range(6)]
    mine = [my_bit(bit) for bit in range(6)]
    other_core = (1 - t, place[0], place[1], place[2])

    turned_by = [[(v + d) % 4 for d in range(4)] for v in place]

    def moved(k, sign):
        steps = (k // 16, (k // 4) % 4, k % 4)
        return [turned_by[axis][(sign * d) % 4] for axis, d in enumerate(steps)]

    def index_of(ids):
        return ids[0] * 16 + ids[1] * 4 + ids[2]

    small_copies = [
        pltpu.make_async_copy(source, target, small_sem.at[i])
        for i, (source, target) in enumerate(
            (
                (hidden_hbm, hidden_ref),
                (routes_hbm, routes_ref),
                (agree_hbm, agree_ref),
                (target_hbm, target_ref),
                (gain_hbm, gain_ref),
                (bias_hbm, bias_ref),
            )
        )
    ]
    for copy in small_copies:
        copy.start()
    barrier = pltpu.get_barrier_semaphore()
    for k in OFFSETS:
        ids = moved(k, 1)
        pl.semaphore_signal(
            barrier, inc=1, device_id=(t, ids[0], ids[1], ids[2]), device_id_type=MESH
        )
    pl.semaphore_signal(barrier, inc=1, device_id=other_core, device_id_type=MESH)

    cuts = (0, 1280, 2560, 3840, VOCAB)
    teacher_copies = [
        pltpu.make_async_copy(
            teacher_hbm.at[cuts[q]:cuts[q + 1], :],
            teacher.at[cuts[q]:cuts[q + 1], :],
            teacher_sem.at[q],
        )
        for q in range(PIECES)
    ]
    for copy in teacher_copies:
        copy.start()
    weight_copies = [
        pltpu.make_async_copy(
            weight_hbm.at[pl.ds(pl.multiple_of(t * HALF_V + i * BLOCK_V, BLOCK_V), BLOCK_V), :],
            weight.at[i * BLOCK_V:(i + 1) * BLOCK_V, :],
            weight_sem.at[i],
        )
        for i in range(BLOCKS - 1)
    ]
    last_at = (BLOCKS - 1) * BLOCK_V
    rest = VOCAB - HALF_V
    last_first = pltpu.make_async_copy(
        weight_hbm.at[last_at:HALF_V, :],
        weight.at[last_at:HALF_V, :],
        weight_sem.at[BLOCKS - 1],
    )
    last_second = pltpu.make_async_copy(
        weight_hbm.at[HALF_V + last_at:VOCAB, :],
        weight.at[last_at:rest, :],
        weight_sem.at[BLOCKS - 1],
    )
    for copy in weight_copies:
        copy.start()

    @pl.when(t == 0)
    def _():
        last_first.start()

    @pl.when(t == 1)
    def _():
        last_second.start()
        weight[rest:HALF_V, :] = jnp.zeros((HALF_V - rest, WIDTH), BF16)

    low = sublane_ids(8, 512) < 4
    for copy in small_copies:
        copy.wait()

    def pack(k, carry):
        x = hidden_ref[pl.ds(pl.multiple_of(k * 16, 16), 16), :].astype(F32)
        for i in range(2):
            left, right = x[8 * i:8 * i + 8, 0:512], x[8 * i:8 * i + 8, 512:1024]
            message[4 * k + 2 * i] = jnp.where(low, left, pltpu.roll(right, 4, 0)).astype(BF16)
            message[4 * k + 2 * i + 1] = jnp.where(low, pltpu.roll(left, 4, 0), right).astype(BF16)
        return carry

    lax.fori_loop(0, ROWS // 16, pack, 0)
    arrived[me] = message[me]

    routes_row = routes_ref[...].astype(F32)
    live = (lane_ids(1, ROWS) < length_ref[0]).astype(F32)
    half_live = live * 0.5
    weight_row = half_live * agree_ref[...].astype(F32)
    frames_here = jnp.sum(live, axis=1, keepdims=True)
    named = (routes_row == sublane_ids(STUDENTS, ROWS).astype(F32)).astype(F32)
    earlier = (sublane_ids(ROWS, ROWS) < lane_ids(ROWS, ROWS)).astype(F32)
    before = jnp.dot(named.astype(BF16), earlier.astype(BF16), preferred_element_type=F32)
    slot = jnp.sum(before * named, axis=0, keepdims=True)
    wanted = (routes_row - (t * CHIPS).astype(F32)) * 8.0 + slot
    wanted = jnp.transpose(jnp.broadcast_to(wanted, (8, ROWS)))[:, 0:1]

    bias_row[:, 0:VOCAB] = bias_ref[...]
    bias_row[:, VOCAB:2 * HALF_V] = jnp.zeros((1, 2 * HALF_V - VOCAB), F32)

    def bias_step(k, carry):
        strip = bias_row[:, pl.ds(pl.multiple_of(t * HALF_V + k * 128, 128), 128)]
        bias_t[rows_at(k, 128), :] = jnp.transpose(jnp.broadcast_to(strip, (128, 128)))
        return carry

    lax.fori_loop(0, HALF_V // 128, bias_step, 0)

    teacher[VOCAB:2 * HALF_V, :] = jnp.full((2 * HALF_V - VOCAB, ROWS), -1e30, BF16)

    def max_step(k, top):
        return jnp.maximum(top, folded(teacher[rows_at(k), :], 16, jnp.maximum))

    top = jnp.full((16, ROWS), -1e30, BF16)
    for q in range(PIECES):
        teacher_copies[q].wait()
        last = cuts[q + 1] // STEP if q < PIECES - 1 else 2 * HALF_V // STEP
        top = lax.fori_loop(cuts[q] // STEP, last, max_step, top, unroll=2)
    top = jnp.max(top.astype(F32), axis=0, keepdims=True)

    pl.semaphore_wait(barrier, CHIPS)

    def hidden_copy(k, receiving):
        ids = moved(k, 1)
        source = index_of(moved(k, -1)) if receiving else me
        return pltpu.make_async_remote_copy(
            src_ref=message.at[index_of(ids)],
            dst_ref=arrived.at[source],
            send_sem=hidden_send.at[k],
            recv_sem=hidden_recv.at[k],
            device_id=(t, ids[0], ids[1], ids[2]),
            device_id_type=MESH,
        )

    for k in OFFSETS:
        hidden_copy(k, False).start()

    def sum_step(k, total):
        return total + folded(jnp.exp(teacher[rows_at(k), :].astype(F32) - top), 8, jnp.add)

    total = lax.fori_loop(0, 2 * HALF_V // STEP, sum_step, jnp.zeros((8, ROWS), F32), unroll=2)
    scale_row = weight_row / jnp.sum(total, axis=0, keepdims=True)

    target_row = target_ref[...]
    step_rows = sublane_ids(STEP, ROWS)

    def soft_step(k, mass):
        rows = rows_at(k)
        e = jnp.exp(teacher[rows, :].astype(F32) - top)
        hit = step_rows == target_row - k * STEP
        s = (e * scale_row + jnp.where(hit, half_live, 0.0)).astype(BF16)
        soft[rows, :] = s
        return mass + folded(s.astype(F32), 8, jnp.add)

    piece = HALF_V // PIECES
    soft_copies = [
        pltpu.make_async_remote_copy(
            src_ref=soft.at[pl.ds(pl.multiple_of((1 - t) * HALF_V + q * piece, 64), piece), :],
            dst_ref=soft_in.at[q * piece:(q + 1) * piece, :],
            send_sem=soft_send.at[q],
            recv_sem=soft_recv.at[q],
            device_id=other_core,
            device_id_type=MESH,
        )
        for q in range(PIECES)
    ]
    mass = jnp.zeros((8, ROWS), F32)
    for q in range(PIECES):
        first = (1 - t) * (HALF_V // STEP) + q * (piece // STEP)
        mass = lax.fori_loop(first, first + piece // STEP, soft_step, mass)
        soft_copies[q].start()
    first = t * (HALF_V // STEP)
    mass = lax.fori_loop(first, first + HALF_V // STEP, soft_step, mass)
    mass = jnp.sum(mass, axis=0, keepdims=True)

    for k in OFFSETS:
        hidden_copy(k, True).wait_recv()
    rows_in = arrived[...].reshape(CHIPS * 8, 512)

    def to_pair(source, target, index):
        return pltpu.make_async_remote_copy(
            src_ref=source,
            dst_ref=target,
            send_sem=pair_send.at[index],
            recv_sem=pair_recv.at[index],
            device_id=other_core,
            device_id_type=MESH,
        )

    hidden_swaps = []
    for i in range(2):
        pick = (wanted + 4.0 * i == lane_ids(ROWS, CHIPS * 8).astype(F32)).astype(F32).astype(BF16)
        at = slice(512 * i, 512 * i + 512)
        mine_h[:, at] = jnp.dot(pick, rows_in, preferred_element_type=F32).astype(BF16)
        hidden_swaps.append(to_pair(mine_h.at[:, at], their_h.at[:, at], 3 * i))
        hidden_swaps[i].start()

    for copy in hidden_swaps:
        copy.wait_recv()
    states = mine_h[...].astype(F32) + their_h[...].astype(F32)
    states = states - jnp.mean(states, axis=1, keepdims=True)
    spread = jnp.mean(jnp.square(states), axis=1, keepdims=True)
    states = states * lax.rsqrt(spread + EPSILON)
    normed[...] = states
    turned = jnp.transpose((states * gain_ref[...]).astype(BF16).astype(F32))
    scaled_t[...] = turned.reshape(WIDTH // 8, 8, ROWS)
    scaled[...] = turned.astype(BF16)

    for copy in weight_copies:
        copy.wait()

    @pl.when(t == 0)
    def _():
        last_first.wait()

    @pl.when(t == 1)
    def _():
        last_second.wait()

    peaks, sums = [], []
    for i in range(BLOCKS):
        at = slice(i * BLOCK_V, (i + 1) * BLOCK_V)
        slope = bias_t[at, :]
        block = jnp.dot(weight[at, :], scaled[...], preferred_element_type=F32)
        block = block + jnp.concatenate([slope, slope], axis=1)
        if i == BLOCKS - 1:
            inside = sublane_ids(BLOCK_V, ROWS) < VOCAB - i * BLOCK_V - t * HALF_V
            block = jnp.where(inside, block, -1e30)
        logits[at, :] = block
        peak = jnp.max(folded(block, 8, jnp.maximum), axis=0, keepdims=True)
        total = jnp.zeros((8, ROWS), F32)
        for k in range(BLOCK_V // STEP):
            part_at = slice(i * BLOCK_V + k * STEP, i * BLOCK_V + (k + 1) * STEP)
            total = total + folded(jnp.exp(logits[part_at, :] - peak), 8, jnp.add)
        peaks.append(peak)
        sums.append(total)
    peak = peaks[0]
    for other in peaks[1:]:
        peak = jnp.maximum(peak, other)
    total = jnp.zeros((8, ROWS), F32)
    for other, terms in zip(peaks, sums):
        total = total + terms * jnp.exp(other - peak)
    lse = peak + jnp.log(jnp.sum(total, axis=0, keepdims=True))
    stats[...] = jnp.concatenate([lse, mass, jnp.zeros((6, ROWS), F32)], axis=0)
    stats_swap = to_pair(stats, stats_in, 1)
    stats_swap.start()

    for part in range(PARTS):
        half = part // 3
        for row in range(0, 64, 2):
            pair = jnp.concatenate(
                [scaled_t[half * 64 + chunk_of(part, row)], scaled_t[half * 64 + chunk_of(part, row + 1)]],
                axis=0,
            )
            lhs[part, row * 8:row * 8 + 16, :] = pair.astype(BF16)

    for copy in soft_copies:
        copy.wait_recv()
    stats_swap.wait_recv()
    there = stats_in[...]
    other_lse = there[0:1, :]
    highest = jnp.maximum(lse, other_lse)
    lse = highest + jnp.log(jnp.exp(lse - highest) + jnp.exp(other_lse - highest))
    mass = mass + there[1:2, :]

    def grad_step(k, loss):
        rows = slice(k * STEP, (k + 1) * STEP)
        log_probs = logits[rows, :] - lse
        own = pl.ds(pl.multiple_of(t * HALF_V + k * STEP, STEP), STEP)
        both = soft[own, :].astype(F32) + soft_in[rows, :].astype(F32)
        grad[rows, :] = (mass * jnp.exp(log_probs) - both).astype(BF16)
        return loss - folded(both * log_probs, 8, jnp.add)

    def columns(part, chunk):
        first, width = CHUNKS[part % 3][chunk]
        return slice(first, first + width)

    def grad_columns(part, chunk):
        first = THIRDS[part % 3][0]
        at = columns(part, chunk)
        return slice(first + at.start, first + at.stop)

    def remote(part, chunk, source, target, rows, index, device):
        at = columns(part, chunk)
        number = (part * 2 + chunk) * COPIES + index
        return pltpu.make_async_remote_copy(
            src_ref=source.at[part, rows, at],
            dst_ref=target.at[part, rows, at],
            send_sem=send_sem.at[number],
            recv_sem=recv_sem.at[number],
            device_id=device,
            device_id_type=MESH,
        )

    def copy_of(part, chunk, stage):
        rows = slice(STAGE_AT[stage], STAGE_AT[stage] + STAGE_ROWS[stage])
        source, target = (sent, got) if stage < NARROW else (sent_wide, got_wide)
        return remote(part, chunk, source, target, rows, stage, partners[(part + stage) % 6])

    def last_copy(part, chunk, flip):
        rows = slice(LAST_AT + 8 * flip, LAST_AT + 8 * flip + 8)
        bits = [(part + STAGES + k) % 6 for k in range(2) if FLIPS[flip][k]]
        return remote(part, chunk, sent_wide, got_wide, rows, STAGES + flip, partner(*bits))

    def vec_copy(step, flip):
        bits = [2 * step + k for k in range(2) if FLIPS[flip][k]]
        return pltpu.make_async_remote_copy(
            src_ref=vec.at[step],
            dst_ref=vec_in.at[3 * step + flip],
            send_sem=vec_send_sem.at[3 * step + flip],
            recv_sem=vec_recv_sem.at[3 * step + flip],
            device_id=partner(*bits) if step < ROUNDS else other_core,
            device_id_type=MESH,
        )

    def vec_start(step):
        for flip in (2, 0, 1) if step < ROUNDS else (0,):
            vec_copy(step, flip).start()

    def vec_step(step):
        for flip in range(3):
            vec_copy(step - 1, flip).wait_recv()
        at = 3 * (step - 1)
        vec[step] = (vec[step - 1] + vec_in[at]) + (vec_in[at + 1] + vec_in[at + 2])
        vec_start(step)

    def product(part, chunk, at):
        return lax.dot_general(
            lhs[part, pl.ds(pl.multiple_of(at, 256), 256), :], grad[grad_columns(part, chunk), :],
            (((1,), (1,)), ((), ())), preferred_element_type=F32,
        )

    loss = jnp.zeros((8, ROWS), F32)
    for chunk in range(2):
        for third in range(3):
            at = grad_columns(third, chunk)
            for k in range(at.start // STEP, at.stop // STEP):
                loss = grad_step(k, loss)
            for part in (third, third + 3):
                block = product(part, chunk, (1 - mine[part]) * 256)
                sent[part, 0:256, columns(part, chunk)] = block.astype(BF16)
                copy_of(part, chunk, 0).start()

    for i in range(BLOCKS):
        at = slice(i * BLOCK_V, (i + 1) * BLOCK_V)
        grad_n[:, at] = jnp.transpose(grad[at, :].astype(F32)).astype(BF16)
    for i in range(4):
        at = slice(i * 256, (i + 1) * 256)
        back = jnp.dot(grad_n[...], weight[:, at], preferred_element_type=F32)
        vec[0, :, at] = jnp.sum(back * normed[:, at], axis=0, keepdims=True)
    ones = jnp.ones((16, ROWS), BF16)
    vec[0, :, WIDTH:LOSS_AT] = jnp.dot(ones, grad_n[...], preferred_element_type=F32)[0:1, :]
    lane = lane_ids(1, 128)
    loss_here = jnp.sum(jnp.sum(loss, axis=0, keepdims=True), axis=1, keepdims=True)
    vec[0, :, LOSS_AT:VEC] = jnp.where(lane == 0, loss_here, jnp.where(lane == 1, frames_here, 0.0))
    vec_start(0)
    for chunk in range(2):
        for part in ORDER:
            acc[part, :, columns(part, chunk)] = product(part, chunk, mine[part] * 256)
    for k in OFFSETS:
        hidden_copy(k, False).wait_send()
    for copy in hidden_swaps:
        copy.wait_send()
    stats_swap.wait_send()
    for copy in soft_copies:
        copy.wait_send()

    base = [0] * PARTS
    for stage in range(1, STAGES):
        rows = STAGE_ROWS[stage]
        before_at = STAGE_AT[stage - 1]
        incoming = got if stage - 1 < NARROW else got_wide
        for chunk in range(2):
            kept = []
            for part in ORDER:
                bit = mine[(part + stage) % 6]
                away, stay = (1 - bit) * rows, bit * rows
                at = columns(part, chunk)

                def joined(offset, part=part, at=at):
                    first = pl.multiple_of(base[part] + offset, 16)
                    return acc[part, pl.ds(first, rows), at] + incoming[
                        part, pl.ds(pl.multiple_of(before_at + offset, 16), rows), at
                    ].astype(F32)

                copy_of(part, chunk, stage - 1).wait_recv()
                block = joined(away)
                place_at = slice(STAGE_AT[stage], STAGE_AT[stage] + rows)
                if stage < NARROW:
                    sent[part, place_at, at] = block.astype(BF16)
                else:
                    sent_wide[part, place_at, at] = block
                copy_of(part, chunk, stage).start()
                kept.append((part, at, pl.ds(pl.multiple_of(base[part] + stay, 16), rows), joined, stay))
            for part, at, where, sum_at, stay in kept:
                acc[part, where, at] = sum_at(stay)
        vec_step(stage)
        for part in range(PARTS):
            base[part] = base[part] + mine[(part + stage) % 6] * rows

    for chunk in range(2):
        for part in ORDER:
            at = columns(part, chunk)
            rows = pl.ds(pl.multiple_of(base[part], 32), 32)
            high, low_bit = mine[(part + STAGES) % 6], mine[(part + STAGES + 1) % 6]
            copy_of(part, chunk, STAGES - 1).wait_recv()
            acc[part, rows, at] += got_wide[part, 0:32, at]
            for flip in (2, 0, 1):
                to_high = 1 - high if FLIPS[flip][0] else high
                to_low = 1 - low_bit if FLIPS[flip][1] else low_bit
                first = pl.multiple_of(base[part] + to_high * 16 + to_low * 8, 8)
                sent_wide[part, LAST_AT + 8 * flip:LAST_AT + 8 * flip + 8, at] = acc[
                    part, pl.ds(first, 8), at
                ]
                last_copy(part, chunk, flip).start()
    inverse = 1.0 / vec[ROUNDS, :, LOSS_AT + 1:LOSS_AT + 2]
    for chunk in range(2):
        for part in ORDER:
            at = columns(part, chunk)
            high, low_bit = mine[(part + STAGES) % 6], mine[(part + STAGES + 1) % 6]
            first = pl.multiple_of(base[part] + high * 16 + low_bit * 8, 8)
            total = acc[part, pl.ds(first, 8), at]
            for flip in range(3):
                last_copy(part, chunk, flip).wait_recv()
                total = total + got_wide[part, LAST_AT + 8 * flip:LAST_AT + 8 * flip + 8, at]
            final[part // 3, :, grad_columns(part, chunk)] = total * inverse

    swap = to_pair(final.at[1 - t], final_in, 2)
    swap.start()
    vec_copy(ROUNDS, 0).wait_recv()
    total, beside = vec[ROUNDS], vec_in[3 * ROUNDS]
    gain_out[...] = (total[:, 0:WIDTH] + beside[:, 0:WIDTH]) * inverse
    loss_out[...] = (total[:, LOSS_AT:VEC] + beside[:, LOSS_AT:VEC]) * inverse

    @pl.when(t == 0)
    def _():
        bias_out[:, 0:HALF_V] = total[:, WIDTH:LOSS_AT] * inverse
        bias_out[:, HALF_V:VOCAB] = beside[:, WIDTH:WIDTH + rest] * inverse
        weight_out[:, 0:HALF_V] = final[0]

    @pl.when(t == 1)
    def _():
        bias_out[:, 0:HALF_V] = beside[:, WIDTH:LOSS_AT] * inverse
        bias_out[:, HALF_V:VOCAB] = total[:, WIDTH:WIDTH + rest] * inverse
        weight_out[:, HALF_V:VOCAB] = final[1, :, 0:rest]

    for part in range(PARTS):
        for chunk in range(2):
            for stage in range(STAGES):
                copy_of(part, chunk, stage).wait_send()
            for flip in range(3):
                last_copy(part, chunk, flip).wait_send()
    for step in range(ROUNDS):
        for flip in range(3):
            vec_copy(step, flip).wait_send()
    vec_copy(ROUNDS, 0).wait_send()
    swap.wait_recv()

    @pl.when(t == 0)
    def _():
        weight_out[:, HALF_V:VOCAB] = final_in[:, 0:rest]

    @pl.when(t == 1)
    def _():
        weight_out[:, 0:HALF_V] = final_in[...]

    swap.wait_send()


def finish_kernel(weight_in, gain_in, bias_in, loss_in, weight_out, gain_out, bias_out, loss_out):
    weight_out[...] = weight_in[...]
    gain_out[...] = gain_in[...]
    bias_out[...] = bias_in[...]
    loss_out[...] = loss_in[...]


def distill(*arrays):
    vmem = pl.BlockSpec(memory_space=pltpu.VMEM)
    hbm = pl.BlockSpec(memory_space=pl.ANY)
    dma = pltpu.SemaphoreType.DMA
    return pl.pallas_call(
        step_kernel,
        out_shape=(
            jax.ShapeDtypeStruct((8, VOCAB), F32),
            jax.ShapeDtypeStruct((1, WIDTH), F32),
            jax.ShapeDtypeStruct((1, VOCAB), F32),
            jax.ShapeDtypeStruct((1, 128), F32),
        ),
        in_specs=[hbm] * 8 + [pl.BlockSpec(memory_space=pltpu.SMEM)],
        out_specs=(vmem,) * 4,
        scratch_shapes=[
            pltpu.VMEM((ROWS, WIDTH), BF16),
            pltpu.VMEM((1, ROWS), jnp.int32),
            pltpu.VMEM((1, ROWS), jnp.int32),
            pltpu.VMEM((1, ROWS), jnp.int32),
            pltpu.VMEM((1, WIDTH), F32),
            pltpu.VMEM((1, VOCAB), F32),
            pltpu.VMEM((2 * HALF_V, ROWS), BF16),
            pltpu.VMEM((2 * HALF_V, ROWS), BF16),
            pltpu.VMEM((HALF_V, ROWS), BF16),
            pltpu.VMEM((HALF_V, WIDTH), BF16),
            pltpu.VMEM((CHIPS, 8, 512), BF16),
            pltpu.VMEM((CHIPS, 8, 512), BF16),
            pltpu.VMEM((8, ROWS), F32),
            pltpu.VMEM((8, ROWS), F32),
            pltpu.VMEM((ROWS, WIDTH), BF16),
            pltpu.VMEM((ROWS, WIDTH), BF16),
            pltpu.VMEM((1, 2 * HALF_V), F32),
            pltpu.VMEM((HALF_V, 128), F32),
            pltpu.VMEM((ROWS, WIDTH), F32),
            pltpu.VMEM((WIDTH, ROWS), BF16),
            pltpu.VMEM((WIDTH // 8, 8, ROWS), F32),
            pltpu.VMEM((HALF_V, ROWS), F32),
            pltpu.VMEM((HALF_V, ROWS), BF16),
            pltpu.VMEM((ROWS, HALF_V), BF16),
            pltpu.VMEM((PARTS, 512, ROWS), BF16),
            pltpu.VMEM((PARTS, 256, WIDEST), F32),
            pltpu.VMEM((PARTS, NARROW_ROWS, WIDEST), BF16),
            pltpu.VMEM((PARTS, NARROW_ROWS, WIDEST), BF16),
            pltpu.VMEM((PARTS, WIDE_ROWS, WIDEST), F32),
            pltpu.VMEM((PARTS, WIDE_ROWS, WIDEST), F32),
            pltpu.VMEM((2, 8, HALF_V), F32),
            pltpu.VMEM((8, HALF_V), F32),
            pltpu.VMEM((ROUNDS + 1, 1, VEC), F32),
            pltpu.VMEM((3 * ROUNDS + 1, 1, VEC), F32),
            dma((6,)),
            dma((PIECES,)),
            dma((BLOCKS,)),
            dma((CHIPS,)),
            dma((CHIPS,)),
            dma((PIECES,)),
            dma((PIECES,)),
            dma((4,)),
            dma((4,)),
            dma((PARTS * 2 * COPIES,)),
            dma((PARTS * 2 * COPIES,)),
            dma((3 * ROUNDS + 1,)),
            dma((3 * ROUNDS + 1,)),
        ],
        compiler_params=pltpu.CompilerParams(
            collective_id=0, has_side_effects=True, vmem_limit_bytes=60 * 1024 * 1024
        ),
    )(*arrays)


def body(
    teacher_logits, routes, agreement, targets, lengths, student_hidden, out_weight, out_bias, gain
):
    weight_grad, gain_grad, bias_grad, loss = distill(
        teacher_logits[0].T,
        out_weight.T,
        student_hidden,
        routes.reshape(1, ROWS),
        agreement[None],
        targets[None],
        out_bias[None],
        gain[None],
        lengths,
    )
    vmem = pl.BlockSpec(memory_space=pltpu.VMEM)
    parts = (weight_grad, gain_grad, bias_grad, loss)
    weight_grad, gain_grad, bias_grad, loss = pl.pallas_call(
        finish_kernel,
        out_shape=tuple(jax.ShapeDtypeStruct(x.shape, x.dtype) for x in parts),
        in_specs=[vmem] * 4,
        out_specs=(vmem,) * 4,
    )(*parts)
    return (weight_grad, gain_grad[0], bias_grad[0], loss[0, 0])


def solution(mesh):
    finer = Mesh(
        mesh.devices.reshape(mesh.shape["teach"], 4, 4, 4), ("teach", "dp_0", "dp_1", "dp_2")
    )
    in_specs = (
        P("teach", DP, None),
        P(DP, None),
        P(DP),
        P(DP),
        P(DP),
        P(TEACH_DP, None),
        P(),
        P(),
        P(),
    )
    out_specs = (P(TEACH_DP, None), P(), P(), P())
    return jax.shard_map(body, mesh=finer, in_specs=in_specs, out_specs=out_specs, check_vma=False)
```

```python
import jax
import jax.numpy as jnp
from jax import lax
from jax.experimental import pallas as pl
from jax.experimental.pallas import tpu as pltpu
from jax.sharding import Mesh
from jax.sharding import PartitionSpec as P

DP = ("dp_0", "dp_1", "dp_2")
TEACH_DP = ("teach", "dp_0", "dp_1", "dp_2")
MESH = pl.DeviceIdType.MESH
F32 = jnp.float32
BF16 = jnp.bfloat16

EPSILON = 1e-05
VOCAB = 5000
WIDTH = 1024
ROWS = 256
STUDENTS = 128

HALF_V = 2560
BLOCK_V = 512
BLOCKS = 5
THIRDS = ((0, 896), (896, 896), (1792, 768))
WIDEST = 896
CHUNKS = (((0, 512), (512, 384)), ((0, 512), (512, 384)), ((0, 384), (384, 384)))
STAGE_ROWS = (256, 128)
STAGE_AT = (0, 256)
QUAD_ROWS = (32, 8)
QUAD_AT = (384, 0)
NARROW_ROWS = 480
WIDE_ROWS = 24
FLIPS = ((1, 0), (0, 1), (1, 1))
PARTS = 6
STAGES = 2
COPIES = 8
ORDER = (0, 3, 1, 4, 2, 5)
ROUNDS = 3
VEC = WIDTH + HALF_V + 128
LOSS_AT = WIDTH + HALF_V
STEP = 64
PIECES = 4
CHIPS = 64


def chunk_of(part, row):
    bits = [0] * 6
    for k in range(6):
        bits[(part + k) % 6] = (row >> (5 - k)) & 1
    chip = 0
    for dim in range(3):
        low, high = bits[dim], bits[3 + dim]
        chip = chip * 4 + high * 2 + (high ^ low)
    return chip


def hops(k):
    return sum(min(d, 4 - d) for d in (k // 16, (k // 4) % 4, k % 4))


OFFSETS = tuple(sorted(((k * 21) % CHIPS for k in range(1, CHIPS)), key=lambda k: -hops(k)))


def rows_at(k, size=STEP):
    return pl.ds(pl.multiple_of(k * size, size), size)


def lane_ids(rows, width):
    return lax.broadcasted_iota(jnp.int32, (rows, width), 1)


def sublane_ids(rows, width):
    return lax.broadcasted_iota(jnp.int32, (rows, width), 0)


def folded(x, rows, op):
    groups = x.reshape(x.shape[0] // rows, rows, x.shape[1])
    total = groups[0]
    for k in range(1, groups.shape[0]):
        total = op(total, groups[k])
    return total


def step_kernel(
    teacher_hbm, weight_hbm, hidden_hbm, routes_hbm, agree_hbm, target_hbm, bias_hbm, gain_hbm, length_ref,
    weight_out, gain_out, bias_out, loss_out,
    hidden_ref, routes_ref, agree_ref, target_ref, gain_ref, bias_ref,
    teacher, soft, soft_in, weight, message, arrived, stats, stats_in, mine_h, their_h,
    bias_row, bias_t, normed, scaled, scaled_t, logits, grad, grad_n,
    lhs, acc, sent, got, sent_wide, got_wide, final, final_in, vec, vec_in,
    small_sem, teacher_sem, weight_sem, hidden_send, hidden_recv, soft_send, soft_recv, pair_send, pair_recv,
    send_sem, recv_sem, vec_send_sem, vec_recv_sem,
):
    t = lax.axis_index("teach")
    place = [lax.axis_index(axis) for axis in DP]
    me = place[0] * 16 + place[1] * 4 + place[2]

    def partner(*bits):
        ids = list(place)
        for bit in bits:
            v = place[bit % 3]
            ids[bit % 3] = (3 - v) if bit >= 3 else (v + 1 - 2 * (v % 2))
        return (t, ids[0], ids[1], ids[2])

    def my_bit(bit):
        v = place[bit % 3]
        return v // 2 if bit >= 3 else (v // 2 + v % 2) % 2

    partners = [partner(bit) for bit in range(6)]
    mine = [my_bit(bit) for bit in range(6)]
    other_core = (1 - t, place[0], place[1], place[2])

    turned_by = [[(v + d) % 4 for d in range(4)] for v in place]

    def moved(k, sign):
        steps = (k // 16, (k // 4) % 4, k % 4)
        return [turned_by[axis][(sign * d) % 4] for axis, d in enumerate(steps)]

    def index_of(ids):
        return ids[0] * 16 + ids[1] * 4 + ids[2]

    small_copies = [
        pltpu.make_async_copy(source, target, small_sem.at[i])
        for i, (source, target) in enumerate(
            (
                (hidden_hbm, hidden_ref),
                (routes_hbm, routes_ref),
                (agree_hbm, agree_ref),
                (target_hbm, target_ref),
                (gain_hbm, gain_ref),
                (bias_hbm, bias_ref),
            )
        )
    ]
    for copy in small_copies:
        copy.start()
    barrier = pltpu.get_barrier_semaphore()
    for k in OFFSETS:
        ids = moved(k, 1)
        pl.semaphore_signal(
            barrier, inc=1, device_id=(t, ids[0], ids[1], ids[2]), device_id_type=MESH
        )
    pl.semaphore_signal(barrier, inc=1, device_id=other_core, device_id_type=MESH)

    cuts = (0, 1280, 2560, 3840, VOCAB)
    teacher_copies = [
        pltpu.make_async_copy(
            teacher_hbm.at[cuts[q]:cuts[q + 1], :],
            teacher.at[cuts[q]:cuts[q + 1], :],
            teacher_sem.at[q],
        )
        for q in range(PIECES)
    ]
    for copy in teacher_copies:
        copy.start()
    weight_copies = [
        pltpu.make_async_copy(
            weight_hbm.at[pl.ds(pl.multiple_of(t * HALF_V + i * BLOCK_V, BLOCK_V), BLOCK_V), :],
            weight.at[i * BLOCK_V:(i + 1) * BLOCK_V, :],
            weight_sem.at[i],
        )
        for i in range(BLOCKS - 1)
    ]
    last_at = (BLOCKS - 1) * BLOCK_V
    rest = VOCAB - HALF_V
    last_first = pltpu.make_async_copy(
        weight_hbm.at[last_at:HALF_V, :],
        weight.at[last_at:HALF_V, :],
        weight_sem.at[BLOCKS - 1],
    )
    last_second = pltpu.make_async_copy(
        weight_hbm.at[HALF_V + last_at:VOCAB, :],
        weight.at[last_at:rest, :],
        weight_sem.at[BLOCKS - 1],
    )
    for copy in weight_copies:
        copy.start()

    @pl.when(t == 0)
    def _():
        last_first.start()

    @pl.when(t == 1)
    def _():
        last_second.start()
        weight[rest:HALF_V, :] = jnp.zeros((HALF_V - rest, WIDTH), BF16)

    low = sublane_ids(8, 512) < 4
    for copy in small_copies:
        copy.wait()

    def pack(k, carry):
        x = hidden_ref[pl.ds(pl.multiple_of(k * 16, 16), 16), :].astype(F32)
        for i in range(2):
            left, right = x[8 * i:8 * i + 8, 0:512], x[8 * i:8 * i + 8, 512:1024]
            message[4 * k + 2 * i] = jnp.where(low, left, pltpu.roll(right, 4, 0)).astype(BF16)
            message[4 * k + 2 * i + 1] = jnp.where(low, pltpu.roll(left, 4, 0), right).astype(BF16)
        return carry

    lax.fori_loop(0, ROWS // 16, pack, 0)
    arrived[me] = message[me]

    routes_row = routes_ref[...].astype(F32)
    live = (lane_ids(1, ROWS) < length_ref[0]).astype(F32)
    half_live = live * 0.5
    weight_row = half_live * agree_ref[...].astype(F32)
    frames_here = jnp.sum(live, axis=1, keepdims=True)
    named = (routes_row == sublane_ids(STUDENTS, ROWS).astype(F32)).astype(F32)
    earlier = (sublane_ids(ROWS, ROWS) < lane_ids(ROWS, ROWS)).astype(F32)
    before = jnp.dot(named.astype(BF16), earlier.astype(BF16), preferred_element_type=F32)
    slot = jnp.sum(before * named, axis=0, keepdims=True)
    wanted = (routes_row - (t * CHIPS).astype(F32)) * 8.0 + slot
    wanted = jnp.transpose(jnp.broadcast_to(wanted, (8, ROWS)))[:, 0:1]

    bias_row[:, 0:VOCAB] = bias_ref[...]
    bias_row[:, VOCAB:2 * HALF_V] = jnp.zeros((1, 2 * HALF_V - VOCAB), F32)

    def bias_step(k, carry):
        strip = bias_row[:, pl.ds(pl.multiple_of(t * HALF_V + k * 128, 128), 128)]
        bias_t[rows_at(k, 128), :] = jnp.transpose(jnp.broadcast_to(strip, (128, 128)))
        return carry

    lax.fori_loop(0, HALF_V // 128, bias_step, 0)

    teacher[VOCAB:2 * HALF_V, :] = jnp.full((2 * HALF_V - VOCAB, ROWS), -1e30, BF16)

    def max_step(k, top):
        return jnp.maximum(top, folded(teacher[rows_at(k), :], 16, jnp.maximum))

    top = jnp.full((16, ROWS), -1e30, BF16)
    for q in range(PIECES):
        teacher_copies[q].wait()
        last = cuts[q + 1] // STEP if q < PIECES - 1 else 2 * HALF_V // STEP
        top = lax.fori_loop(cuts[q] // STEP, last, max_step, top, unroll=2)
    top = jnp.max(top.astype(F32), axis=0, keepdims=True)

    pl.semaphore_wait(barrier, CHIPS)

    def hidden_copy(k, receiving):
        ids = moved(k, 1)
        source = index_of(moved(k, -1)) if receiving else me
        return pltpu.make_async_remote_copy(
            src_ref=message.at[index_of(ids)],
            dst_ref=arrived.at[source],
            send_sem=hidden_send.at[k],
            recv_sem=hidden_recv.at[k],
            device_id=(t, ids[0], ids[1], ids[2]),
            device_id_type=MESH,
        )

    for k in OFFSETS:
        hidden_copy(k, False).start()

    def sum_step(k, total):
        return total + folded(jnp.exp(teacher[rows_at(k), :].astype(F32) - top), 8, jnp.add)

    total = lax.fori_loop(0, 2 * HALF_V // STEP, sum_step, jnp.zeros((8, ROWS), F32), unroll=2)
    scale_row = weight_row / jnp.sum(total, axis=0, keepdims=True)

    target_row = target_ref[...]
    step_rows = sublane_ids(STEP, ROWS)

    def soft_step(k, mass):
        rows = rows_at(k)
        e = jnp.exp(teacher[rows, :].astype(F32) - top)
        hit = step_rows == target_row - k * STEP
        s = (e * scale_row + jnp.where(hit, half_live, 0.0)).astype(BF16)
        soft[rows, :] = s
        return mass + folded(s.astype(F32), 8, jnp.add)

    piece = HALF_V // PIECES
    soft_copies = [
        pltpu.make_async_remote_copy(
            src_ref=soft.at[pl.ds(pl.multiple_of((1 - t) * HALF_V + q * piece, 64), piece), :],
            dst_ref=soft_in.at[q * piece:(q + 1) * piece, :],
            send_sem=soft_send.at[q],
            recv_sem=soft_recv.at[q],
            device_id=other_core,
            device_id_type=MESH,
        )
        for q in range(PIECES)
    ]
    mass = jnp.zeros((8, ROWS), F32)
    for q in range(PIECES):
        first = (1 - t) * (HALF_V // STEP) + q * (piece // STEP)
        mass = lax.fori_loop(first, first + piece // STEP, soft_step, mass)
        soft_copies[q].start()
    first = t * (HALF_V // STEP)
    mass = lax.fori_loop(first, first + HALF_V // STEP, soft_step, mass)
    mass = jnp.sum(mass, axis=0, keepdims=True)

    for k in OFFSETS:
        hidden_copy(k, True).wait_recv()
    rows_in = arrived[...].reshape(CHIPS * 8, 512)

    def to_pair(source, target, index):
        return pltpu.make_async_remote_copy(
            src_ref=source,
            dst_ref=target,
            send_sem=pair_send.at[index],
            recv_sem=pair_recv.at[index],
            device_id=other_core,
            device_id_type=MESH,
        )

    hidden_swaps = []
    for i in range(2):
        pick = (wanted + 4.0 * i == lane_ids(ROWS, CHIPS * 8).astype(F32)).astype(F32).astype(BF16)
        at = slice(512 * i, 512 * i + 512)
        mine_h[:, at] = jnp.dot(pick, rows_in, preferred_element_type=F32).astype(BF16)
        hidden_swaps.append(to_pair(mine_h.at[:, at], their_h.at[:, at], 3 * i))
        hidden_swaps[i].start()

    for copy in hidden_swaps:
        copy.wait_recv()
    states = mine_h[...].astype(F32) + their_h[...].astype(F32)
    states = states - jnp.mean(states, axis=1, keepdims=True)
    spread = jnp.mean(jnp.square(states), axis=1, keepdims=True)
    states = states * lax.rsqrt(spread + EPSILON)
    normed[...] = states
    turned = jnp.transpose((states * gain_ref[...]).astype(BF16).astype(F32))
    scaled_t[...] = turned.reshape(WIDTH // 8, 8, ROWS)
    scaled[...] = turned.astype(BF16)

    for copy in weight_copies:
        copy.wait()

    @pl.when(t == 0)
    def _():
        last_first.wait()

    @pl.when(t == 1)
    def _():
        last_second.wait()

    peaks, sums = [], []
    for i in range(BLOCKS):
        at = slice(i * BLOCK_V, (i + 1) * BLOCK_V)
        slope = bias_t[at, :]
        block = jnp.dot(weight[at, :], scaled[...], preferred_element_type=F32)
        block = block + jnp.concatenate([slope, slope], axis=1)
        if i == BLOCKS - 1:
            inside = sublane_ids(BLOCK_V, ROWS) < VOCAB - i * BLOCK_V - t * HALF_V
            block = jnp.where(inside, block, -1e30)
        logits[at, :] = block
        peak = jnp.max(folded(block, 8, jnp.maximum), axis=0, keepdims=True)
        total = jnp.zeros((8, ROWS), F32)
        for k in range(BLOCK_V // STEP):
            part_at = slice(i * BLOCK_V + k * STEP, i * BLOCK_V + (k + 1) * STEP)
            total = total + folded(jnp.exp(logits[part_at, :] - peak), 8, jnp.add)
        peaks.append(peak)
        sums.append(total)
    peak = peaks[0]
    for other in peaks[1:]:
        peak = jnp.maximum(peak, other)
    total = jnp.zeros((8, ROWS), F32)
    for other, terms in zip(peaks, sums):
        total = total + terms * jnp.exp(other - peak)
    lse = peak + jnp.log(jnp.sum(total, axis=0, keepdims=True))
    stats[...] = jnp.concatenate([lse, mass, jnp.zeros((6, ROWS), F32)], axis=0)
    stats_swap = to_pair(stats, stats_in, 1)
    stats_swap.start()

    for part in range(PARTS):
        half = part // 3
        for row in range(0, 64, 2):
            pair = jnp.concatenate(
                [scaled_t[half * 64 + chunk_of(part, row)], scaled_t[half * 64 + chunk_of(part, row + 1)]],
                axis=0,
            )
            lhs[part, row * 8:row * 8 + 16, :] = pair.astype(BF16)

    for copy in soft_copies:
        copy.wait_recv()
    stats_swap.wait_recv()
    there = stats_in[...]
    other_lse = there[0:1, :]
    highest = jnp.maximum(lse, other_lse)
    lse = highest + jnp.log(jnp.exp(lse - highest) + jnp.exp(other_lse - highest))
    mass = mass + there[1:2, :]

    def grad_step(k, loss):
        rows = slice(k * STEP, (k + 1) * STEP)
        log_probs = logits[rows, :] - lse
        own = pl.ds(pl.multiple_of(t * HALF_V + k * STEP, STEP), STEP)
        both = soft[own, :].astype(F32) + soft_in[rows, :].astype(F32)
        grad[rows, :] = (mass * jnp.exp(log_probs) - both).astype(BF16)
        return loss - folded(both * log_probs, 8, jnp.add)

    def columns(part, chunk):
        first, width = CHUNKS[part % 3][chunk]
        return slice(first, first + width)

    def grad_columns(part, chunk):
        first = THIRDS[part % 3][0]
        at = columns(part, chunk)
        return slice(first + at.start, first + at.stop)

    def remote(part, chunk, source, target, rows, index, device):
        at = columns(part, chunk)
        number = (part * 2 + chunk) * COPIES + index
        return pltpu.make_async_remote_copy(
            src_ref=source.at[part, rows, at],
            dst_ref=target.at[part, rows, at],
            send_sem=send_sem.at[number],
            recv_sem=recv_sem.at[number],
            device_id=device,
            device_id_type=MESH,
        )

    def copy_of(part, chunk, stage):
        rows = slice(STAGE_AT[stage], STAGE_AT[stage] + STAGE_ROWS[stage])
        return remote(part, chunk, sent, got, rows, stage, partners[(part + stage) % 6])

    def quad_bits(part, turn):
        first = part + STAGES + 2 * turn
        return first % 6, (first + 1) % 6

    def quad_rows(turn, flip):
        first = QUAD_AT[turn] + QUAD_ROWS[turn] * flip
        return slice(first, first + QUAD_ROWS[turn])

    def quad_copy(part, chunk, turn, flip):
        bits = [bit for bit, wanted in zip(quad_bits(part, turn), FLIPS[flip]) if wanted]
        source, target = (sent, got) if turn == 0 else (sent_wide, got_wide)
        index = STAGES + 3 * turn + flip
        return remote(part, chunk, source, target, quad_rows(turn, flip), index, partner(*bits))

    def quad_offset(part, turn, flip):
        first, second = (mine[bit] for bit in quad_bits(part, turn))
        if flip is not None:
            first = 1 - first if FLIPS[flip][0] else first
            second = 1 - second if FLIPS[flip][1] else second
        return (first * 2 + second) * QUAD_ROWS[turn]

    def vec_copy(step, flip):
        bits = [2 * step + k for k in range(2) if FLIPS[flip][k]]
        return pltpu.make_async_remote_copy(
            src_ref=vec.at[step],
            dst_ref=vec_in.at[3 * step + flip],
            send_sem=vec_send_sem.at[3 * step + flip],
            recv_sem=vec_recv_sem.at[3 * step + flip],
            device_id=partner(*bits) if step < ROUNDS else other_core,
            device_id_type=MESH,
        )

    def vec_start(step):
        for flip in (2, 0, 1) if step < ROUNDS else (0,):
            vec_copy(step, flip).start()

    def vec_step(step):
        for flip in range(3):
            vec_copy(step - 1, flip).wait_recv()
        at = 3 * (step - 1)
        vec[step] = (vec[step - 1] + vec_in[at]) + (vec_in[at + 1] + vec_in[at + 2])
        vec_start(step)

    def product(part, chunk, at):
        return lax.dot_general(
            lhs[part, pl.ds(pl.multiple_of(at, 256), 256), :], grad[grad_columns(part, chunk), :],
            (((1,), (1,)), ((), ())), preferred_element_type=F32,
        )

    loss = jnp.zeros((8, ROWS), F32)
    for chunk in range(2):
        for third in range(3):
            at = grad_columns(third, chunk)
            for k in range(at.start // STEP, at.stop // STEP):
                loss = grad_step(k, loss)
            for part in (third, third + 3):
                block = product(part, chunk, (1 - mine[part]) * 256)
                sent[part, 0:256, columns(part, chunk)] = block.astype(BF16)
                copy_of(part, chunk, 0).start()

    for i in range(BLOCKS):
        at = slice(i * BLOCK_V, (i + 1) * BLOCK_V)
        grad_n[:, at] = jnp.transpose(grad[at, :].astype(F32)).astype(BF16)
    for i in range(4):
        at = slice(i * 256, (i + 1) * 256)
        back = jnp.dot(grad_n[...], weight[:, at], preferred_element_type=F32)
        vec[0, :, at] = jnp.sum(back * normed[:, at], axis=0, keepdims=True)
    ones = jnp.ones((16, ROWS), BF16)
    vec[0, :, WIDTH:LOSS_AT] = jnp.dot(ones, grad_n[...], preferred_element_type=F32)[0:1, :]
    lane = lane_ids(1, 128)
    loss_here = jnp.sum(jnp.sum(loss, axis=0, keepdims=True), axis=1, keepdims=True)
    vec[0, :, LOSS_AT:VEC] = jnp.where(lane == 0, loss_here, jnp.where(lane == 1, frames_here, 0.0))
    vec_start(0)
    for chunk in range(2):
        for part in ORDER:
            acc[part, :, columns(part, chunk)] = product(part, chunk, mine[part] * 256)
    for k in OFFSETS:
        hidden_copy(k, False).wait_send()
    for copy in hidden_swaps:
        copy.wait_send()
    stats_swap.wait_send()
    for copy in soft_copies:
        copy.wait_send()

    def taken(part, at, first, rows, begin):
        return acc[part, pl.ds(first, rows), at] + got[
            part, pl.ds(pl.multiple_of(begin, 16), rows), at
        ].astype(F32)

    rows, base = STAGE_ROWS[1], [0] * PARTS
    for chunk in range(2):
        for part in ORDER:
            at = columns(part, chunk)
            away = pl.multiple_of((1 - mine[(part + 1) % 6]) * rows, rows)
            copy_of(part, chunk, 0).wait_recv()
            sent[part, STAGE_AT[1]:STAGE_AT[1] + rows, at] = taken(part, at, away, rows, away).astype(BF16)
            copy_of(part, chunk, 1).start()
        for part in ORDER:
            at = columns(part, chunk)
            stay = pl.multiple_of(mine[(part + 1) % 6] * rows, rows)
            acc[part, pl.ds(stay, rows), at] = taken(part, at, stay, rows, stay)
    vec_step(1)
    base = [mine[(part + 1) % 6] * rows for part in range(PARTS)]

    rows = QUAD_ROWS[0]
    for chunk in range(2):
        for part in ORDER:
            at = columns(part, chunk)
            copy_of(part, chunk, 1).wait_recv()
            for flip in (2, 0, 1):
                offset = quad_offset(part, 0, flip)
                first = pl.multiple_of(base[part] + offset, rows)
                block = taken(part, at, first, rows, STAGE_AT[1] + offset)
                sent[part, quad_rows(0, flip), at] = block.astype(BF16)
                quad_copy(part, chunk, 0, flip).start()
        for part in ORDER:
            at = columns(part, chunk)
            offset = quad_offset(part, 0, None)
            first = pl.multiple_of(base[part] + offset, rows)
            acc[part, pl.ds(first, rows), at] = taken(part, at, first, rows, STAGE_AT[1] + offset)
    vec_step(2)
    base = [base[part] + quad_offset(part, 0, None) for part in range(PARTS)]

    for chunk in range(2):
        for part in ORDER:
            at = columns(part, chunk)
            where = pl.ds(pl.multiple_of(base[part], rows), rows)
            block = acc[part, where, at]
            for flip in range(3):
                quad_copy(part, chunk, 0, flip).wait_recv()
                block = block + got[part, quad_rows(0, flip), at].astype(F32)
            acc[part, where, at] = block
            for flip in (2, 0, 1):
                first = pl.multiple_of(base[part] + quad_offset(part, 1, flip), 8)
                sent_wide[part, quad_rows(1, flip), at] = acc[part, pl.ds(first, 8), at]
                quad_copy(part, chunk, 1, flip).start()
    vec_step(3)
    inverse = 1.0 / vec[ROUNDS, :, LOSS_AT + 1:LOSS_AT + 2]
    for chunk in range(2):
        for part in ORDER:
            at = columns(part, chunk)
            first = pl.multiple_of(base[part] + quad_offset(part, 1, None), 8)
            total = acc[part, pl.ds(first, 8), at]
            for flip in range(3):
                quad_copy(part, chunk, 1, flip).wait_recv()
                total = total + got_wide[part, quad_rows(1, flip), at]
            final[part // 3, :, grad_columns(part, chunk)] = total * inverse

    swap = to_pair(final.at[1 - t], final_in, 2)
    swap.start()
    vec_copy(ROUNDS, 0).wait_recv()
    total, beside = vec[ROUNDS], vec_in[3 * ROUNDS]
    gain_out[...] = (total[:, 0:WIDTH] + beside[:, 0:WIDTH]) * inverse
    loss_out[...] = (total[:, LOSS_AT:VEC] + beside[:, LOSS_AT:VEC]) * inverse

    @pl.when(t == 0)
    def _():
        bias_out[:, 0:HALF_V] = total[:, WIDTH:LOSS_AT] * inverse
        bias_out[:, HALF_V:VOCAB] = beside[:, WIDTH:WIDTH + rest] * inverse
        weight_out[:, 0:HALF_V] = final[0]

    @pl.when(t == 1)
    def _():
        bias_out[:, 0:HALF_V] = beside[:, WIDTH:LOSS_AT] * inverse
        bias_out[:, HALF_V:VOCAB] = total[:, WIDTH:WIDTH + rest] * inverse
        weight_out[:, HALF_V:VOCAB] = final[1, :, 0:rest]

    for part in range(PARTS):
        for chunk in range(2):
            for stage in range(STAGES):
                copy_of(part, chunk, stage).wait_send()
            for turn in range(2):
                for flip in range(3):
                    quad_copy(part, chunk, turn, flip).wait_send()
    for step in range(ROUNDS):
        for flip in range(3):
            vec_copy(step, flip).wait_send()
    vec_copy(ROUNDS, 0).wait_send()
    swap.wait_recv()

    @pl.when(t == 0)
    def _():
        weight_out[:, HALF_V:VOCAB] = final_in[:, 0:rest]

    @pl.when(t == 1)
    def _():
        weight_out[:, 0:HALF_V] = final_in[...]

    swap.wait_send()


def finish_kernel(weight_in, gain_in, bias_in, loss_in, weight_out, gain_out, bias_out, loss_out):
    weight_out[...] = weight_in[...]
    gain_out[...] = gain_in[...]
    bias_out[...] = bias_in[...]
    loss_out[...] = loss_in[...]


def distill(*arrays):
    vmem = pl.BlockSpec(memory_space=pltpu.VMEM)
    hbm = pl.BlockSpec(memory_space=pl.ANY)
    dma = pltpu.SemaphoreType.DMA
    return pl.pallas_call(
        step_kernel,
        out_shape=(
            jax.ShapeDtypeStruct((8, VOCAB), F32),
            jax.ShapeDtypeStruct((1, WIDTH), F32),
            jax.ShapeDtypeStruct((1, VOCAB), F32),
            jax.ShapeDtypeStruct((1, 128), F32),
        ),
        in_specs=[hbm] * 8 + [pl.BlockSpec(memory_space=pltpu.SMEM)],
        out_specs=(vmem,) * 4,
        scratch_shapes=[
            pltpu.VMEM((ROWS, WIDTH), BF16),
            pltpu.VMEM((1, ROWS), jnp.int32),
            pltpu.VMEM((1, ROWS), jnp.int32),
            pltpu.VMEM((1, ROWS), jnp.int32),
            pltpu.VMEM((1, WIDTH), F32),
            pltpu.VMEM((1, VOCAB), F32),
            pltpu.VMEM((2 * HALF_V, ROWS), BF16),
            pltpu.VMEM((2 * HALF_V, ROWS), BF16),
            pltpu.VMEM((HALF_V, ROWS), BF16),
            pltpu.VMEM((HALF_V, WIDTH), BF16),
            pltpu.VMEM((CHIPS, 8, 512), BF16),
            pltpu.VMEM((CHIPS, 8, 512), BF16),
            pltpu.VMEM((8, ROWS), F32),
            pltpu.VMEM((8, ROWS), F32),
            pltpu.VMEM((ROWS, WIDTH), BF16),
            pltpu.VMEM((ROWS, WIDTH), BF16),
            pltpu.VMEM((1, 2 * HALF_V), F32),
            pltpu.VMEM((HALF_V, 128), F32),
            pltpu.VMEM((ROWS, WIDTH), F32),
            pltpu.VMEM((WIDTH, ROWS), BF16),
            pltpu.VMEM((WIDTH // 8, 8, ROWS), F32),
            pltpu.VMEM((HALF_V, ROWS), F32),
            pltpu.VMEM((HALF_V, ROWS), BF16),
            pltpu.VMEM((ROWS, HALF_V), BF16),
            pltpu.VMEM((PARTS, 512, ROWS), BF16),
            pltpu.VMEM((PARTS, 256, WIDEST), F32),
            pltpu.VMEM((PARTS, NARROW_ROWS, WIDEST), BF16),
            pltpu.VMEM((PARTS, NARROW_ROWS, WIDEST), BF16),
            pltpu.VMEM((PARTS, WIDE_ROWS, WIDEST), F32),
            pltpu.VMEM((PARTS, WIDE_ROWS, WIDEST), F32),
            pltpu.VMEM((2, 8, HALF_V), F32),
            pltpu.VMEM((8, HALF_V), F32),
            pltpu.VMEM((ROUNDS + 1, 1, VEC), F32),
            pltpu.VMEM((3 * ROUNDS + 1, 1, VEC), F32),
            dma((6,)),
            dma((PIECES,)),
            dma((BLOCKS,)),
            dma((CHIPS,)),
            dma((CHIPS,)),
            dma((PIECES,)),
            dma((PIECES,)),
            dma((4,)),
            dma((4,)),
            dma((PARTS * 2 * COPIES,)),
            dma((PARTS * 2 * COPIES,)),
            dma((3 * ROUNDS + 1,)),
            dma((3 * ROUNDS + 1,)),
        ],
        compiler_params=pltpu.CompilerParams(
            collective_id=0, has_side_effects=True, vmem_limit_bytes=60 * 1024 * 1024
        ),
    )(*arrays)


def body(
    teacher_logits, routes, agreement, targets, lengths, student_hidden, out_weight, out_bias, gain
):
    weight_grad, gain_grad, bias_grad, loss = distill(
        teacher_logits[0].T,
        out_weight.T,
        student_hidden,
        routes.reshape(1, ROWS),
        agreement[None],
        targets[None],
        out_bias[None],
        gain[None],
        lengths,
    )
    vmem = pl.BlockSpec(memory_space=pltpu.VMEM)
    parts = (weight_grad, gain_grad, bias_grad, loss)
    weight_grad, gain_grad, bias_grad, loss = pl.pallas_call(
        finish_kernel,
        out_shape=tuple(jax.ShapeDtypeStruct(x.shape, x.dtype) for x in parts),
        in_specs=[vmem] * 4,
        out_specs=(vmem,) * 4,
    )(*parts)
    return (weight_grad, gain_grad[0], bias_grad[0], loss[0, 0])


def solution(mesh):
    finer = Mesh(
        mesh.devices.reshape(mesh.shape["teach"], 4, 4, 4), ("teach", "dp_0", "dp_1", "dp_2")
    )
    in_specs = (
        P("teach", DP, None),
        P(DP, None),
        P(DP),
        P(DP),
        P(DP),
        P(TEACH_DP, None),
        P(),
        P(),
        P(),
    )
    out_specs = (P(TEACH_DP, None), P(), P(), P())
    return jax.shard_map(body, mesh=finer, in_specs=in_specs, out_specs=out_specs, check_vma=False)
```

```python
import jax
import jax.numpy as jnp
from jax import lax
from jax.experimental import pallas as pl
from jax.experimental.pallas import tpu as pltpu
from jax.sharding import Mesh
from jax.sharding import PartitionSpec as P

DP = ("dp_0", "dp_1", "dp_2")
TEACH_DP = ("teach", "dp_0", "dp_1", "dp_2")
MESH = pl.DeviceIdType.MESH
F32 = jnp.float32
BF16 = jnp.bfloat16

EPSILON = 1e-05
VOCAB = 5000
WIDTH = 1024
ROWS = 256
STUDENTS = 128

HALF_V = 2560
BLOCK_V = 512
BLOCKS = 5
THIRDS = ((0, 896), (896, 896), (1792, 768))
WIDEST = 896
CHUNKS = (((0, 512), (512, 384)), ((0, 512), (512, 384)), ((0, 384), (384, 384)))
STAGE_ROWS = (256, 128)
STAGE_AT = (0, 256)
QUAD_ROWS = (32, 8)
QUAD_AT = (384, 0)
NARROW_ROWS = 480
WIDE_ROWS = 24
FLIPS = ((1, 0), (0, 1), (1, 1))
PARTS = 6
STAGES = 2
COPIES = 8
ORDER = (0, 3, 1, 4, 2, 5)
ROUNDS = 3
VEC = WIDTH + HALF_V + 128
LOSS_AT = WIDTH + HALF_V
STEP = 64
PIECES = 4
CHIPS = 64


def chunk_of(part, row):
    bits = [0] * 6
    for k in range(6):
        bits[(part + k) % 6] = (row >> (5 - k)) & 1
    chip = 0
    for dim in range(3):
        low, high = bits[dim], bits[3 + dim]
        chip = chip * 4 + high * 2 + (high ^ low)
    return chip


def hops(k):
    return sum(min(d, 4 - d) for d in (k // 16, (k // 4) % 4, k % 4))


OFFSETS = tuple(sorted(((k * 21) % CHIPS for k in range(1, CHIPS)), key=lambda k: -hops(k)))


def rows_at(k, size=STEP):
    return pl.ds(pl.multiple_of(k * size, size), size)


def lane_ids(rows, width):
    return lax.broadcasted_iota(jnp.int32, (rows, width), 1)


def sublane_ids(rows, width):
    return lax.broadcasted_iota(jnp.int32, (rows, width), 0)


def folded(x, rows, op):
    groups = x.reshape(x.shape[0] // rows, rows, x.shape[1])
    total = groups[0]
    for k in range(1, groups.shape[0]):
        total = op(total, groups[k])
    return total


def step_kernel(
    teacher_hbm, weight_hbm, hidden_hbm, routes_hbm, agree_hbm, target_hbm, bias_hbm, gain_hbm, length_ref,
    weight_out, gain_out, bias_out, loss_out,
    hidden_ref, routes_ref, agree_ref, target_ref, gain_ref, bias_ref,
    teacher, soft, soft_in, weight, message, arrived, stats, stats_in, mine_h, their_h,
    bias_row, bias_t, normed, scaled, scaled_t, logits, grad, grad_n,
    lhs, acc, sent, got, sent_wide, got_wide, final, final_in, vec, vec_in,
    small_sem, teacher_sem, weight_sem, hidden_send, hidden_recv, soft_send, soft_recv, pair_send, pair_recv,
    send_sem, recv_sem, vec_send_sem, vec_recv_sem,
):
    t = lax.axis_index("teach")
    place = [lax.axis_index(axis) for axis in DP]
    me = place[0] * 16 + place[1] * 4 + place[2]

    def partner(*bits):
        ids = list(place)
        for bit in bits:
            v = place[bit % 3]
            ids[bit % 3] = (3 - v) if bit >= 3 else (v + 1 - 2 * (v % 2))
        return (t, ids[0], ids[1], ids[2])

    def my_bit(bit):
        v = place[bit % 3]
        return v // 2 if bit >= 3 else (v // 2 + v % 2) % 2

    partners = [partner(bit) for bit in range(6)]
    mine = [my_bit(bit) for bit in range(6)]
    other_core = (1 - t, place[0], place[1], place[2])

    turned_by = [[(v + d) % 4 for d in range(4)] for v in place]

    def moved(k, sign):
        steps = (k // 16, (k // 4) % 4, k % 4)
        return [turned_by[axis][(sign * d) % 4] for axis, d in enumerate(steps)]

    def index_of(ids):
        return ids[0] * 16 + ids[1] * 4 + ids[2]

    small_copies = [
        pltpu.make_async_copy(source, target, small_sem.at[i])
        for i, (source, target) in enumerate(
            (
                (hidden_hbm, hidden_ref),
                (routes_hbm, routes_ref),
                (agree_hbm, agree_ref),
                (target_hbm, target_ref),
                (gain_hbm, gain_ref),
                (bias_hbm, bias_ref),
            )
        )
    ]
    for copy in small_copies:
        copy.start()
    barrier = pltpu.get_barrier_semaphore()
    for k in OFFSETS:
        ids = moved(k, 1)
        pl.semaphore_signal(
            barrier, inc=1, device_id=(t, ids[0], ids[1], ids[2]), device_id_type=MESH
        )
    pl.semaphore_signal(barrier, inc=1, device_id=other_core, device_id_type=MESH)

    cuts = (0, 1280, 2560, 3840, VOCAB)
    teacher_copies = [
        pltpu.make_async_copy(
            teacher_hbm.at[cuts[q]:cuts[q + 1], :],
            teacher.at[cuts[q]:cuts[q + 1], :],
            teacher_sem.at[q],
        )
        for q in range(PIECES)
    ]
    for copy in teacher_copies:
        copy.start()
    weight_copies = [
        pltpu.make_async_copy(
            weight_hbm.at[pl.ds(pl.multiple_of(t * HALF_V + i * BLOCK_V, BLOCK_V), BLOCK_V), :],
            weight.at[i * BLOCK_V:(i + 1) * BLOCK_V, :],
            weight_sem.at[i],
        )
        for i in range(BLOCKS - 1)
    ]
    last_at = (BLOCKS - 1) * BLOCK_V
    rest = VOCAB - HALF_V
    last_first = pltpu.make_async_copy(
        weight_hbm.at[last_at:HALF_V, :],
        weight.at[last_at:HALF_V, :],
        weight_sem.at[BLOCKS - 1],
    )
    last_second = pltpu.make_async_copy(
        weight_hbm.at[HALF_V + last_at:VOCAB, :],
        weight.at[last_at:rest, :],
        weight_sem.at[BLOCKS - 1],
    )
    for copy in weight_copies:
        copy.start()

    @pl.when(t == 0)
    def _():
        last_first.start()

    @pl.when(t == 1)
    def _():
        last_second.start()
        weight[rest:HALF_V, :] = jnp.zeros((HALF_V - rest, WIDTH), BF16)

    low = sublane_ids(8, 512) < 4
    for copy in small_copies:
        copy.wait()

    def pack(k, carry):
        x = hidden_ref[pl.ds(pl.multiple_of(k * 16, 16), 16), :].astype(F32)
        for i in range(2):
            left, right = x[8 * i:8 * i + 8, 0:512], x[8 * i:8 * i + 8, 512:1024]
            message[4 * k + 2 * i] = jnp.where(low, left, pltpu.roll(right, 4, 0)).astype(BF16)
            message[4 * k + 2 * i + 1] = jnp.where(low, pltpu.roll(left, 4, 0), right).astype(BF16)
        return carry

    lax.fori_loop(0, ROWS // 16, pack, 0)
    arrived[me] = message[me]

    routes_row = routes_ref[...].astype(F32)
    live = (lane_ids(1, ROWS) < length_ref[0]).astype(F32)
    half_live = live * 0.5
    weight_row = half_live * agree_ref[...].astype(F32)
    frames_here = jnp.sum(live, axis=1, keepdims=True)
    named = (routes_row == sublane_ids(STUDENTS, ROWS).astype(F32)).astype(F32)
    earlier = (sublane_ids(ROWS, ROWS) < lane_ids(ROWS, ROWS)).astype(F32)
    before = jnp.dot(named.astype(BF16), earlier.astype(BF16), preferred_element_type=F32)
    slot = jnp.sum(before * named, axis=0, keepdims=True)
    wanted = (routes_row - (t * CHIPS).astype(F32)) * 8.0 + slot
    wanted = jnp.transpose(jnp.broadcast_to(wanted, (8, ROWS)))[:, 0:1]

    bias_row[:, 0:VOCAB] = bias_ref[...]
    bias_row[:, VOCAB:2 * HALF_V] = jnp.zeros((1, 2 * HALF_V - VOCAB), F32)

    def bias_step(k, carry):
        strip = bias_row[:, pl.ds(pl.multiple_of(t * HALF_V + k * 128, 128), 128)]
        bias_t[rows_at(k, 128), :] = jnp.transpose(jnp.broadcast_to(strip, (128, 128)))
        return carry

    lax.fori_loop(0, HALF_V // 128, bias_step, 0)

    teacher[VOCAB:2 * HALF_V, :] = jnp.full((2 * HALF_V - VOCAB, ROWS), -1e30, BF16)

    def max_step(k, top):
        return jnp.maximum(top, folded(teacher[rows_at(k), :], 16, jnp.maximum))

    top = jnp.full((16, ROWS), -1e30, BF16)
    for q in range(PIECES):
        teacher_copies[q].wait()
        last = cuts[q + 1] // STEP if q < PIECES - 1 else 2 * HALF_V // STEP
        top = lax.fori_loop(cuts[q] // STEP, last, max_step, top, unroll=2)
    top = jnp.max(top.astype(F32), axis=0, keepdims=True)

    pl.semaphore_wait(barrier, CHIPS)

    def hidden_copy(k, receiving):
        ids = moved(k, 1)
        source = index_of(moved(k, -1)) if receiving else me
        return pltpu.make_async_remote_copy(
            src_ref=message.at[index_of(ids)],
            dst_ref=arrived.at[source],
            send_sem=hidden_send.at[k],
            recv_sem=hidden_recv.at[k],
            device_id=(t, ids[0], ids[1], ids[2]),
            device_id_type=MESH,
        )

    for k in OFFSETS:
        hidden_copy(k, False).start()

    def sum_step(k, total):
        return total + folded(jnp.exp(teacher[rows_at(k), :].astype(F32) - top), 8, jnp.add)

    total = lax.fori_loop(0, 2 * HALF_V // STEP, sum_step, jnp.zeros((8, ROWS), F32), unroll=2)
    scale_row = weight_row / jnp.sum(total, axis=0, keepdims=True)

    target_row = target_ref[...]
    step_rows = sublane_ids(STEP, ROWS)

    def soft_step(k, mass):
        rows = rows_at(k)
        e = jnp.exp(teacher[rows, :].astype(F32) - top)
        hit = step_rows == target_row - k * STEP
        s = (e * scale_row + jnp.where(hit, half_live, 0.0)).astype(BF16)
        soft[rows, :] = s
        return mass + folded(s.astype(F32), 8, jnp.add)

    piece = HALF_V // PIECES
    soft_copies = [
        pltpu.make_async_remote_copy(
            src_ref=soft.at[pl.ds(pl.multiple_of((1 - t) * HALF_V + q * piece, 64), piece), :],
            dst_ref=soft_in.at[q * piece:(q + 1) * piece, :],
            send_sem=soft_send.at[q],
            recv_sem=soft_recv.at[q],
            device_id=other_core,
            device_id_type=MESH,
        )
        for q in range(PIECES)
    ]
    mass = jnp.zeros((8, ROWS), F32)
    for q in range(PIECES):
        first = (1 - t) * (HALF_V // STEP) + q * (piece // STEP)
        mass = lax.fori_loop(first, first + piece // STEP, soft_step, mass)
        soft_copies[q].start()
    first = t * (HALF_V // STEP)
    mass = lax.fori_loop(first, first + HALF_V // STEP, soft_step, mass)
    mass = jnp.sum(mass, axis=0, keepdims=True)

    for k in OFFSETS:
        hidden_copy(k, True).wait_recv()
    rows_in = arrived[...].reshape(CHIPS * 8, 512)

    def to_pair(source, target, index):
        return pltpu.make_async_remote_copy(
            src_ref=source,
            dst_ref=target,
            send_sem=pair_send.at[index],
            recv_sem=pair_recv.at[index],
            device_id=other_core,
            device_id_type=MESH,
        )

    hidden_swaps = []
    for i in range(2):
        pick = (wanted + 4.0 * i == lane_ids(ROWS, CHIPS * 8).astype(F32)).astype(F32).astype(BF16)
        at = slice(512 * i, 512 * i + 512)
        mine_h[:, at] = jnp.dot(pick, rows_in, preferred_element_type=F32).astype(BF16)
        hidden_swaps.append(to_pair(mine_h.at[:, at], their_h.at[:, at], 3 * i))
        hidden_swaps[i].start()

    for copy in hidden_swaps:
        copy.wait_recv()
    states = mine_h[...].astype(F32) + their_h[...].astype(F32)
    states = states - jnp.mean(states, axis=1, keepdims=True)
    spread = jnp.mean(jnp.square(states), axis=1, keepdims=True)
    states = states * lax.rsqrt(spread + EPSILON)
    normed[...] = states
    turned = jnp.transpose((states * gain_ref[...]).astype(BF16).astype(F32))
    scaled_t[...] = turned.reshape(WIDTH // 8, 8, ROWS)
    scaled[...] = turned.astype(BF16)

    for copy in weight_copies:
        copy.wait()

    @pl.when(t == 0)
    def _():
        last_first.wait()

    @pl.when(t == 1)
    def _():
        last_second.wait()

    peaks, sums = [], []
    for i in range(BLOCKS):
        at = slice(i * BLOCK_V, (i + 1) * BLOCK_V)
        slope = bias_t[at, :]
        block = jnp.dot(weight[at, :], scaled[...], preferred_element_type=F32)
        block = block + jnp.concatenate([slope, slope], axis=1)
        if i == BLOCKS - 1:
            inside = sublane_ids(BLOCK_V, ROWS) < VOCAB - i * BLOCK_V - t * HALF_V
            block = jnp.where(inside, block, -1e30)
        logits[at, :] = block
        peak = jnp.max(folded(block, 8, jnp.maximum), axis=0, keepdims=True)
        total = jnp.zeros((8, ROWS), F32)
        for k in range(BLOCK_V // STEP):
            part_at = slice(i * BLOCK_V + k * STEP, i * BLOCK_V + (k + 1) * STEP)
            total = total + folded(jnp.exp(logits[part_at, :] - peak), 8, jnp.add)
        peaks.append(peak)
        sums.append(total)
    peak = peaks[0]
    for other in peaks[1:]:
        peak = jnp.maximum(peak, other)
    total = jnp.zeros((8, ROWS), F32)
    for other, terms in zip(peaks, sums):
        total = total + terms * jnp.exp(other - peak)
    lse = peak + jnp.log(jnp.sum(total, axis=0, keepdims=True))
    stats[...] = jnp.concatenate([lse, mass, jnp.zeros((6, ROWS), F32)], axis=0)
    stats_swap = to_pair(stats, stats_in, 1)
    stats_swap.start()

    for part in range(PARTS):
        half = part // 3
        for row in range(0, 64, 2):
            pair = jnp.concatenate(
                [scaled_t[half * 64 + chunk_of(part, row)], scaled_t[half * 64 + chunk_of(part, row + 1)]],
                axis=0,
            )
            lhs[part, row * 8:row * 8 + 16, :] = pair.astype(BF16)

    for copy in soft_copies:
        copy.wait_recv()
    stats_swap.wait_recv()
    there = stats_in[...]
    other_lse = there[0:1, :]
    highest = jnp.maximum(lse, other_lse)
    lse = highest + jnp.log(jnp.exp(lse - highest) + jnp.exp(other_lse - highest))
    mass = mass + there[1:2, :]

    def grad_step(k, loss):
        rows = slice(k * STEP, (k + 1) * STEP)
        log_probs = logits[rows, :] - lse
        own = pl.ds(pl.multiple_of(t * HALF_V + k * STEP, STEP), STEP)
        both = soft[own, :].astype(F32) + soft_in[rows, :].astype(F32)
        grad[rows, :] = (mass * jnp.exp(log_probs) - both).astype(BF16)
        return loss - folded(both * log_probs, 8, jnp.add)

    def columns(part, chunk):
        first, width = CHUNKS[part % 3][chunk]
        return slice(first, first + width)

    def grad_columns(part, chunk):
        first = THIRDS[part % 3][0]
        at = columns(part, chunk)
        return slice(first + at.start, first + at.stop)

    def remote(part, chunk, source, target, rows, index, device):
        at = columns(part, chunk)
        number = (part * 2 + chunk) * COPIES + index
        return pltpu.make_async_remote_copy(
            src_ref=source.at[part, rows, at],
            dst_ref=target.at[part, rows, at],
            send_sem=send_sem.at[number],
            recv_sem=recv_sem.at[number],
            device_id=device,
            device_id_type=MESH,
        )

    def copy_of(part, chunk, stage):
        rows = slice(STAGE_AT[stage], STAGE_AT[stage] + STAGE_ROWS[stage])
        return remote(part, chunk, sent, got, rows, stage, partners[(part + stage) % 6])

    def quad_bits(part, turn):
        first = part + STAGES + 2 * turn
        return first % 6, (first + 1) % 6

    def quad_rows(turn, flip):
        first = QUAD_AT[turn] + QUAD_ROWS[turn] * flip
        return slice(first, first + QUAD_ROWS[turn])

    def quad_copy(part, chunk, turn, flip):
        bits = [bit for bit, wanted in zip(quad_bits(part, turn), FLIPS[flip]) if wanted]
        source, target = (sent, got) if turn == 0 else (sent_wide, got_wide)
        index = STAGES + 3 * turn + flip
        return remote(part, chunk, source, target, quad_rows(turn, flip), index, partner(*bits))

    def quad_offset(part, turn, flip):
        first, second = (mine[bit] for bit in quad_bits(part, turn))
        if flip is not None:
            first = 1 - first if FLIPS[flip][0] else first
            second = 1 - second if FLIPS[flip][1] else second
        return (first * 2 + second) * QUAD_ROWS[turn]

    def vec_copy(step, flip):
        bits = [2 * step + k for k in range(2) if FLIPS[flip][k]]
        return pltpu.make_async_remote_copy(
            src_ref=vec.at[step],
            dst_ref=vec_in.at[3 * step + flip],
            send_sem=vec_send_sem.at[3 * step + flip],
            recv_sem=vec_recv_sem.at[3 * step + flip],
            device_id=partner(*bits) if step < ROUNDS else other_core,
            device_id_type=MESH,
        )

    def vec_start(step):
        for flip in (2, 0, 1) if step < ROUNDS else (0,):
            vec_copy(step, flip).start()

    def vec_step(step):
        for flip in range(3):
            vec_copy(step - 1, flip).wait_recv()
        at = 3 * (step - 1)
        vec[step] = (vec[step - 1] + vec_in[at]) + (vec_in[at + 1] + vec_in[at + 2])
        vec_start(step)

    def product(part, chunk, at):
        return lax.dot_general(
            lhs[part, pl.ds(pl.multiple_of(at, 256), 256), :], grad[grad_columns(part, chunk), :],
            (((1,), (1,)), ((), ())), preferred_element_type=F32,
        )

    loss = jnp.zeros((8, ROWS), F32)
    for chunk in range(2):
        for third in range(3):
            at = grad_columns(third, chunk)
            for k in range(at.start // STEP, at.stop // STEP):
                loss = grad_step(k, loss)
            for part in (third, third + 3):
                block = product(part, chunk, (1 - mine[part]) * 256)
                sent[part, 0:256, columns(part, chunk)] = block.astype(BF16)

            @pl.when(t == 0)
            def _(third=third, chunk=chunk):
                for part in (third, third + 3):
                    copy_of(part, chunk, 0).start()

    for i in range(BLOCKS):
        at = slice(i * BLOCK_V, (i + 1) * BLOCK_V)
        grad_n[:, at] = jnp.transpose(grad[at, :].astype(F32)).astype(BF16)
    for i in range(4):
        at = slice(i * 256, (i + 1) * 256)
        back = jnp.dot(grad_n[...], weight[:, at], preferred_element_type=F32)
        vec[0, :, at] = jnp.sum(back * normed[:, at], axis=0, keepdims=True)
    ones = jnp.ones((16, ROWS), BF16)
    vec[0, :, WIDTH:LOSS_AT] = jnp.dot(ones, grad_n[...], preferred_element_type=F32)[0:1, :]
    lane = lane_ids(1, 128)
    loss_here = jnp.sum(jnp.sum(loss, axis=0, keepdims=True), axis=1, keepdims=True)
    vec[0, :, LOSS_AT:VEC] = jnp.where(lane == 0, loss_here, jnp.where(lane == 1, frames_here, 0.0))
    vec_start(0)

    @pl.when(t == 1)
    def _():
        for chunk in range(2):
            for part in ORDER:
                copy_of(part, chunk, 0).start()

    for chunk in range(2):
        for part in ORDER:
            acc[part, :, columns(part, chunk)] = product(part, chunk, mine[part] * 256)
    for k in OFFSETS:
        hidden_copy(k, False).wait_send()
    for copy in hidden_swaps:
        copy.wait_send()
    stats_swap.wait_send()
    for copy in soft_copies:
        copy.wait_send()

    def taken(part, at, first, rows, begin):
        return acc[part, pl.ds(first, rows), at] + got[
            part, pl.ds(pl.multiple_of(begin, 16), rows), at
        ].astype(F32)

    rows, base = STAGE_ROWS[1], [0] * PARTS
    for chunk in range(2):
        for part in ORDER:
            at = columns(part, chunk)
            away = pl.multiple_of((1 - mine[(part + 1) % 6]) * rows, rows)
            copy_of(part, chunk, 0).wait_recv()
            sent[part, STAGE_AT[1]:STAGE_AT[1] + rows, at] = taken(part, at, away, rows, away).astype(BF16)
            copy_of(part, chunk, 1).start()
        for part in ORDER:
            at = columns(part, chunk)
            stay = pl.multiple_of(mine[(part + 1) % 6] * rows, rows)
            acc[part, pl.ds(stay, rows), at] = taken(part, at, stay, rows, stay)
    vec_step(1)
    base = [mine[(part + 1) % 6] * rows for part in range(PARTS)]

    rows = QUAD_ROWS[0]
    for chunk in range(2):
        for part in ORDER:
            at = columns(part, chunk)
            copy_of(part, chunk, 1).wait_recv()
            for flip in (2, 0, 1):
                offset = quad_offset(part, 0, flip)
                first = pl.multiple_of(base[part] + offset, rows)
                block = taken(part, at, first, rows, STAGE_AT[1] + offset)
                sent[part, quad_rows(0, flip), at] = block.astype(BF16)
                quad_copy(part, chunk, 0, flip).start()
        for part in ORDER:
            at = columns(part, chunk)
            offset = quad_offset(part, 0, None)
            first = pl.multiple_of(base[part] + offset, rows)
            acc[part, pl.ds(first, rows), at] = taken(part, at, first, rows, STAGE_AT[1] + offset)
    vec_step(2)
    base = [base[part] + quad_offset(part, 0, None) for part in range(PARTS)]

    for chunk in range(2):
        for part in ORDER:
            at = columns(part, chunk)
            where = pl.ds(pl.multiple_of(base[part], rows), rows)
            block = acc[part, where, at]
            for flip in range(3):
                quad_copy(part, chunk, 0, flip).wait_recv()
                block = block + got[part, quad_rows(0, flip), at].astype(F32)
            acc[part, where, at] = block
            for flip in (2, 0, 1):
                first = pl.multiple_of(base[part] + quad_offset(part, 1, flip), 8)
                sent_wide[part, quad_rows(1, flip), at] = acc[part, pl.ds(first, 8), at]
                quad_copy(part, chunk, 1, flip).start()
    vec_step(3)
    inverse = 1.0 / vec[ROUNDS, :, LOSS_AT + 1:LOSS_AT + 2]
    for chunk in range(2):
        for part in ORDER:
            at = columns(part, chunk)
            first = pl.multiple_of(base[part] + quad_offset(part, 1, None), 8)
            total = acc[part, pl.ds(first, 8), at]
            for flip in range(3):
                quad_copy(part, chunk, 1, flip).wait_recv()
                total = total + got_wide[part, quad_rows(1, flip), at]
            final[part // 3, :, grad_columns(part, chunk)] = total * inverse

    swap = to_pair(final.at[1 - t], final_in, 2)
    swap.start()
    vec_copy(ROUNDS, 0).wait_recv()
    total, beside = vec[ROUNDS], vec_in[3 * ROUNDS]
    gain_out[...] = (total[:, 0:WIDTH] + beside[:, 0:WIDTH]) * inverse
    loss_out[...] = (total[:, LOSS_AT:VEC] + beside[:, LOSS_AT:VEC]) * inverse

    @pl.when(t == 0)
    def _():
        bias_out[:, 0:HALF_V] = total[:, WIDTH:LOSS_AT] * inverse
        bias_out[:, HALF_V:VOCAB] = beside[:, WIDTH:WIDTH + rest] * inverse
        weight_out[:, 0:HALF_V] = final[0]

    @pl.when(t == 1)
    def _():
        bias_out[:, 0:HALF_V] = beside[:, WIDTH:LOSS_AT] * inverse
        bias_out[:, HALF_V:VOCAB] = total[:, WIDTH:WIDTH + rest] * inverse
        weight_out[:, HALF_V:VOCAB] = final[1, :, 0:rest]

    for part in range(PARTS):
        for chunk in range(2):
            for stage in range(STAGES):
                copy_of(part, chunk, stage).wait_send()
            for turn in range(2):
                for flip in range(3):
                    quad_copy(part, chunk, turn, flip).wait_send()
    for step in range(ROUNDS):
        for flip in range(3):
            vec_copy(step, flip).wait_send()
    vec_copy(ROUNDS, 0).wait_send()
    swap.wait_recv()

    @pl.when(t == 0)
    def _():
        weight_out[:, HALF_V:VOCAB] = final_in[:, 0:rest]

    @pl.when(t == 1)
    def _():
        weight_out[:, 0:HALF_V] = final_in[...]

    swap.wait_send()


def finish_kernel(weight_in, gain_in, bias_in, loss_in, weight_out, gain_out, bias_out, loss_out):
    weight_out[...] = weight_in[...]
    gain_out[...] = gain_in[...]
    bias_out[...] = bias_in[...]
    loss_out[...] = loss_in[...]


def distill(*arrays):
    vmem = pl.BlockSpec(memory_space=pltpu.VMEM)
    hbm = pl.BlockSpec(memory_space=pl.ANY)
    dma = pltpu.SemaphoreType.DMA
    return pl.pallas_call(
        step_kernel,
        out_shape=(
            jax.ShapeDtypeStruct((8, VOCAB), F32),
            jax.ShapeDtypeStruct((1, WIDTH), F32),
            jax.ShapeDtypeStruct((1, VOCAB), F32),
            jax.ShapeDtypeStruct((1, 128), F32),
        ),
        in_specs=[hbm] * 8 + [pl.BlockSpec(memory_space=pltpu.SMEM)],
        out_specs=(vmem,) * 4,
        scratch_shapes=[
            pltpu.VMEM((ROWS, WIDTH), BF16),
            pltpu.VMEM((1, ROWS), jnp.int32),
            pltpu.VMEM((1, ROWS), jnp.int32),
            pltpu.VMEM((1, ROWS), jnp.int32),
            pltpu.VMEM((1, WIDTH), F32),
            pltpu.VMEM((1, VOCAB), F32),
            pltpu.VMEM((2 * HALF_V, ROWS), BF16),
            pltpu.VMEM((2 * HALF_V, ROWS), BF16),
            pltpu.VMEM((HALF_V, ROWS), BF16),
            pltpu.VMEM((HALF_V, WIDTH), BF16),
            pltpu.VMEM((CHIPS, 8, 512), BF16),
            pltpu.VMEM((CHIPS, 8, 512), BF16),
            pltpu.VMEM((8, ROWS), F32),
            pltpu.VMEM((8, ROWS), F32),
            pltpu.VMEM((ROWS, WIDTH), BF16),
            pltpu.VMEM((ROWS, WIDTH), BF16),
            pltpu.VMEM((1, 2 * HALF_V), F32),
            pltpu.VMEM((HALF_V, 128), F32),
            pltpu.VMEM((ROWS, WIDTH), F32),
            pltpu.VMEM((WIDTH, ROWS), BF16),
            pltpu.VMEM((WIDTH // 8, 8, ROWS), F32),
            pltpu.VMEM((HALF_V, ROWS), F32),
            pltpu.VMEM((HALF_V, ROWS), BF16),
            pltpu.VMEM((ROWS, HALF_V), BF16),
            pltpu.VMEM((PARTS, 512, ROWS), BF16),
            pltpu.VMEM((PARTS, 256, WIDEST), F32),
            pltpu.VMEM((PARTS, NARROW_ROWS, WIDEST), BF16),
            pltpu.VMEM((PARTS, NARROW_ROWS, WIDEST), BF16),
            pltpu.VMEM((PARTS, WIDE_ROWS, WIDEST), F32),
            pltpu.VMEM((PARTS, WIDE_ROWS, WIDEST), F32),
            pltpu.VMEM((2, 8, HALF_V), F32),
            pltpu.VMEM((8, HALF_V), F32),
            pltpu.VMEM((ROUNDS + 1, 1, VEC), F32),
            pltpu.VMEM((3 * ROUNDS + 1, 1, VEC), F32),
            dma((6,)),
            dma((PIECES,)),
            dma((BLOCKS,)),
            dma((CHIPS,)),
            dma((CHIPS,)),
            dma((PIECES,)),
            dma((PIECES,)),
            dma((4,)),
            dma((4,)),
            dma((PARTS * 2 * COPIES,)),
            dma((PARTS * 2 * COPIES,)),
            dma((3 * ROUNDS + 1,)),
            dma((3 * ROUNDS + 1,)),
        ],
        compiler_params=pltpu.CompilerParams(
            collective_id=0, has_side_effects=True, vmem_limit_bytes=60 * 1024 * 1024
        ),
    )(*arrays)


def body(
    teacher_logits, routes, agreement, targets, lengths, student_hidden, out_weight, out_bias, gain
):
    weight_grad, gain_grad, bias_grad, loss = distill(
        teacher_logits[0].T,
        out_weight.T,
        student_hidden,
        routes.reshape(1, ROWS),
        agreement[None],
        targets[None],
        out_bias[None],
        gain[None],
        lengths,
    )
    vmem = pl.BlockSpec(memory_space=pltpu.VMEM)
    parts = (weight_grad, gain_grad, bias_grad, loss)
    weight_grad, gain_grad, bias_grad, loss = pl.pallas_call(
        finish_kernel,
        out_shape=tuple(jax.ShapeDtypeStruct(x.shape, x.dtype) for x in parts),
        in_specs=[vmem] * 4,
        out_specs=(vmem,) * 4,
    )(*parts)
    return (weight_grad, gain_grad[0], bias_grad[0], loss[0, 0])


def solution(mesh):
    finer = Mesh(
        mesh.devices.reshape(mesh.shape["teach"], 4, 4, 4), ("teach", "dp_0", "dp_1", "dp_2")
    )
    in_specs = (
        P("teach", DP, None),
        P(DP, None),
        P(DP),
        P(DP),
        P(DP),
        P(TEACH_DP, None),
        P(),
        P(),
        P(),
    )
    out_specs = (P(TEACH_DP, None), P(), P(), P())
    return jax.shard_map(body, mesh=finer, in_specs=in_specs, out_specs=out_specs, check_vma=False)
```
